32 devices in a mesh: inter: 16 (over z, y, core), intra: 2 (over x).
Axes of the slice: x: 2, y: 2, z: 4, core: 2. Of those that a mesh axis runs over, the one named last changes fastest.
Arguments:
- hidden_in: bfloat16 [16, 256, 4096], P('inter', 'intra'), may hold values from -120 to 120, as said below
- norm_gain: bfloat16 [4096], P(('inter', 'intra')), may hold values from 0.5 to 2, as said below
- qkv_weight: bfloat16 [4096, 768], P(('inter', 'intra')), may hold values from -0.09375 to 0.09375
- attn_cotangent: bfloat16 [16, 256, 512], P('inter', 'intra'), may hold values from -6 to 6
Outputs:
- attn: bfloat16 [16, 256, 512], P('inter', 'intra')
- grad_in: bfloat16 [16, 256, 4096], P('inter', 'intra')
- weight_grad: float32 [4096, 768], P(('intra', 'inter'))
- gain_grad: float32 [4096], P(('intra', 'inter'))
The draws below stay inside these ranges and needn't reach their ends.
Inputs may be any that keep to these rules, and one draw needn't show every extreme that they name: `hidden_in`: activations with spread row and feature scales. `norm_gain`: positive gains.
All inputs are finite; a program needn't handle non-finite values.
Results may differ from the reference program's by a relative error of at most 0.015.
Values may be sent and summed in bfloat16 or wider, within the bound.
A program may use at most 64 MiB of HBM per device.

```python
import math
import jax
import jax.numpy as jnp
from jax import lax

D = 4096
HD = 128
HEADS = 4
SEQ = 256
SEQS = 16


def draw_hidden_in(key, part):
    key_base, key_rows, key_cols = jax.random.split(jax.random.fold_in(key, 11), 3)
    shape = (SEQS, SEQ, D)
    row_scale = jnp.exp(jax.random.uniform(key_rows, (SEQS, SEQ, 1), minval=0.0, maxval=math.log(10.0)))
    col_scale = jnp.exp(jax.random.uniform(key_cols, (1, 1, D), minval=math.log(0.5), maxval=math.log(3.0)))
    base = jnp.clip(jax.random.normal(key_base, shape), -4.0, 4.0)
    return (base * row_scale * col_scale).astype(jnp.bfloat16)


def draw_norm_gain(key, part):
    key_gain = jax.random.fold_in(key, 23)
    values_out = jnp.exp(jax.random.uniform(key_gain, (D,), minval=math.log(0.5), maxval=math.log(2.0)))
    return values_out.astype(jnp.bfloat16)


def block_scale(key, shape, cuts, least, high):
    loudness, own = 1.0, jax.random.fold_in(key, 6)
    for position, blocks in cuts:
        draws = jnp.exp(jax.random.uniform(jax.random.fold_in(own, position), (blocks,), jnp.float32, least / len(cuts), high / len(cuts)))
        loudness = loudness * jnp.repeat(draws, shape[position] // blocks).reshape([-1 if axis == position else 1 for axis in range(len(shape))])
    return loudness


def centred(stream_key, extent, width, bound, pieces=(), held_as=jnp.bfloat16):
    entries = width * jax.random.normal(stream_key, extent, jnp.float32)
    if pieces:
        entries = entries * block_scale(stream_key, extent, pieces, -0.22, 0.18)
    return jnp.clip(entries, -bound, bound).astype(held_as)


def setup_inputs(seed: int = 0) -> dict:
    arg_keys = jax.random.split(jax.random.key(seed), 5)
    return {
        "hidden_in": draw_hidden_in(jax.random.fold_in(arg_keys[4], 71), 0),
        "norm_gain": draw_norm_gain(jax.random.fold_in(arg_keys[4], 71), 0),
        "qkv_weight": centred(arg_keys[2], (D, (HEADS + 2) * HD), D ** -0.5, 0.09375, ((0, 32),)),
        "attn_cotangent": centred(arg_keys[3], (SEQS, SEQ, HEADS * HD), 1.0, 6.0, ((0, 16), (1, 2))),
    }


eps_norm = 1e-05
rope_base = 500000.0

def rope_tables(positions, head_size):
    half_size = head_size // 2
    freqs = rope_base ** (-jnp.arange(half_size, dtype=jnp.float32) / half_size)
    angles = positions.astype(jnp.float32)[:, None] * freqs[None, :]
    return (jnp.cos(angles), jnp.sin(angles))

def rotate(values_in, cosine, sine):
    half_size = values_in.shape[-1] // 2
    first, second = (values_in[..., :half_size], values_in[..., half_size:])
    return jnp.concatenate([first * cosine - second * sine, second * cosine + first * sine], axis=-1)

def unrotate(grad_out, cosine, sine):
    half_size = grad_out.shape[-1] // 2
    first, second = (grad_out[..., :half_size], grad_out[..., half_size:])
    return jnp.concatenate([first * cosine + second * sine, second * cosine - first * sine], axis=-1)

def reference(hidden_in, norm_gain, qkv_weight, attn_cotangent):
    gain = norm_gain.astype(jnp.float32)
    positions = jnp.arange(SEQ, dtype=jnp.int32)
    cosine, sine = rope_tables(positions, HD)
    row_pos = jnp.arange(SEQ * HEADS, dtype=jnp.int32) // HEADS
    allowed = positions[None, :] <= row_pos[:, None]
    scale = HD ** (-0.5)
    qcols = HEADS * HD

    def one_sequence(carry, items):
        weight_acc, gain_acc = carry
        rows_in, grad_attn = items
        wide_rows = rows_in.astype(jnp.float32)
        inv_rms = lax.rsqrt(lax.optimization_barrier(jnp.mean(wide_rows * wide_rows, axis=1, keepdims=True)) + eps_norm)
        normed = (wide_rows * inv_rms * gain[None, :]).astype(jnp.bfloat16)
        mixed = jnp.dot(normed, qkv_weight, preferred_element_type=jnp.float32)
        query = (rotate(mixed[:, :qcols].reshape(SEQ, HEADS, HD), cosine[:, None, :], sine[:, None, :]) * scale).astype(jnp.bfloat16).reshape(SEQ * HEADS, HD)
        key_rows = rotate(mixed[:, qcols:qcols + HD], cosine, sine).astype(jnp.bfloat16)
        value_rows = mixed[:, qcols + HD:].astype(jnp.bfloat16)
        grad_flat = grad_attn.reshape(SEQ * HEADS, HD)
        scores = jnp.dot(query, key_rows.T, preferred_element_type=jnp.float32)
        scores = jnp.where(allowed, scores, -1e+30)
        row_top = lax.optimization_barrier(jnp.max(scores, axis=1))
        row_total = lax.optimization_barrier(jnp.sum(jnp.where(allowed, jnp.exp(scores - row_top[:, None]), 0.0), axis=1))
        log_total = row_top + jnp.log(row_total)
        probs = jnp.where(allowed, jnp.exp(scores - log_total[:, None]), 0.0)
        probs_low = probs.astype(jnp.bfloat16)
        attn_flat = jnp.dot(probs, value_rows.astype(jnp.float32), precision=lax.Precision.HIGHEST, preferred_element_type=jnp.float32).astype(jnp.bfloat16)
        row_delta = lax.optimization_barrier(jnp.sum(grad_flat.astype(jnp.float32) * attn_flat.astype(jnp.float32), axis=1))
        grad_probs = jnp.dot(grad_flat, value_rows.T, preferred_element_type=jnp.float32)
        grad_scores = (probs * (grad_probs - row_delta[:, None])).astype(jnp.bfloat16)
        grad_query = jnp.dot(grad_scores, key_rows, preferred_element_type=jnp.float32)
        grad_keys = jnp.dot(grad_scores.T, query, preferred_element_type=jnp.float32)
        grad_values = jnp.dot(probs_low.T, grad_flat, preferred_element_type=jnp.float32)
        query_back = (unrotate(grad_query.reshape(SEQ, HEADS, HD), cosine[:, None, :], sine[:, None, :]) * scale).reshape(SEQ, qcols)
        grad_mixed = jnp.concatenate([query_back, unrotate(grad_keys, cosine, sine), grad_values], axis=1).astype(jnp.bfloat16)
        grad_normed = jnp.dot(grad_mixed, qkv_weight.T, preferred_element_type=jnp.float32)
        inner = lax.optimization_barrier(jnp.sum(grad_normed * gain[None, :] * wide_rows, axis=1, keepdims=True))
        grad_rows = (gain[None, :] * grad_normed * inv_rms - wide_rows * inv_rms ** 3 / D * inner).astype(jnp.bfloat16)
        gain_acc = gain_acc + lax.optimization_barrier(jnp.sum(grad_normed * wide_rows * inv_rms, axis=0))
        term_low = jnp.dot(normed.T, grad_mixed, preferred_element_type=jnp.float32).astype(jnp.bfloat16)
        term_low = lax.optimization_barrier(term_low)
        weight_acc = weight_acc + term_low.astype(jnp.float32)
        return ((weight_acc, gain_acc), (attn_flat.reshape(SEQ, qcols), grad_rows))
    start = (jnp.zeros((D, (HEADS + 2) * HD), jnp.float32), jnp.zeros((D,), jnp.float32))
    (weight_grad, gain_grad), (attn, grad_in) = lax.scan(one_sequence, start, (hidden_in, attn_cotangent))
    return (attn, grad_in, weight_grad, gain_grad)
```

```python
import functools
import jax
import jax.numpy as jnp
import numpy as np
from jax import lax
from jax.experimental import pallas as pl
from jax.experimental.pallas import tpu as pltpu
from jax.sharding import PartitionSpec as P

HD = 128
HEADS = 4


eps_norm = 1e-05
rope_base = 500000.0


def rope_tables(positions, head_size):
    half_size = head_size // 2
    freqs = rope_base ** (-jnp.arange(half_size, dtype=jnp.float32) / half_size)
    angles = positions.astype(jnp.float32)[:, None] * freqs[None, :]
    return (jnp.cos(angles), jnp.sin(angles))


def rotate(values_in, cosine, sine):
    half_size = values_in.shape[-1] // 2
    first, second = (values_in[..., :half_size], values_in[..., half_size:])
    return jnp.concatenate(
        [first * cosine - second * sine, second * cosine + first * sine], axis=-1
    )


def unrotate(grad_out, cosine, sine):
    half_size = grad_out.shape[-1] // 2
    first, second = (grad_out[..., :half_size], grad_out[..., half_size:])
    return jnp.concatenate(
        [first * cosine + second * sine, second * cosine - first * sine], axis=-1
    )


def forward_fold(query_rows, row_pos):

    def forward_advance(carry, piece, start):
        row_top, row_total, weighted = carry
        key_part, value_part = piece
        scores = jnp.einsum("qd,kd->qk", query_rows, key_part, preferred_element_type=jnp.float32)
        key_pos = jnp.arange(key_part.shape[0], dtype=jnp.int32)
        allowed = key_pos[None, :] <= row_pos[:, None]
        scores = jnp.where(allowed, scores, -1e30)
        new_top = jnp.maximum(row_top, jnp.max(scores, axis=1))
        numbers = jnp.where(allowed, jnp.exp(scores - new_top[:, None]), 0.0)
        row_total = jnp.sum(numbers, axis=1)
        weighted = jnp.dot(
            numbers,
            value_part.astype(jnp.float32),
            precision=lax.Precision.HIGHEST,
            preferred_element_type=jnp.float32,
        )
        return (new_top, row_total, weighted)

    return forward_advance


def query_grad_fold(query_rows, row_pos, grad_flat, log_total, row_delta):

    def query_advance(grad_query, piece, start):
        key_part, value_part = piece
        scores = jnp.einsum("qd,kd->qk", query_rows, key_part, preferred_element_type=jnp.float32)
        key_pos = jnp.arange(key_part.shape[0], dtype=jnp.int32)
        allowed = key_pos[None, :] <= row_pos[:, None]
        probs = jnp.where(
            allowed, jnp.exp(jnp.where(allowed, scores, -1e30) - log_total[:, None]), 0.0
        )
        grad_probs = jnp.einsum(
            "qd,kd->qk", grad_flat, value_part, preferred_element_type=jnp.float32
        )
        grad_scores = (probs * (grad_probs - row_delta[:, None])).astype(jnp.bfloat16)
        return jnp.dot(grad_scores, key_part, preferred_element_type=jnp.float32)

    return query_advance


def key_grad_fold(key_rows, value_rows, key_pos, log_all, delta_all, heads_count):

    def key_advance(carry, piece, start):
        query_part, attn_grad_part = piece
        count = query_part.shape[0]
        scores = jnp.einsum("qd,kd->qk", query_part, key_rows, preferred_element_type=jnp.float32)
        query_pos = jnp.arange(count, dtype=jnp.int32) // heads_count
        allowed = key_pos[None, :] <= query_pos[:, None]
        probs = jnp.where(
            allowed, jnp.exp(jnp.where(allowed, scores, -1e30) - log_all[:, None]), 0.0
        )
        grad_values = jnp.einsum(
            "qk,qd->kd",
            probs.astype(jnp.bfloat16),
            attn_grad_part,
            preferred_element_type=jnp.float32,
        )
        grad_probs = jnp.einsum(
            "qd,kd->qk", attn_grad_part, value_rows, preferred_element_type=jnp.float32
        )
        grad_scores = (probs * (grad_probs - delta_all[:, None])).astype(jnp.bfloat16)
        grad_keys = jnp.einsum(
            "qk,qd->kd", grad_scores, query_part, preferred_element_type=jnp.float32
        )
        return (grad_keys, grad_values)

    return key_advance


def local(hidden_in, norm_gain, qkv_weight, attn_cotangent):
    rows_in = hidden_in[0]
    grad_attn = attn_cotangent[0]
    tokens_here = rows_in.shape[0]
    width = rows_in.shape[1]
    head_size = HD
    heads_count = HEADS
    qcols = heads_count * head_size
    scale = head_size ** (-0.5)
    weight_group, gain_group = (
        lax.all_gather(qkv_weight, "intra", axis=0, tiled=True),
        lax.all_gather(norm_gain, "intra", axis=0, tiled=True),
    )
    weight_full, gain_full = (
        lax.all_gather(weight_group, "inter", axis=0, tiled=True),
        lax.all_gather(gain_group, "inter", axis=0, tiled=True),
    )
    query_pos = lax.axis_index("intra") * tokens_here + jnp.arange(tokens_here, dtype=jnp.int32)
    row_pos = jnp.broadcast_to(query_pos[:, None], (tokens_here, heads_count)).reshape(
        tokens_here * heads_count
    )
    cosine, sine = rope_tables(query_pos, head_size)
    wide_rows = rows_in.astype(jnp.float32)
    inv_rms = lax.rsqrt(jnp.mean(wide_rows * wide_rows, axis=1, keepdims=True) + eps_norm)
    normed = (wide_rows * inv_rms * gain_full.astype(jnp.float32)[None, :]).astype(jnp.bfloat16)
    mixed = jnp.dot(normed, weight_full, preferred_element_type=jnp.float32)
    query_rows = (
        (
            rotate(
                mixed[:, :qcols].reshape(tokens_here, heads_count, head_size),
                cosine[:, None, :],
                sine[:, None, :],
            )
            * scale
        )
        .astype(jnp.bfloat16)
        .reshape(tokens_here * heads_count, head_size)
    )
    key_rows = rotate(mixed[:, qcols : qcols + head_size], cosine, sine).astype(jnp.bfloat16)
    value_rows = mixed[:, qcols + head_size :].astype(jnp.bfloat16)
    grad_flat = grad_attn.reshape(tokens_here * heads_count, head_size)
    flat_rows = tokens_here * heads_count
    forward_step = forward_fold(query_rows, row_pos)
    start_carry = (
        jnp.full((flat_rows,), -1e30, jnp.float32),
        jnp.zeros((flat_rows,), jnp.float32),
        jnp.zeros((flat_rows, head_size), jnp.float32),
    )
    row_top, row_total, weighted = forward_step(
        start_carry,
        (
            lax.all_gather(key_rows, "intra", axis=0, tiled=True),
            lax.all_gather(value_rows, "intra", axis=0, tiled=True),
        ),
        jnp.int32(0),
    )
    attn_flat = (weighted / row_total[:, None]).astype(jnp.bfloat16)
    log_total = row_top + jnp.log(row_total)
    row_delta = jnp.sum(grad_flat.astype(jnp.float32) * attn_flat.astype(jnp.float32), axis=1)
    query_step = query_grad_fold(query_rows, row_pos, grad_flat, log_total, row_delta)
    grad_query = query_step(
        jnp.zeros((flat_rows, head_size), jnp.float32),
        (
            lax.all_gather(key_rows, "intra", axis=0, tiled=True),
            lax.all_gather(value_rows, "intra", axis=0, tiled=True),
        ),
        jnp.int32(0),
    )
    log_all, delta_all = (
        lax.all_gather(log_total, "intra", axis=0, tiled=True),
        lax.all_gather(row_delta, "intra", axis=0, tiled=True),
    )
    key_step = key_grad_fold(key_rows, value_rows, query_pos, log_all, delta_all, heads_count)
    grad_keys, grad_values = key_step(
        (
            jnp.zeros((tokens_here, head_size), jnp.float32),
            jnp.zeros((tokens_here, head_size), jnp.float32),
        ),
        (
            lax.all_gather(query_rows, "intra", axis=0, tiled=True),
            lax.all_gather(grad_flat, "intra", axis=0, tiled=True),
        ),
        jnp.int32(0),
    )
    query_back = (
        unrotate(
            grad_query.reshape(tokens_here, heads_count, head_size),
            cosine[:, None, :],
            sine[:, None, :],
        )
        * scale
    ).reshape(tokens_here, qcols)
    grad_mixed = jnp.concatenate(
        [query_back, unrotate(grad_keys, cosine, sine), grad_values], axis=1
    ).astype(jnp.bfloat16)
    weight_back, gain_back = (weight_full, gain_full)
    gain_wide = gain_back.astype(jnp.float32)[None, :]
    grad_normed = jnp.einsum(
        "tc,dc->td", grad_mixed, weight_back, preferred_element_type=jnp.float32
    )
    inner = jnp.sum(grad_normed * gain_wide * wide_rows, axis=1, keepdims=True)
    grad_rows = (
        gain_wide * grad_normed * inv_rms - wide_rows * inv_rms**3 / width * inner
    ).astype(jnp.bfloat16)
    gain_term = jnp.sum(grad_normed * wide_rows * inv_rms, axis=0)
    normed_cols = lax.all_to_all(normed, "intra", split_axis=1, concat_axis=0, tiled=True)
    group_term = lax.dot_general(
        normed_cols,
        lax.all_gather(grad_mixed, "intra", axis=0, tiled=True),
        (((0,), (0,)), ((), ())),
        preferred_element_type=jnp.float32,
    )
    term_low = lax.optimization_barrier(group_term.astype(jnp.bfloat16))
    gain_sums = lax.psum_scatter(gain_term, "intra", scatter_dimension=0, tiled=True)
    weight_grad, gain_grad = (
        lax.psum_scatter(term_low.astype(jnp.float32), "inter", scatter_dimension=0, tiled=True),
        lax.psum_scatter(gain_sums, "inter", scatter_dimension=0, tiled=True),
    )
    return (attn_flat.reshape(tokens_here, qcols)[None], grad_rows[None], weight_grad, gain_grad)

MESH = pl.DeviceIdType.MESH
CORES = 2
SIDE = 2
PIECES = 4
CHUNK = 2 * HD


def nt_dot(a, b):
    return lax.dot_general(a, b, (((1,), (1,)), ((), ())), preferred_element_type=jnp.float32)


def tn_dot(a, b):
    return lax.dot_general(a, b, (((0,), (0,)), ((), ())), preferred_element_type=jnp.float32)


def nn_dot(a, b):
    return jnp.dot(a, b, preferred_element_type=jnp.float32)


def fused_kernel(
    n_inter,
    hid_ref, gain_ref, w_ref, ct_ref, cos_hbm, sin_hbm,
    attn_ref, gin_ref, wg_ref, gg_ref,
    wbuf, gbuf, gain_in, hx, hs, nbuf, ntr, inv_all, inv_s, inv_r, ctb, cts, cos_ref, sin_ref,
    mix, kv_s, kv_r, qm_s, qm_r, gq, gkv_s, gkv_r, gkv, in_s, in_r, at_s, at_r, gi_s, gi_r,
    tbuf, rs1, ybuf, rs2, zbuf, rs3, dg_s, dg_r, gg_s, gg_r,
    ld_sem, ag_send, ag_recv, g_send, g_recv, x_send, x_recv,
    c_send, c_recv, y_send, y_recv, z_send, z_recv, d_send, d_recv,
):
    i = lax.axis_index("inter")
    x = lax.axis_index("intra")
    nz = n_inter // (CORES * SIDE)
    c = lax.rem(i, CORES)
    y = lax.rem(i // CORES, SIDE)
    z = i // (CORES * SIDE)
    toks, width = hid_ref.shape
    rows, cols = w_ref.shape
    seq = 2 * toks
    qcols = HEADS * HD
    chips = nz * SIDE
    chunks = cols // CHUNK
    span = n_inter // PIECES
    lanes = span * rows
    scale = HD ** (-0.5)
    f32, bf = jnp.float32, jnp.bfloat16

    def dev(zz, yy, cc, xx):
        return ((zz * SIDE + yy) * CORES + cc, xx)

    def slot(zz, yy, cc):
        return (zz * SIDE + yy) * CORES + cc

    def across(d):
        zz, bit = z, 1
        while bit < nz:
            if d & bit:
                zz = zz + bit - 2 * bit * lax.rem(z // bit, 2)
            bit *= 2
        return zz

    hops = list(range(1, nz))
    x_peer = dev(z, y, c, 1 - x)
    y_peer = dev(z, 1 - y, c, x)
    c_peer = dev(z, y, 1 - c, x)
    d_peer = dev(z, y, 1 - c, 1 - x)
    plane = [(d, yy, cc) for d in range(nz) for yy in (0, 1) for cc in (0, 1) if d or yy or cc]

    def plane_dev(e):
        d, yy, cc = e
        return (across(d), y + yy - 2 * yy * y, c + cc - 2 * cc * c)

    own = slot(z, y, c)
    here = pl.ds(pl.multiple_of(x * toks, toks), toks)
    there = pl.ds(pl.multiple_of((1 - x) * toks, toks), toks)

    def rcopy(src, dst, ss, rs, device):
        return pltpu.make_async_remote_copy(
            src_ref=src, dst_ref=dst, send_sem=ss, recv_sem=rs, device_id=device, device_id_type=MESH
        )

    barrier = pltpu.get_barrier_semaphore()
    peers = [dev(*plane_dev(e), x) for e in plane] + [x_peer, d_peer]
    for peer in peers:
        pl.semaphore_signal(barrier, inc=1, device_id=peer, device_id_type=MESH)

    def load(src, dst, k):
        pltpu.make_async_copy(src, dst, ld_sem.at[k]).start()

    def loaded(dst, k):
        pltpu.make_async_copy(dst, dst, ld_sem.at[k]).wait()

    for p in range(PIECES):
        for b in range(span):
            j = p * span + b
            mine = pl.ds(pl.multiple_of((2 * j + x) * rows, rows), rows)
            other = pl.ds(pl.multiple_of((2 * j + 1 - x) * rows, rows), rows)
            load(hid_ref.at[:, mine], hx.at[p, here, b * rows : (b + 1) * rows], 0)
            load(hid_ref.at[:, other], hs.at[p, :, b * rows : (b + 1) * rows], 1)
    load(w_ref.at[:, qcols:], wbuf.at[0, own], 2)
    half = HEADS // 2
    for n in range(half):
        for xx in range(2):
            first = (xx * half + n) * HD
            load(w_ref.at[:, first : first + HD], wbuf.at[1 + n, own, :, xx * HD : (xx + 1) * HD], 3 + n)
    nxt = 3 + half
    load(gain_ref, gain_in, nxt)
    load(ct_ref.at[:, pl.ds(pl.multiple_of(x * half * HD, HD), half * HD)], ctb.at[here], nxt + 1)
    load(ct_ref.at[:, pl.ds(pl.multiple_of((1 - x) * half * HD, HD), half * HD)], cts, nxt + 2)
    load(cos_hbm, cos_ref, nxt + 3)
    load(sin_hbm, sin_ref, nxt + 4)

    loaded(gain_in, nxt)
    gcol = lambda g: pl.ds(pl.multiple_of(g * rows, rows), rows)
    gbuf[:, gcol(own)] = gain_in[...].astype(f32)
    loaded(hx.at[:, here], 0)
    loaded(hs, 1)
    total = jnp.zeros((toks, 1), f32)
    for p in range(PIECES):
        a = hx[p, here, :].astype(f32)
        b = hs[p].astype(f32)
        total = total + jnp.sum(a * a + b * b, axis=1, keepdims=True)
    inv = jnp.broadcast_to(lax.rsqrt(total / width + eps_norm), (toks, HD))
    inv_all[here, :] = inv
    inv_s[...] = inv.T[:8, :]
    for q in range(chunks):
        loaded(wbuf.at[q, own], 2 + q)
    loaded(cts, nxt + 2)
    pl.semaphore_wait(barrier, len(peers))

    def ag(q, g, link, device):
        return rcopy(wbuf.at[q, g], wbuf.at[q, g], ag_send.at[q, link], ag_recv.at[q, g], device)

    def arrive(q, g):
        ag(q, g, 0, x_peer).wait_recv()

    def x_copy(k, src, dst):
        return rcopy(src, dst, x_send.at[k], x_recv.at[k], x_peer)

    n_links = 3 * nz + chips
    y_link = nz
    c_link = 2 * nz
    sent = []

    def push(q, g, link, device):
        cp = ag(q, g, link, device)
        cp.start()
        sent.append(cp)

    for q in range(chunks):
        for d in hops:
            push(q, own, d, dev(across(d), y, c, x))
        push(q, own, y_link, y_peer)
        push(q, own, c_link, c_peer)
        if q == 0:
            for n, e in enumerate(plane):
                rcopy(gbuf.at[:, gcol(own)], gbuf.at[:, gcol(own)], g_send.at[n], g_recv.at[own],
                      dev(*plane_dev(e), x)).start()
    messages = []

    def x_push(src, dst):
        cp = x_copy(len(messages), src, dst)
        cp.start()
        messages.append(cp)
        return cp

    inv_msg = x_push(inv_s, inv_r)
    hid_msg = [x_push(hs.at[p], hx.at[p, here]) for p in range(PIECES)]
    ct_msg = x_push(cts, ctb.at[here])

    def z_arrivals(q):
        for d in hops:
            g = slot(across(d), y, c)
            arrive(q, g)
            push(q, g, y_link + d, y_peer)
            push(q, g, c_link + d, c_peer)

    def y_arrival(q, d):
        g = slot(across(d), 1 - y, c)
        arrive(q, g)
        push(q, g, c_link + nz + d, c_peer)

    def c_arrivals(q):
        for d in range(nz):
            for yy in (y, 1 - y):
                arrive(q, slot(across(d), yy, 1 - c))

    def norm(which):
        scaled = inv_all[which, :1]
        for p in range(PIECES):
            value = hx[p, which, :].astype(f32) * scaled * gbuf[:, p * lanes : (p + 1) * lanes]
            value = value.astype(bf)
            nbuf[p, which, :] = value
            ntr[p * lanes : (p + 1) * lanes, which] = value.T

    def partial(q):
        out = jnp.zeros((seq, CHUNK), f32)
        for p in range(PIECES):
            w = wbuf[q, p * span : (p + 1) * span].reshape(lanes, CHUNK)
            out = out + nn_dot(nbuf[p], w)
        mix[q] = out

    mycol = pl.ds(pl.multiple_of(x * HD, HD), HD)
    itscol = pl.ds(pl.multiple_of((1 - x) * HD, HD), HD)

    z_arrivals(0)
    for q in range(chunks):
        y_arrival(q, 0)
    for n, e in enumerate(plane):
        g = slot(*plane_dev(e))
        rcopy(gbuf.at[:, gcol(g)], gbuf.at[:, gcol(g)], g_send.at[n], g_recv.at[g], x_peer).wait_recv()
    norm(here)
    z_arrivals(1)
    for d in hops:
        y_arrival(0, d)
    inv_msg.wait_recv()
    for cp in hid_msg:
        cp.wait_recv()
    inv_all[there, :] = jnp.broadcast_to(inv_r[:1, :], (toks, toks)).T
    norm(there)
    c_arrivals(0)
    partial(0)
    kv_s[...] = mix[0].astype(bf)
    kv_msg = x_push(kv_s, kv_r)
    z_arrivals(2)
    q_msg = []
    for n in range(half):
        for d in hops:
            y_arrival(1 + n, d)
        c_arrivals(1 + n)
        partial(1 + n)
        qm_s[n] = mix[1 + n, :, itscol].astype(bf)
        q_msg.append(x_push(qm_s.at[n], qm_r.at[n]))

    loaded(cos_ref, nxt + 3)
    loaded(sin_ref, nxt + 4)
    loaded(ctb.at[here], nxt + 1)
    ct_msg.wait_recv()
    cosine, sine = cos_ref[...], sin_ref[...]

    def rope(u):
        return u * cosine + pltpu.roll(u, HD // 2, 1) * sine

    def unrope(u):
        return u * cosine - pltpu.roll(u, HD // 2, 1) * sine

    kv_msg.wait_recv()
    mix_kv = mix[0] + kv_r[...].astype(f32)
    mix[0] = mix_kv
    keys = rope(mix_kv[:, :HD]).astype(bf)
    values = mix_kv[:, HD:].astype(bf)
    allowed = lax.broadcasted_iota(jnp.int32, (seq, seq), 1) <= lax.broadcasted_iota(jnp.int32, (seq, seq), 0)
    inner = jnp.zeros((seq, 1), f32)
    grad_keys = jnp.zeros((seq, HD), f32)
    grad_values = jnp.zeros((seq, HD), f32)
    gq_msg = []
    for n in range(half):
        q_msg[n].wait_recv()
        mixed = mix[1 + n, :, mycol] + qm_r[n].astype(f32)
        query = (rope(mixed) * scale).astype(bf)
        grad = ctb[:, n * HD : (n + 1) * HD]
        scores = jnp.where(allowed, nt_dot(query, keys), -1e30)
        top = jnp.max(scores, axis=1, keepdims=True)
        numbers = jnp.where(allowed, jnp.exp(scores - top), 0.0)
        norm_sum = jnp.sum(numbers, axis=1, keepdims=True)
        high = numbers.astype(bf)
        low = (numbers - high.astype(f32)).astype(bf)
        attn = ((nn_dot(high, values) + nn_dot(low, values)) / norm_sum).astype(bf)
        at_s[n] = attn
        delta = jnp.sum(grad.astype(f32) * attn.astype(f32), axis=1, keepdims=True)
        probs = numbers / norm_sum
        grad_scores = (probs * (nt_dot(grad, values) - delta)).astype(bf)
        back = (unrope(nn_dot(grad_scores, keys)) * scale).astype(bf)
        gq[n, x] = back
        gq_msg.append(x_push(gq.at[n, x], gq.at[n, x]))
        inner = inner + jnp.sum(back.astype(f32) * mixed, axis=1, keepdims=True)
        grad_keys = grad_keys + tn_dot(grad_scores, query)
        grad_values = grad_values + tn_dot(probs.astype(bf), grad)
    grad_keys = unrope(grad_keys)
    gkv_s[:, :HD] = grad_keys.astype(bf)
    gkv_s[:, HD:] = grad_values.astype(bf)
    gkv_msg = x_push(gkv_s, gkv_r)
    inner_all = jnp.broadcast_to(inner, (seq, HD))
    in_s[...] = inner_all.T[:8, :]
    in_msg = x_push(in_s, in_r)
    for n in range(half):
        attn_ref[:, pl.ds(pl.multiple_of((x * half + n) * HD, HD), HD)] = at_s[n, here, :]

    def to_core(q, k):
        return rcopy(tbuf.at[q, (1 - c) * chips + k], rs1.at[q, k], c_send.at[q, k], c_recv.at[q, k], c_peer)

    def to_y(q, d):
        return rcopy(ybuf.at[q, d], rs2.at[q, d], y_send.at[q, d], y_recv.at[q, d], y_peer)

    def to_z(q, d):
        return rcopy(zbuf.at[q, d - 1], rs3.at[q, d - 1], z_send.at[q, d - 1], z_recv.at[q, d - 1],
                     dev(across(d), y, c, x))

    order = hops[::-1] + [0]

    def term(q, grads, j):
        part = nn_dot(ntr[pl.ds(pl.multiple_of(j * rows, rows), rows), :], grads)
        tbuf[q, j] = part.astype(bf)

    def core_sum(q, k):
        to_core(q, k).wait_recv()
        return tbuf[q, c * chips + k].astype(f32) + rs1[q, k].astype(f32)

    def rs_start(q, grads):
        for yy in (1 - y, y):
            for d in order:
                k = across(d) * SIDE + yy
                term(q, grads, (1 - c) * chips + k)
                to_core(q, k).start()
                term(q, grads, c * chips + k)
        for d in order:
            ybuf[q, d] = core_sum(q, across(d) * SIDE + 1 - y).astype(bf)
            to_y(q, d).start()

    def rs_middle(q):
        for d in order:
            part = core_sum(q, across(d) * SIDE + y)
            to_y(q, d).wait_recv()
            part = part + rs2[q, d].astype(f32)
            if d:
                zbuf[q, d - 1] = part.astype(bf)
                to_z(q, d).start()
            else:
                mix[q, :rows, :] = part

    block = c * chips + z * SIDE + y
    cross = c != x
    sums = []

    def rs_end(q):
        result = mix[q, :rows, :]
        for d in order[:-1]:
            to_z(q, d).wait_recv()
            result = result + rs3[q, d - 1].astype(f32)
        prod = wbuf[q, block].astype(f32) * result
        sums.append(prod[:, :HD] + prod[:, HD:])
        dg_s[q] = result.astype(bf)
        pl.when(cross)(lambda: to_diag(q).start())
        store(q, result)

    def store(q, result):
        if q == 0:
            wg_ref[:, qcols:] = result
        else:
            for xx in range(2):
                first = (xx * half + q - 1) * HD
                wg_ref[:, first : first + HD] = result[:, xx * HD : (xx + 1) * HD]

    def to_diag(q):
        return rcopy(dg_s.at[q], dg_r.at[q], d_send.at[q], d_recv.at[q], d_peer)

    gg_copy = rcopy(gg_s, gg_r, d_send.at[chunks], d_recv.at[chunks], d_peer)

    for n in range(half):
        gq_msg[n].wait_recv()
        rs_start(1 + n, jnp.concatenate([gq[n, 0], gq[n, 1]], axis=1))
    gkv_msg.wait_recv()
    keys_sum = gkv_s[:, :HD].astype(f32) + gkv_r[:, :HD].astype(f32)
    values_sum = gkv_s[:, HD:].astype(f32) + gkv_r[:, HD:].astype(f32)
    gkv_all = jnp.concatenate([keys_sum, values_sum], axis=1).astype(bf)
    gkv[...] = gkv_all
    rs_start(0, gkv_all)
    in_msg.wait_recv()
    inner = inner + jnp.broadcast_to(in_r[:1, :], (HD, seq)).T[:, :1]
    inner = inner + jnp.sum(gkv_all.astype(f32) * mix[0], axis=1, keepdims=True)
    inv = inv_all[...]
    inv_all[...] = inner * (inv * inv / width)
    ntr_inv = inv

    def grad_piece(p, which, scaled):
        out = jnp.zeros((toks, lanes), f32)
        for q in range(chunks):
            w = wbuf[q, p * span : (p + 1) * span].reshape(lanes, CHUNK)
            g = gkv[which, :] if q == 0 else jnp.concatenate([gq[q - 1, 0, which, :], gq[q - 1, 1, which, :]], axis=1)
            out = out + nt_dot(g, w)
        gain = gbuf[:, p * lanes : (p + 1) * lanes]
        return (gain * out * scaled - hx[p, which, :].astype(f32) * inv_all[which, :1]).astype(bf)

    mix[1, :, :HD] = ntr_inv
    gi_msg = []
    for p in range(PIECES):
        gi_s[p] = grad_piece(p, there, mix[1, there, :1])
        gi_msg.append(x_push(gi_s.at[p], gi_r.at[p]))
    at_msg = x_push(at_s.at[:, there], at_r)
    for p in range(PIECES):
        value = grad_piece(p, here, mix[1, here, :1])
        for b in range(span):
            j = p * span + b
            gin_ref[:, pl.ds(pl.multiple_of((2 * j + x) * rows, rows), rows)] = value[:, b * rows : (b + 1) * rows]

    queue = list(range(1, chunks)) + [0]
    rs_middle(queue[0])
    for n in range(1, chunks):
        rs_middle(queue[n])
        rs_end(queue[n - 1])
    rs_end(queue[-1])
    lanes_sum = sums[0]
    for part in sums[1:]:
        lanes_sum = lanes_sum + part
    gg = jnp.sum(lanes_sum.T, axis=0, keepdims=True) / gbuf[:, gcol(block)]
    gg_ref[...] = gg
    gg_s[...] = gg
    pl.when(cross)(lambda: gg_copy.start())

    at_msg.wait_recv()
    for n in range(half):
        attn_ref[:, pl.ds(pl.multiple_of(((1 - x) * half + n) * HD, HD), HD)] = at_r[n]
    for p in range(PIECES):
        gi_msg[p].wait_recv()
        for b in range(span):
            j = p * span + b
            gin_ref[:, pl.ds(pl.multiple_of((2 * j + 1 - x) * rows, rows), rows)] = gi_r[p, :, b * rows : (b + 1) * rows]

    for cp in sent + messages:
        cp.wait_send()
    for n, e in enumerate(plane):
        rcopy(gbuf.at[:, gcol(own)], gbuf.at[:, gcol(own)], g_send.at[n], g_recv.at[own], x_peer).wait_send()
    for q in range(chunks):
        for k in range(chips):
            to_core(q, k).wait_send()
        for d in range(nz):
            to_y(q, d).wait_send()
        for d in hops:
            to_z(q, d).wait_send()

    @pl.when(cross)
    def _():
        for q in queue:
            to_diag(q).wait_recv()
            store(q, dg_r[q].astype(f32))
        gg_copy.wait_recv()
        gg_ref[...] = gg_r[...]
        for q in range(chunks):
            to_diag(q).wait_send()
        gg_copy.wait_send()


def copy_kernel(*refs):
    for k in range(4):
        refs[4 + k][...] = refs[k][...]


def fused(n_inter, hidden_in, norm_gain, qkv_weight, attn_cotangent):
    toks, width = hidden_in.shape[1:]
    rows, cols = qkv_weight.shape
    nz = n_inter // (CORES * SIDE)
    chips = nz * SIDE
    seq, half, chunks = 2 * toks, HEADS // 2, cols // CHUNK
    lanes = n_inter // PIECES * rows
    freqs = rope_base ** (-np.arange(HD // 2, dtype=np.float32) / np.float32(HD // 2))
    angles = (np.arange(seq, dtype=np.float32)[:, None] * freqs.astype(np.float32)[None, :]).astype(np.float32)
    cosine = np.concatenate([np.cos(angles)] * 2, axis=1).astype(np.float32)
    sine = np.concatenate([-np.sin(angles), np.sin(angles)], axis=1).astype(np.float32)
    bf, f32, dma = jnp.bfloat16, jnp.float32, pltpu.SemaphoreType.DMA
    vmem = pl.BlockSpec(memory_space=pltpu.VMEM)
    hbm = pl.BlockSpec(memory_space=pltpu.HBM)
    V = pltpu.VMEM
    n_msgs = 2 * PIECES + 2 * half + 6
    attn, gin, wg, gg = pl.pallas_call(
        functools.partial(fused_kernel, n_inter),
        out_shape=(
            jax.ShapeDtypeStruct((toks, HEADS * HD), bf),
            jax.ShapeDtypeStruct((toks, width), bf),
            jax.ShapeDtypeStruct((rows, cols), f32),
            jax.ShapeDtypeStruct((1, rows), f32),
        ),
        in_specs=[hbm] * 6,
        out_specs=(vmem,) * 4,
        scratch_shapes=[
            V((chunks, n_inter, rows, CHUNK), bf),
            V((1, n_inter * rows), f32),
            V((1, rows), bf),
            V((PIECES, seq, lanes), bf),
            V((PIECES, toks, lanes), bf),
            V((PIECES, seq, lanes), bf),
            V((n_inter * rows, seq), bf),
            V((seq, HD), f32),
            V((8, toks), f32),
            V((8, toks), f32),
            V((seq, half * HD), bf),
            V((toks, half * HD), bf),
            V((seq, HD), f32),
            V((seq, HD), f32),
            V((chunks, seq, CHUNK), f32),
            V((seq, CHUNK), bf),
            V((seq, CHUNK), bf),
            V((half, seq, HD), bf),
            V((half, seq, HD), bf),
            V((half, 2, seq, HD), bf),
            V((seq, CHUNK), bf),
            V((seq, CHUNK), bf),
            V((seq, CHUNK), bf),
            V((8, seq), f32),
            V((8, seq), f32),
            V((half, seq, HD), bf),
            V((half, toks, HD), bf),
            V((PIECES, toks, lanes), bf),
            V((PIECES, toks, lanes), bf),
            V((chunks, n_inter, rows, CHUNK), bf),
            V((chunks, chips, rows, CHUNK), bf),
            V((chunks, nz, rows, CHUNK), bf),
            V((chunks, nz, rows, CHUNK), bf),
            V((chunks, nz - 1, rows, CHUNK), bf),
            V((chunks, nz - 1, rows, CHUNK), bf),
            V((chunks, rows, CHUNK), bf),
            V((chunks, rows, CHUNK), bf),
            V((1, rows), f32),
            V((1, rows), f32),
            dma((8 + half,)),
            dma((chunks, 2 * nz + chips)), dma((chunks, n_inter)),
            dma((n_inter,)), dma((n_inter,)),
            dma((n_msgs,)), dma((n_msgs,)),
            dma((chunks, chips)), dma((chunks, chips)),
            dma((chunks, nz)), dma((chunks, nz)),
            dma((chunks, nz - 1)), dma((chunks, nz - 1)),
            dma((chunks + 1,)), dma((chunks + 1,)),
        ],
        compiler_params=pltpu.CompilerParams(
            collective_id=0, has_side_effects=True, vmem_limit_bytes=32 * 2**20
        ),
    )(hidden_in[0], norm_gain[None], qkv_weight, attn_cotangent[0], cosine, sine)
    outs = (attn, gin, wg, gg)
    attn, gin, wg, gg = pl.pallas_call(
        copy_kernel,
        out_shape=tuple(jax.ShapeDtypeStruct(o.shape, o.dtype) for o in outs),
        in_specs=[vmem] * 4,
        out_specs=(vmem,) * 4,
    )(*outs)
    return attn[None], gin[None], wg, gg[0]


def solution(mesh):
    n_inter, n_intra = mesh.shape["inter"], mesh.shape["intra"]

    def body(hidden_in, norm_gain, qkv_weight, attn_cotangent):
        nz = n_inter // (CORES * SIDE)
        fits = n_intra == 2 and n_inter % (CORES * SIDE) == 0 and nz > 1 and nz & (nz - 1) == 0
        fits = fits and qkv_weight.shape[0] == HD and hidden_in.shape[0] == 1
        fits = fits and hidden_in.shape[1] == HD and n_inter % PIECES == 0
        if fits:
            return fused(n_inter, hidden_in, norm_gain, qkv_weight, attn_cotangent)
        return local(hidden_in, norm_gain, qkv_weight, attn_cotangent)

    return jax.shard_map(
        body,
        mesh=mesh,
        in_specs=(
            P("inter", "intra", None),
            P(("inter", "intra")),
            P(("inter", "intra"), None),
            P("inter", "intra", None),
        ),
        out_specs=(
            P("inter", "intra", None),
            P("inter", "intra", None),
            P(("intra", "inter"), None),
            P(("intra", "inter")),
        ),
        check_vma=False,
    )
```

```python
import functools
import jax
import jax.numpy as jnp
import numpy as np
from jax import lax
from jax.experimental import pallas as pl
from jax.experimental.pallas import tpu as pltpu
from jax.sharding import PartitionSpec as P

HD = 128
HEADS = 4


eps_norm = 1e-05
rope_base = 500000.0


def rope_tables(positions, head_size):
    half_size = head_size // 2
    freqs = rope_base ** (-jnp.arange(half_size, dtype=jnp.float32) / half_size)
    angles = positions.astype(jnp.float32)[:, None] * freqs[None, :]
    return (jnp.cos(angles), jnp.sin(angles))


def rotate(values_in, cosine, sine):
    half_size = values_in.shape[-1] // 2
    first, second = (values_in[..., :half_size], values_in[..., half_size:])
    return jnp.concatenate(
        [first * cosine - second * sine, second * cosine + first * sine], axis=-1
    )


def unrotate(grad_out, cosine, sine):
    half_size = grad_out.shape[-1] // 2
    first, second = (grad_out[..., :half_size], grad_out[..., half_size:])
    return jnp.concatenate(
        [first * cosine + second * sine, second * cosine - first * sine], axis=-1
    )


def forward_fold(query_rows, row_pos):

    def forward_advance(carry, piece, start):
        row_top, row_total, weighted = carry
        key_part, value_part = piece
        scores = jnp.einsum("qd,kd->qk", query_rows, key_part, preferred_element_type=jnp.float32)
        key_pos = jnp.arange(key_part.shape[0], dtype=jnp.int32)
        allowed = key_pos[None, :] <= row_pos[:, None]
        scores = jnp.where(allowed, scores, -1e30)
        new_top = jnp.maximum(row_top, jnp.max(scores, axis=1))
        numbers = jnp.where(allowed, jnp.exp(scores - new_top[:, None]), 0.0)
        row_total = jnp.sum(numbers, axis=1)
        weighted = jnp.dot(
            numbers,
            value_part.astype(jnp.float32),
            precision=lax.Precision.HIGHEST,
            preferred_element_type=jnp.float32,
        )
        return (new_top, row_total, weighted)

    return forward_advance


def query_grad_fold(query_rows, row_pos, grad_flat, log_total, row_delta):

    def query_advance(grad_query, piece, start):
        key_part, value_part = piece
        scores = jnp.einsum("qd,kd->qk", query_rows, key_part, preferred_element_type=jnp.float32)
        key_pos = jnp.arange(key_part.shape[0], dtype=jnp.int32)
        allowed = key_pos[None, :] <= row_pos[:, None]
        probs = jnp.where(
            allowed, jnp.exp(jnp.where(allowed, scores, -1e30) - log_total[:, None]), 0.0
        )
        grad_probs = jnp.einsum(
            "qd,kd->qk", grad_flat, value_part, preferred_element_type=jnp.float32
        )
        grad_scores = (probs * (grad_probs - row_delta[:, None])).astype(jnp.bfloat16)
        return jnp.dot(grad_scores, key_part, preferred_element_type=jnp.float32)

    return query_advance


def key_grad_fold(key_rows, value_rows, key_pos, log_all, delta_all, heads_count):

    def key_advance(carry, piece, start):
        query_part, attn_grad_part = piece
        count = query_part.shape[0]
        scores = jnp.einsum("qd,kd->qk", query_part, key_rows, preferred_element_type=jnp.float32)
        query_pos = jnp.arange(count, dtype=jnp.int32) // heads_count
        allowed = key_pos[None, :] <= query_pos[:, None]
        probs = jnp.where(
            allowed, jnp.exp(jnp.where(allowed, scores, -1e30) - log_all[:, None]), 0.0
        )
        grad_values = jnp.einsum(
            "qk,qd->kd",
            probs.astype(jnp.bfloat16),
            attn_grad_part,
            preferred_element_type=jnp.float32,
        )
        grad_probs = jnp.einsum(
            "qd,kd->qk", attn_grad_part, value_rows, preferred_element_type=jnp.float32
        )
        grad_scores = (probs * (grad_probs - delta_all[:, None])).astype(jnp.bfloat16)
        grad_keys = jnp.einsum(
            "qk,qd->kd", grad_scores, query_part, preferred_element_type=jnp.float32
        )
        return (grad_keys, grad_values)

    return key_advance


def local(hidden_in, norm_gain, qkv_weight, attn_cotangent):
    rows_in = hidden_in[0]
    grad_attn = attn_cotangent[0]
    tokens_here = rows_in.shape[0]
    width = rows_in.shape[1]
    head_size = HD
    heads_count = HEADS
    qcols = heads_count * head_size
    scale = head_size ** (-0.5)
    weight_group, gain_group = (
        lax.all_gather(qkv_weight, "intra", axis=0, tiled=True),
        lax.all_gather(norm_gain, "intra", axis=0, tiled=True),
    )
    weight_full, gain_full = (
        lax.all_gather(weight_group, "inter", axis=0, tiled=True),
        lax.all_gather(gain_group, "inter", axis=0, tiled=True),
    )
    query_pos = lax.axis_index("intra") * tokens_here + jnp.arange(tokens_here, dtype=jnp.int32)
    row_pos = jnp.broadcast_to(query_pos[:, None], (tokens_here, heads_count)).reshape(
        tokens_here * heads_count
    )
    cosine, sine = rope_tables(query_pos, head_size)
    wide_rows = rows_in.astype(jnp.float32)
    inv_rms = lax.rsqrt(jnp.mean(wide_rows * wide_rows, axis=1, keepdims=True) + eps_norm)
    normed = (wide_rows * inv_rms * gain_full.astype(jnp.float32)[None, :]).astype(jnp.bfloat16)
    mixed = jnp.dot(normed, weight_full, preferred_element_type=jnp.float32)
    query_rows = (
        (
            rotate(
                mixed[:, :qcols].reshape(tokens_here, heads_count, head_size),
                cosine[:, None, :],
                sine[:, None, :],
            )
            * scale
        )
        .astype(jnp.bfloat16)
        .reshape(tokens_here * heads_count, head_size)
    )
    key_rows = rotate(mixed[:, qcols : qcols + head_size], cosine, sine).astype(jnp.bfloat16)
    value_rows = mixed[:, qcols + head_size :].astype(jnp.bfloat16)
    grad_flat = grad_attn.reshape(tokens_here * heads_count, head_size)
    flat_rows = tokens_here * heads_count
    forward_step = forward_fold(query_rows, row_pos)
    start_carry = (
        jnp.full((flat_rows,), -1e30, jnp.float32),
        jnp.zeros((flat_rows,), jnp.float32),
        jnp.zeros((flat_rows, head_size), jnp.float32),
    )
    row_top, row_total, weighted = forward_step(
        start_carry,
        (
            lax.all_gather(key_rows, "intra", axis=0, tiled=True),
            lax.all_gather(value_rows, "intra", axis=0, tiled=True),
        ),
        jnp.int32(0),
    )
    attn_flat = (weighted / row_total[:, None]).astype(jnp.bfloat16)
    log_total = row_top + jnp.log(row_total)
    row_delta = jnp.sum(grad_flat.astype(jnp.float32) * attn_flat.astype(jnp.float32), axis=1)
    query_step = query_grad_fold(query_rows, row_pos, grad_flat, log_total, row_delta)
    grad_query = query_step(
        jnp.zeros((flat_rows, head_size), jnp.float32),
        (
            lax.all_gather(key_rows, "intra", axis=0, tiled=True),
            lax.all_gather(value_rows, "intra", axis=0, tiled=True),
        ),
        jnp.int32(0),
    )
    log_all, delta_all = (
        lax.all_gather(log_total, "intra", axis=0, tiled=True),
        lax.all_gather(row_delta, "intra", axis=0, tiled=True),
    )
    key_step = key_grad_fold(key_rows, value_rows, query_pos, log_all, delta_all, heads_count)
    grad_keys, grad_values = key_step(
        (
            jnp.zeros((tokens_here, head_size), jnp.float32),
            jnp.zeros((tokens_here, head_size), jnp.float32),
        ),
        (
            lax.all_gather(query_rows, "intra", axis=0, tiled=True),
            lax.all_gather(grad_flat, "intra", axis=0, tiled=True),
        ),
        jnp.int32(0),
    )
    query_back = (
        unrotate(
            grad_query.reshape(tokens_here, heads_count, head_size),
            cosine[:, None, :],
            sine[:, None, :],
        )
        * scale
    ).reshape(tokens_here, qcols)
    grad_mixed = jnp.concatenate(
        [query_back, unrotate(grad_keys, cosine, sine), grad_values], axis=1
    ).astype(jnp.bfloat16)
    weight_back, gain_back = (weight_full, gain_full)
    gain_wide = gain_back.astype(jnp.float32)[None, :]
    grad_normed = jnp.einsum(
        "tc,dc->td", grad_mixed, weight_back, preferred_element_type=jnp.float32
    )
    inner = jnp.sum(grad_normed * gain_wide * wide_rows, axis=1, keepdims=True)
    grad_rows = (
        gain_wide * grad_normed * inv_rms - wide_rows * inv_rms**3 / width * inner
    ).astype(jnp.bfloat16)
    gain_term = jnp.sum(grad_normed * wide_rows * inv_rms, axis=0)
    normed_cols = lax.all_to_all(normed, "intra", split_axis=1, concat_axis=0, tiled=True)
    group_term = lax.dot_general(
        normed_cols,
        lax.all_gather(grad_mixed, "intra", axis=0, tiled=True),
        (((0,), (0,)), ((), ())),
        preferred_element_type=jnp.float32,
    )
    term_low = lax.optimization_barrier(group_term.astype(jnp.bfloat16))
    gain_sums = lax.psum_scatter(gain_term, "intra", scatter_dimension=0, tiled=True)
    weight_grad, gain_grad = (
        lax.psum_scatter(term_low.astype(jnp.float32), "inter", scatter_dimension=0, tiled=True),
        lax.psum_scatter(gain_sums, "inter", scatter_dimension=0, tiled=True),
    )
    return (attn_flat.reshape(tokens_here, qcols)[None], grad_rows[None], weight_grad, gain_grad)

MESH = pl.DeviceIdType.MESH
CORES = 2
SIDE = 2
PIECES = 4
CHUNK = 2 * HD


def nt_dot(a, b):
    return lax.dot_general(a, b, (((1,), (1,)), ((), ())), preferred_element_type=jnp.float32)


def tn_dot(a, b):
    return lax.dot_general(a, b, (((0,), (0,)), ((), ())), preferred_element_type=jnp.float32)


def nn_dot(a, b):
    return jnp.dot(a, b, preferred_element_type=jnp.float32)


def fused_kernel(
    n_inter,
    hid_ref, gain_ref, w_ref, ct_ref, cos_hbm, sin_hbm,
    attn_ref, gin_ref, wg_ref, gg_ref,
    wbuf, gbuf, gain_in, hx, hs, nbuf, ntr, inv_all, inv_s, inv_r, ctb, cts, cos_ref, sin_ref,
    mix, kv_s, kv_r, qm_s, qm_r, gq, gkv_s, gkv_r, in_s, in_r, at_s, at_r, gi_s, gi_r,
    tbuf, rs1, ybuf, rs2, zbuf, rs3, side, dg_s, dg_r, gg_s, gg_r,
    ld_sem, ag_send, ag_recv, g_send, g_recv, x_send, x_recv,
    c_send, c_recv, y_send, y_recv, z_send, z_recv, s_send, s_recv, d_send, d_recv,
):
    i = lax.axis_index("inter")
    x = lax.axis_index("intra")
    nz = n_inter // (CORES * SIDE)
    c = lax.rem(i, CORES)
    y = lax.rem(i // CORES, SIDE)
    z = i // (CORES * SIDE)
    toks, width = hid_ref.shape
    rows, cols = w_ref.shape
    seq = 2 * toks
    qcols = HEADS * HD
    chips = nz * SIDE
    chunks = cols // CHUNK
    span = n_inter // PIECES
    lanes = span * rows
    scale = HD ** (-0.5)
    f32, bf = jnp.float32, jnp.bfloat16

    def dev(zz, yy, cc, xx):
        return ((zz * SIDE + yy) * CORES + cc, xx)

    def slot(zz, yy, cc):
        return (zz * SIDE + yy) * CORES + cc

    def across(d):
        zz, bit = z, 1
        while bit < nz:
            if d & bit:
                zz = zz + bit - 2 * bit * lax.rem(z // bit, 2)
            bit *= 2
        return zz

    hops = list(range(1, nz))
    x_peer = dev(z, y, c, 1 - x)
    y_peer = dev(z, 1 - y, c, x)
    c_peer = dev(z, y, 1 - c, x)
    d_peer = dev(z, y, 1 - c, 1 - x)
    plane = [(d, yy, cc) for d in range(nz) for yy in (0, 1) for cc in (0, 1) if d or yy or cc]

    def plane_dev(e):
        d, yy, cc = e
        return (across(d), y + yy - 2 * yy * y, c + cc - 2 * cc * c)

    own = slot(z, y, c)
    here = pl.ds(pl.multiple_of(x * toks, toks), toks)
    there = pl.ds(pl.multiple_of((1 - x) * toks, toks), toks)

    def rcopy(src, dst, ss, rs, device):
        return pltpu.make_async_remote_copy(
            src_ref=src, dst_ref=dst, send_sem=ss, recv_sem=rs, device_id=device, device_id_type=MESH
        )

    barrier = pltpu.get_barrier_semaphore()
    peers = [dev(*plane_dev(e), x) for e in plane] + [x_peer, d_peer]
    for peer in peers:
        pl.semaphore_signal(barrier, inc=1, device_id=peer, device_id_type=MESH)

    def load(src, dst, k):
        pltpu.make_async_copy(src, dst, ld_sem.at[k]).start()

    def loaded(dst, k):
        pltpu.make_async_copy(dst, dst, ld_sem.at[k]).wait()

    for p in range(PIECES):
        for b in range(span):
            j = p * span + b
            mine = pl.ds(pl.multiple_of((2 * j + x) * rows, rows), rows)
            other = pl.ds(pl.multiple_of((2 * j + 1 - x) * rows, rows), rows)
            load(hid_ref.at[:, mine], hx.at[p, here, b * rows : (b + 1) * rows], 0)
            load(hid_ref.at[:, other], hs.at[p, :, b * rows : (b + 1) * rows], 1)
    load(w_ref.at[:, qcols:], wbuf.at[0, own], 2)
    half = HEADS // 2
    for n in range(half):
        for xx in range(2):
            first = (xx * half + n) * HD
            load(w_ref.at[:, first : first + HD], wbuf.at[1 + n, own, :, xx * HD : (xx + 1) * HD], 3 + n)
    nxt = 3 + half
    load(gain_ref, gain_in, nxt)
    load(ct_ref.at[:, pl.ds(pl.multiple_of(x * half * HD, HD), half * HD)], ctb.at[here], nxt + 1)
    load(ct_ref.at[:, pl.ds(pl.multiple_of((1 - x) * half * HD, HD), half * HD)], cts, nxt + 2)
    load(cos_hbm, cos_ref, nxt + 3)
    load(sin_hbm, sin_ref, nxt + 4)

    loaded(gain_in, nxt)
    gcol = lambda g: pl.ds(pl.multiple_of(g * rows, rows), rows)
    gbuf[:, gcol(own)] = gain_in[...].astype(f32)
    loaded(hx.at[:, here], 0)
    loaded(hs, 1)
    total = jnp.zeros((toks, 1), f32)
    for p in range(PIECES):
        a = hx[p, here, :].astype(f32)
        b = hs[p].astype(f32)
        total = total + jnp.sum(a * a + b * b, axis=1, keepdims=True)
    inv = jnp.broadcast_to(lax.rsqrt(total / width + eps_norm), (toks, HD))
    inv_all[here, :] = inv
    inv_s[...] = inv.T[:8, :]
    for q in range(chunks):
        loaded(wbuf.at[q, own], 2 + q)
    loaded(cts, nxt + 2)
    pl.semaphore_wait(barrier, len(peers))

    inner_z = jnp.logical_and(z > 0, z < nz - 1)
    far = nz - 1 if nz > 2 else None
    spare = chunks - 1

    def ag(q, g, link, device):
        return rcopy(wbuf.at[q, g], wbuf.at[q, g], ag_send.at[q, link], ag_recv.at[q, g], device)

    def arrive(q, g):
        ag(q, g, 0, x_peer).wait_recv()

    def x_copy(k, src, dst):
        return rcopy(src, dst, x_send.at[k], x_recv.at[k], x_peer)

    y_link = nz
    c_link = 2 * nz
    spare_link = 2 * nz + chips
    sent = []

    def push(q, g, link, device, cond=None):
        cp = ag(q, g, link, device)
        sent.append((cp, cond))
        if cond is None:
            cp.start()
        else:
            pl.when(cond)(cp.start)

    for n, e in enumerate(plane):
        rcopy(gbuf.at[:, gcol(own)], gbuf.at[:, gcol(own)], g_send.at[n], g_recv.at[own],
              dev(*plane_dev(e), x)).start()
    for q in range(chunks):
        for d in sorted(hops, key=lambda d: d % 2):
            push(q, own, d, dev(across(d), y, c, x), inner_z if d == far else None)
        push(q, own, y_link, y_peer)
        push(q, own, c_link, c_peer)
    messages = []

    def x_push(src, dst):
        cp = x_copy(len(messages), src, dst)
        cp.start()
        messages.append(cp)
        return cp

    inv_msg = x_push(inv_s, inv_r)
    hid_msg = [x_push(hs.at[p], hx.at[p, here]) for p in range(PIECES)]
    ct_msg = x_push(cts, ctb.at[here])

    def z_arrivals(q):
        for d in hops:
            g = slot(across(d), y, c)
            arrive(q, g)
            if d == 2:
                push(q, g, 0, dev(across(1), y, c, x), inner_z)
            if q != spare or d != 1:
                push(q, g, y_link + d, y_peer)
            push(q, g, c_link + d, c_peer)

    def y_arrival(q, d):
        g = slot(across(d), 1 - y, c)
        arrive(q, g)
        if q == spare and d == 0:
            push(q, g, spare_link, dev(across(1), y, c, x))
        push(q, g, c_link + nz + d, c_peer)

    def c_arrivals(q):
        for d in range(nz):
            for yy in (y, 1 - y):
                arrive(q, slot(across(d), yy, 1 - c))

    def norm(which):
        scaled = inv_all[which, :1]
        for p in range(PIECES):
            value = hx[p, which, :].astype(f32) * scaled * gbuf[:, p * lanes : (p + 1) * lanes]
            value = value.astype(bf)
            nbuf[p, which, :] = value
            ntr[p * lanes : (p + 1) * lanes, which] = value.T

    def partial(q):
        out = jnp.zeros((seq, CHUNK), f32)
        for p in range(PIECES):
            w = wbuf[q, p * span : (p + 1) * span].reshape(lanes, CHUNK)
            out = out + nn_dot(nbuf[p], w)
        mix[q] = out

    mycol = pl.ds(pl.multiple_of(x * HD, HD), HD)
    itscol = pl.ds(pl.multiple_of((1 - x) * HD, HD), HD)

    z_arrivals(0)
    for q in range(chunks):
        y_arrival(q, 0)
    z_arrivals(1)
    for n, e in enumerate(plane):
        g = slot(*plane_dev(e))
        rcopy(gbuf.at[:, gcol(g)], gbuf.at[:, gcol(g)], g_send.at[n], g_recv.at[g], x_peer).wait_recv()
    norm(here)
    for d in hops:
        y_arrival(0, d)
    inv_msg.wait_recv()
    for cp in hid_msg:
        cp.wait_recv()
    inv_all[there, :] = jnp.broadcast_to(inv_r[:1, :], (toks, toks)).T
    norm(there)
    c_arrivals(0)
    partial(0)
    kv_s[...] = mix[0].astype(bf)
    kv_msg = x_push(kv_s, kv_r)
    z_arrivals(2)
    q_msg = []
    for n in range(half):
        for d in hops:
            y_arrival(1 + n, d)
        c_arrivals(1 + n)
        partial(1 + n)
        qm_s[n] = mix[1 + n, :, itscol].astype(bf)
        q_msg.append(x_push(qm_s.at[n], qm_r.at[n]))

    loaded(cos_ref, nxt + 3)
    loaded(sin_ref, nxt + 4)
    loaded(ctb.at[here], nxt + 1)
    ct_msg.wait_recv()
    cosine, sine = cos_ref[...], sin_ref[...]

    def rope(u):
        return u * cosine + pltpu.roll(u, HD // 2, 1) * sine

    def unrope(u):
        return u * cosine - pltpu.roll(u, HD // 2, 1) * sine

    kv_msg.wait_recv()
    mix_kv = mix[0] + kv_r[...].astype(f32)
    mix[0] = mix_kv
    keys = rope(mix_kv[:, :HD]).astype(bf)
    values = mix_kv[:, HD:].astype(bf)
    allowed = lax.broadcasted_iota(jnp.int32, (seq, seq), 1) <= lax.broadcasted_iota(jnp.int32, (seq, seq), 0)
    inner = jnp.zeros((seq, 1), f32)
    grad_keys = jnp.zeros((seq, HD), f32)
    grad_values = jnp.zeros((seq, HD), f32)
    gq_msg = []

    def head(n, inner, grad_keys, grad_values):
        q_msg[n].wait_recv()
        mixed = mix[1 + n, :, mycol] + qm_r[n].astype(f32)
        query = (rope(mixed) * scale).astype(bf)
        grad = ctb[:, n * HD : (n + 1) * HD]
        scores = jnp.where(allowed, nt_dot(query, keys), -1e30)
        top = jnp.max(scores, axis=1, keepdims=True)
        numbers = jnp.where(allowed, jnp.exp(scores - top), 0.0)
        norm_sum = jnp.sum(numbers, axis=1, keepdims=True)
        high = numbers.astype(bf)
        low = (numbers - high.astype(f32)).astype(bf)
        attn = ((nn_dot(high, values) + nn_dot(low, values)) / norm_sum).astype(bf)
        at_s[n] = attn
        delta = jnp.sum(grad.astype(f32) * attn.astype(f32), axis=1, keepdims=True)
        probs = numbers / norm_sum
        grad_scores = (probs * (nt_dot(grad, values) - delta)).astype(bf)
        back = (unrope(nn_dot(grad_scores, keys)) * scale).astype(bf)
        gq[n, x] = back
        gq_msg.append(x_push(gq.at[n, x], gq.at[n, x]))
        inner = inner + jnp.sum(back.astype(f32) * mixed, axis=1, keepdims=True)
        grad_keys = grad_keys + tn_dot(grad_scores, query)
        grad_values = grad_values + tn_dot(probs.astype(bf), grad)
        return inner, grad_keys, grad_values

    def to_core(q, k):
        return rcopy(tbuf.at[q, (1 - c) * chips + k], rs1.at[q, k], c_send.at[q, k], c_recv.at[q, k], c_peer)

    def to_y(q, d):
        return rcopy(ybuf.at[q, d], rs2.at[q, d], y_send.at[q, d], y_recv.at[q, d], y_peer)

    def to_z(q, d):
        return rcopy(zbuf.at[q, d - 1], rs3.at[q, d - 1], z_send.at[q, d - 1], z_recv.at[q, d - 1],
                     dev(across(d), y, c, x))

    order = ([far] if far else []) + hops[:far - 1 if far else None] + [0]
    turn = chunks - 1

    def terms(q, grads, cc):
        part = nn_dot(ntr[pl.ds(pl.multiple_of(cc * chips * rows, rows), chips * rows), :], grads)
        tbuf[q, pl.ds(cc * chips, chips)] = part.astype(bf).reshape(chips, rows, CHUNK)

    def to_side(q, k, src):
        return rcopy(src, side.at[k, q], s_send.at[k, q], s_recv.at[k, q], dev(across(1), y, c, x))

    def core_sum(q, k):
        to_core(q, k).wait_recv()
        return tbuf[q, c * chips + k].astype(f32) + rs1[q, k].astype(f32)

    def rs_start(q, grads):
        terms(q, grads, 1 - c)
        for yy in (1 - y, y):
            for d in order:
                to_core(q, across(d) * SIDE + yy).start()
        terms(q, grads, c)
        for d in order:
            part = core_sum(q, across(d) * SIDE + 1 - y)
            if q == turn and d == 0:
                to_side(q, 0, ybuf.at[q, 1]).wait_recv()
                part = part + side[0, q].astype(f32)
            ybuf[q, d] = part.astype(bf)
            if q == turn and d == 1:
                to_side(q, 0, ybuf.at[q, d]).start()
            else:
                to_y(q, d).start()

    def rs_middle(q):
        for d in order:
            part = core_sum(q, across(d) * SIDE + y)
            if q != turn or d != 1:
                to_y(q, d).wait_recv()
                part = part + rs2[q, d].astype(f32)
            if d == 0:
                mix[q, :rows, :] = part
            elif d == far:
                zbuf[q, d - 1] = part.astype(bf)
                pl.when(inner_z)(to_z(q, d).start)
                pl.when(jnp.logical_not(inner_z))(to_side(q, 1, zbuf.at[q, d - 1]).start)
            elif d == 2:
                pl.when(inner_z)(to_side(q, 1, zbuf.at[q, d - 1]).wait_recv)
                extra = jnp.where(inner_z, side[1, q].astype(f32), 0.0)
                zbuf[q, d - 1] = (part + extra).astype(bf)
                to_z(q, d).start()
            else:
                zbuf[q, d - 1] = part.astype(bf)
                to_z(q, d).start()

    block = c * chips + z * SIDE + y
    cross = c != x
    sums = []

    def rs_end(q):
        result = mix[q, :rows, :]
        for d in hops:
            if d == far:
                pl.when(inner_z)(to_z(q, d).wait_recv)
                result = result + jnp.where(inner_z, rs3[q, d - 1].astype(f32), 0.0)
            else:
                to_z(q, d).wait_recv()
                result = result + rs3[q, d - 1].astype(f32)
        prod = wbuf[q, block].astype(f32) * result
        sums.append(prod[:, :HD] + prod[:, HD:])
        dg_s[q] = result.astype(bf)
        pl.when(cross)(lambda: to_diag(q).start())
        store(q, result)

    def store(q, result):
        if q == 0:
            wg_ref[:, qcols:] = result
        else:
            for xx in range(2):
                first = (xx * half + q - 1) * HD
                wg_ref[:, first : first + HD] = result[:, xx * HD : (xx + 1) * HD]

    def to_diag(q):
        return rcopy(dg_s.at[q], dg_r.at[q], d_send.at[q], d_recv.at[q], d_peer)

    gg_copy = rcopy(gg_s, gg_r, d_send.at[chunks], d_recv.at[chunks], d_peer)

    def rs_head(n):
        gq_msg[n].wait_recv()
        rs_start(1 + n, jnp.concatenate([gq[n, 0], gq[n, 1]], axis=1))

    for n in range(half):
        inner, grad_keys, grad_values = head(n, inner, grad_keys, grad_values)
        if n < half - 1:
            rs_head(n)
    grad_keys = unrope(grad_keys)
    gkv_s[:, :HD] = grad_keys.astype(bf)
    gkv_s[:, HD:] = grad_values.astype(bf)
    gkv_msg = x_push(gkv_s, gkv_r)
    inner_all = jnp.broadcast_to(inner, (seq, HD))
    in_s[...] = inner_all.T[:8, :]
    in_msg = x_push(in_s, in_r)
    for n in range(half):
        attn_ref[:, pl.ds(pl.multiple_of((x * half + n) * HD, HD), HD)] = at_s[n, here, :]

    rs_head(half - 1)
    gkv_msg.wait_recv()
    keys_sum = gkv_s[:, :HD].astype(f32) + gkv_r[:, :HD].astype(f32)
    values_sum = gkv_s[:, HD:].astype(f32) + gkv_r[:, HD:].astype(f32)
    gkv_all = jnp.concatenate([keys_sum, values_sum], axis=1).astype(bf)
    rs_start(0, gkv_all)
    in_msg.wait_recv()
    inner = inner + jnp.broadcast_to(in_r[:1, :], (HD, seq)).T[:, :1]
    inner = inner + jnp.sum(gkv_all.astype(f32) * mix[0], axis=1, keepdims=True)
    inv = inv_all[...]
    inv_all[...] = inner * (inv * inv / width)

    gqs = [jnp.concatenate([gq[n, 0], gq[n, 1]], axis=1) for n in range(half)]
    gi_msg = []
    for p in range(PIECES):
        out = jnp.zeros((seq, lanes), f32)
        for q in range(chunks):
            w = wbuf[q, p * span : (p + 1) * span].reshape(lanes, CHUNK)
            out = out + nt_dot(gkv_all if q == 0 else gqs[q - 1], w)
        gain = gbuf[:, p * lanes : (p + 1) * lanes]
        gi_s[p] = (gain * out * inv[:, :1] - hx[p].astype(f32) * inv_all[:, :1]).astype(bf)
        gi_msg.append(x_push(gi_s.at[p, there], gi_r.at[p]))
    at_msg = x_push(at_s.at[:, there], at_r)

    queue = list(range(1, chunks)) + [0]
    rs_middle(queue[0])
    for p in range(PIECES):
        for b in range(span):
            j = p * span + b
            gin_ref[:, pl.ds(pl.multiple_of((2 * j + x) * rows, rows), rows)] = gi_s[p, here, b * rows : (b + 1) * rows]
    for n in range(1, chunks):
        rs_middle(queue[n])
        rs_end(queue[n - 1])
    rs_end(queue[-1])
    lanes_sum = sums[0]
    for part in sums[1:]:
        lanes_sum = lanes_sum + part
    gg = jnp.sum(lanes_sum.T, axis=0, keepdims=True) / gbuf[:, gcol(block)]
    gg_ref[...] = gg
    gg_s[...] = gg
    pl.when(cross)(lambda: gg_copy.start())

    at_msg.wait_recv()
    for n in range(half):
        attn_ref[:, pl.ds(pl.multiple_of(((1 - x) * half + n) * HD, HD), HD)] = at_r[n]
    for p in range(PIECES):
        gi_msg[p].wait_recv()
        for b in range(span):
            j = p * span + b
            gin_ref[:, pl.ds(pl.multiple_of((2 * j + 1 - x) * rows, rows), rows)] = gi_r[p, :, b * rows : (b + 1) * rows]

    for cp, cond in sent:
        if cond is None:
            cp.wait_send()
        else:
            pl.when(cond)(cp.wait_send)
    for cp in messages:
        cp.wait_send()
    for n, e in enumerate(plane):
        rcopy(gbuf.at[:, gcol(own)], gbuf.at[:, gcol(own)], g_send.at[n], g_recv.at[own], x_peer).wait_send()
    for q in range(chunks):
        for k in range(chips):
            to_core(q, k).wait_send()
        for d in range(nz):
            if q != turn or d != 1:
                to_y(q, d).wait_send()
            else:
                to_side(q, 0, ybuf.at[q, d]).wait_send()
        for d in hops:
            if d == far:
                pl.when(inner_z)(to_z(q, d).wait_send)
                pl.when(jnp.logical_not(inner_z))(to_side(q, 1, zbuf.at[q, d - 1]).wait_send)
            else:
                to_z(q, d).wait_send()

    @pl.when(cross)
    def _():
        for q in queue:
            to_diag(q).wait_recv()
            store(q, dg_r[q].astype(f32))
        gg_copy.wait_recv()
        gg_ref[...] = gg_r[...]
        for q in range(chunks):
            to_diag(q).wait_send()
        gg_copy.wait_send()


def copy_kernel(*refs):
    sems = refs[8]
    copies = [pltpu.make_async_copy(refs[k], refs[4 + k], sems.at[k]) for k in range(4)]
    for cp in copies:
        cp.start()
    for cp in copies:
        cp.wait()


def fused(n_inter, hidden_in, norm_gain, qkv_weight, attn_cotangent):
    toks, width = hidden_in.shape[1:]
    rows, cols = qkv_weight.shape
    nz = n_inter // (CORES * SIDE)
    chips = nz * SIDE
    seq, half, chunks = 2 * toks, HEADS // 2, cols // CHUNK
    lanes = n_inter // PIECES * rows
    freqs = rope_base ** (-np.arange(HD // 2, dtype=np.float32) / np.float32(HD // 2))
    angles = (np.arange(seq, dtype=np.float32)[:, None] * freqs.astype(np.float32)[None, :]).astype(np.float32)
    cosine = np.concatenate([np.cos(angles)] * 2, axis=1).astype(np.float32)
    sine = np.concatenate([-np.sin(angles), np.sin(angles)], axis=1).astype(np.float32)
    bf, f32, dma = jnp.bfloat16, jnp.float32, pltpu.SemaphoreType.DMA
    vmem = pl.BlockSpec(memory_space=pltpu.VMEM)
    hbm = pl.BlockSpec(memory_space=pltpu.HBM)
    V = pltpu.VMEM
    n_msgs = 2 * PIECES + 2 * half + 6
    ins = (hidden_in[0], norm_gain[None], qkv_weight, attn_cotangent[0], jnp.asarray(cosine), jnp.asarray(sine))
    attn, gin, wg, gg = pl.pallas_call(
        functools.partial(fused_kernel, n_inter),
        out_shape=(V((toks, HEADS * HD), bf), V((toks, width), bf), V((rows, cols), f32), V((1, rows), f32)),
        in_specs=[hbm] * 6,
        out_specs=(vmem,) * 4,
        scratch_shapes=[
            V((chunks, n_inter, rows, CHUNK), bf),
            V((1, n_inter * rows), f32),
            V((1, rows), bf),
            V((PIECES, seq, lanes), bf),
            V((PIECES, toks, lanes), bf),
            V((PIECES, seq, lanes), bf),
            V((n_inter * rows, seq), bf),
            V((seq, HD), f32),
            V((8, toks), f32),
            V((8, toks), f32),
            V((seq, half * HD), bf),
            V((toks, half * HD), bf),
            V((seq, HD), f32),
            V((seq, HD), f32),
            V((chunks, seq, CHUNK), f32),
            V((seq, CHUNK), bf),
            V((seq, CHUNK), bf),
            V((half, seq, HD), bf),
            V((half, seq, HD), bf),
            V((half, 2, seq, HD), bf),
            V((seq, CHUNK), bf),
            V((seq, CHUNK), bf),
            V((8, seq), f32),
            V((8, seq), f32),
            V((half, seq, HD), bf),
            V((half, toks, HD), bf),
            V((PIECES, seq, lanes), bf),
            V((PIECES, toks, lanes), bf),
            V((chunks, n_inter, rows, CHUNK), bf),
            V((chunks, chips, rows, CHUNK), bf),
            V((chunks, nz, rows, CHUNK), bf),
            V((chunks, nz, rows, CHUNK), bf),
            V((chunks, nz - 1, rows, CHUNK), bf),
            V((chunks, nz - 1, rows, CHUNK), bf),
            V((2, chunks, rows, CHUNK), bf),
            V((chunks, rows, CHUNK), bf),
            V((chunks, rows, CHUNK), bf),
            V((1, rows), f32),
            V((1, rows), f32),
            dma((8 + half,)),
            dma((chunks, 2 * nz + chips + 1)), dma((chunks, n_inter)),
            dma((n_inter,)), dma((n_inter,)),
            dma((n_msgs,)), dma((n_msgs,)),
            dma((chunks, chips)), dma((chunks, chips)),
            dma((chunks, nz)), dma((chunks, nz)),
            dma((chunks, nz - 1)), dma((chunks, nz - 1)),
            dma((2, chunks)), dma((2, chunks)),
            dma((chunks + 1,)), dma((chunks + 1,)),
        ],
        compiler_params=pltpu.CompilerParams(
            collective_id=0, has_side_effects=True, vmem_limit_bytes=32 * 2**20
        ),
    )(*[pltpu.with_memory_space_constraint(a, pltpu.HBM) for a in ins])
    outs = (attn, gin, wg, gg)
    attn, gin, wg, gg = pl.pallas_call(
        copy_kernel,
        out_shape=tuple(jax.ShapeDtypeStruct(o.shape, o.dtype) for o in outs),
        in_specs=[vmem] * 4,
        out_specs=(hbm,) * 4,
        scratch_shapes=[dma((4,))],
        compiler_params=pltpu.CompilerParams(vmem_limit_bytes=2**20),
    )(*[pltpu.with_memory_space_constraint(o, pltpu.VMEM) for o in outs])
    return attn[None], gin[None], wg, gg[0]


def solution(mesh):
    n_inter, n_intra = mesh.shape["inter"], mesh.shape["intra"]

    def body(hidden_in, norm_gain, qkv_weight, attn_cotangent):
        nz = n_inter // (CORES * SIDE)
        fits = n_intra == 2 and n_inter % (CORES * SIDE) == 0 and nz > 1 and nz & (nz - 1) == 0
        fits = fits and qkv_weight.shape[0] == HD and hidden_in.shape[0] == 1
        fits = fits and hidden_in.shape[1] == HD and n_inter % PIECES == 0
        if fits:
            return fused(n_inter, hidden_in, norm_gain, qkv_weight, attn_cotangent)
        return local(hidden_in, norm_gain, qkv_weight, attn_cotangent)

    return jax.shard_map(
        body,
        mesh=mesh,
        in_specs=(
            P("inter", "intra", None),
            P(("inter", "intra")),
            P(("inter", "intra"), None),
            P("inter", "intra", None),
        ),
        out_specs=(
            P("inter", "intra", None),
            P("inter", "intra", None),
            P(("intra", "inter"), None),
            P(("intra", "inter")),
        ),
        check_vma=False,
    )
```

```python
import functools
import jax
import jax.numpy as jnp
import numpy as np
from jax import lax
from jax.experimental import pallas as pl
from jax.experimental.pallas import tpu as pltpu
from jax.sharding import PartitionSpec as P

HD = 128
HEADS = 4


eps_norm = 1e-05
rope_base = 500000.0


def rope_tables(positions, head_size):
    half_size = head_size // 2
    freqs = rope_base ** (-jnp.arange(half_size, dtype=jnp.float32) / half_size)
    angles = positions.astype(jnp.float32)[:, None] * freqs[None, :]
    return (jnp.cos(angles), jnp.sin(angles))


def rotate(values_in, cosine, sine):
    half_size = values_in.shape[-1] // 2
    first, second = (values_in[..., :half_size], values_in[..., half_size:])
    return jnp.concatenate(
        [first * cosine - second * sine, second * cosine + first * sine], axis=-1
    )


def unrotate(grad_out, cosine, sine):
    half_size = grad_out.shape[-1] // 2
    first, second = (grad_out[..., :half_size], grad_out[..., half_size:])
    return jnp.concatenate(
        [first * cosine + second * sine, second * cosine - first * sine], axis=-1
    )


def forward_fold(query_rows, row_pos):

    def forward_advance(carry, piece, start):
        row_top, row_total, weighted = carry
        key_part, value_part = piece
        scores = jnp.einsum("qd,kd->qk", query_rows, key_part, preferred_element_type=jnp.float32)
        key_pos = jnp.arange(key_part.shape[0], dtype=jnp.int32)
        allowed = key_pos[None, :] <= row_pos[:, None]
        scores = jnp.where(allowed, scores, -1e30)
        new_top = jnp.maximum(row_top, jnp.max(scores, axis=1))
        numbers = jnp.where(allowed, jnp.exp(scores - new_top[:, None]), 0.0)
        row_total = jnp.sum(numbers, axis=1)
        weighted = jnp.dot(
            numbers,
            value_part.astype(jnp.float32),
            precision=lax.Precision.HIGHEST,
            preferred_element_type=jnp.float32,
        )
        return (new_top, row_total, weighted)

    return forward_advance


def query_grad_fold(query_rows, row_pos, grad_flat, log_total, row_delta):

    def query_advance(grad_query, piece, start):
        key_part, value_part = piece
        scores = jnp.einsum("qd,kd->qk", query_rows, key_part, preferred_element_type=jnp.float32)
        key_pos = jnp.arange(key_part.shape[0], dtype=jnp.int32)
        allowed = key_pos[None, :] <= row_pos[:, None]
        probs = jnp.where(
            allowed, jnp.exp(jnp.where(allowed, scores, -1e30) - log_total[:, None]), 0.0
        )
        grad_probs = jnp.einsum(
            "qd,kd->qk", grad_flat, value_part, preferred_element_type=jnp.float32
        )
        grad_scores = (probs * (grad_probs - row_delta[:, None])).astype(jnp.bfloat16)
        return jnp.dot(grad_scores, key_part, preferred_element_type=jnp.float32)

    return query_advance


def key_grad_fold(key_rows, value_rows, key_pos, log_all, delta_all, heads_count):

    def key_advance(carry, piece, start):
        query_part, attn_grad_part = piece
        count = query_part.shape[0]
        scores = jnp.einsum("qd,kd->qk", query_part, key_rows, preferred_element_type=jnp.float32)
        query_pos = jnp.arange(count, dtype=jnp.int32) // heads_count
        allowed = key_pos[None, :] <= query_pos[:, None]
        probs = jnp.where(
            allowed, jnp.exp(jnp.where(allowed, scores, -1e30) - log_all[:, None]), 0.0
        )
        grad_values = jnp.einsum(
            "qk,qd->kd",
            probs.astype(jnp.bfloat16),
            attn_grad_part,
            preferred_element_type=jnp.float32,
        )
        grad_probs = jnp.einsum(
            "qd,kd->qk", attn_grad_part, value_rows, preferred_element_type=jnp.float32
        )
        grad_scores = (probs * (grad_probs - delta_all[:, None])).astype(jnp.bfloat16)
        grad_keys = jnp.einsum(
            "qk,qd->kd", grad_scores, query_part, preferred_element_type=jnp.float32
        )
        return (grad_keys, grad_values)

    return key_advance


def local(hidden_in, norm_gain, qkv_weight, attn_cotangent):
    rows_in = hidden_in[0]
    grad_attn = attn_cotangent[0]
    tokens_here = rows_in.shape[0]
    width = rows_in.shape[1]
    head_size = HD
    heads_count = HEADS
    qcols = heads_count * head_size
    scale = head_size ** (-0.5)
    weight_group, gain_group = (
        lax.all_gather(qkv_weight, "intra", axis=0, tiled=True),
        lax.all_gather(norm_gain, "intra", axis=0, tiled=True),
    )
    weight_full, gain_full = (
        lax.all_gather(weight_group, "inter", axis=0, tiled=True),
        lax.all_gather(gain_group, "inter", axis=0, tiled=True),
    )
    query_pos = lax.axis_index("intra") * tokens_here + jnp.arange(tokens_here, dtype=jnp.int32)
    row_pos = jnp.broadcast_to(query_pos[:, None], (tokens_here, heads_count)).reshape(
        tokens_here * heads_count
    )
    cosine, sine = rope_tables(query_pos, head_size)
    wide_rows = rows_in.astype(jnp.float32)
    inv_rms = lax.rsqrt(jnp.mean(wide_rows * wide_rows, axis=1, keepdims=True) + eps_norm)
    normed = (wide_rows * inv_rms * gain_full.astype(jnp.float32)[None, :]).astype(jnp.bfloat16)
    mixed = jnp.dot(normed, weight_full, preferred_element_type=jnp.float32)
    query_rows = (
        (
            rotate(
                mixed[:, :qcols].reshape(tokens_here, heads_count, head_size),
                cosine[:, None, :],
                sine[:, None, :],
            )
            * scale
        )
        .astype(jnp.bfloat16)
        .reshape(tokens_here * heads_count, head_size)
    )
    key_rows = rotate(mixed[:, qcols : qcols + head_size], cosine, sine).astype(jnp.bfloat16)
    value_rows = mixed[:, qcols + head_size :].astype(jnp.bfloat16)
    grad_flat = grad_attn.reshape(tokens_here * heads_count, head_size)
    flat_rows = tokens_here * heads_count
    forward_step = forward_fold(query_rows, row_pos)
    start_carry = (
        jnp.full((flat_rows,), -1e30, jnp.float32),
        jnp.zeros((flat_rows,), jnp.float32),
        jnp.zeros((flat_rows, head_size), jnp.float32),
    )
    row_top, row_total, weighted = forward_step(
        start_carry,
        (
            lax.all_gather(key_rows, "intra", axis=0, tiled=True),
            lax.all_gather(value_rows, "intra", axis=0, tiled=True),
        ),
        jnp.int32(0),
    )
    attn_flat = (weighted / row_total[:, None]).astype(jnp.bfloat16)
    log_total = row_top + jnp.log(row_total)
    row_delta = jnp.sum(grad_flat.astype(jnp.float32) * attn_flat.astype(jnp.float32), axis=1)
    query_step = query_grad_fold(query_rows, row_pos, grad_flat, log_total, row_delta)
    grad_query = query_step(
        jnp.zeros((flat_rows, head_size), jnp.float32),
        (
            lax.all_gather(key_rows, "intra", axis=0, tiled=True),
            lax.all_gather(value_rows, "intra", axis=0, tiled=True),
        ),
        jnp.int32(0),
    )
    log_all, delta_all = (
        lax.all_gather(log_total, "intra", axis=0, tiled=True),
        lax.all_gather(row_delta, "intra", axis=0, tiled=True),
    )
    key_step = key_grad_fold(key_rows, value_rows, query_pos, log_all, delta_all, heads_count)
    grad_keys, grad_values = key_step(
        (
            jnp.zeros((tokens_here, head_size), jnp.float32),
            jnp.zeros((tokens_here, head_size), jnp.float32),
        ),
        (
            lax.all_gather(query_rows, "intra", axis=0, tiled=True),
            lax.all_gather(grad_flat, "intra", axis=0, tiled=True),
        ),
        jnp.int32(0),
    )
    query_back = (
        unrotate(
            grad_query.reshape(tokens_here, heads_count, head_size),
            cosine[:, None, :],
            sine[:, None, :],
        )
        * scale
    ).reshape(tokens_here, qcols)
    grad_mixed = jnp.concatenate(
        [query_back, unrotate(grad_keys, cosine, sine), grad_values], axis=1
    ).astype(jnp.bfloat16)
    weight_back, gain_back = (weight_full, gain_full)
    gain_wide = gain_back.astype(jnp.float32)[None, :]
    grad_normed = jnp.einsum(
        "tc,dc->td", grad_mixed, weight_back, preferred_element_type=jnp.float32
    )
    inner = jnp.sum(grad_normed * gain_wide * wide_rows, axis=1, keepdims=True)
    grad_rows = (
        gain_wide * grad_normed * inv_rms - wide_rows * inv_rms**3 / width * inner
    ).astype(jnp.bfloat16)
    gain_term = jnp.sum(grad_normed * wide_rows * inv_rms, axis=0)
    normed_cols = lax.all_to_all(normed, "intra", split_axis=1, concat_axis=0, tiled=True)
    group_term = lax.dot_general(
        normed_cols,
        lax.all_gather(grad_mixed, "intra", axis=0, tiled=True),
        (((0,), (0,)), ((), ())),
        preferred_element_type=jnp.float32,
    )
    term_low = lax.optimization_barrier(group_term.astype(jnp.bfloat16))
    gain_sums = lax.psum_scatter(gain_term, "intra", scatter_dimension=0, tiled=True)
    weight_grad, gain_grad = (
        lax.psum_scatter(term_low.astype(jnp.float32), "inter", scatter_dimension=0, tiled=True),
        lax.psum_scatter(gain_sums, "inter", scatter_dimension=0, tiled=True),
    )
    return (attn_flat.reshape(tokens_here, qcols)[None], grad_rows[None], weight_grad, gain_grad)

MESH = pl.DeviceIdType.MESH
CORES = 2
SIDE = 2
PIECES = 4
CHUNK = 2 * HD


def nt_dot(a, b):
    return lax.dot_general(a, b, (((1,), (1,)), ((), ())), preferred_element_type=jnp.float32)


def tn_dot(a, b):
    return lax.dot_general(a, b, (((0,), (0,)), ((), ())), preferred_element_type=jnp.float32)


def nn_dot(a, b):
    return jnp.dot(a, b, preferred_element_type=jnp.float32)


def fused_kernel(
    n_inter,
    hid_ref, gain_ref, w_ref, ct_ref, cos_hbm, sin_hbm,
    attn_ref, gin_ref, wg_ref, gg_ref,
    wbuf, gbuf, gain_in, hx, hs, nbuf, ntr, inv_all, inv_s, inv_r, ctb, cts, cos_ref, sin_ref,
    mix, kv_s, kv_r, qm_s, qm_r, gq, gkv_s, gkv_r, in_s, in_r, at_s, at_r, gi_s, gi_r,
    tbuf, rs1, ybuf, rs2, zbuf, rs3, side, dg_s, dg_r, gg_s, gg_r,
    ld_sem, ag_send, ag_recv, g_send, g_recv, x_send, x_recv,
    c_send, c_recv, y_send, y_recv, z_send, z_recv, s_send, s_recv, d_send, d_recv,
):
    i = lax.axis_index("inter")
    x = lax.axis_index("intra")
    nz = n_inter // (CORES * SIDE)
    c = lax.rem(i, CORES)
    y = lax.rem(i // CORES, SIDE)
    z = i // (CORES * SIDE)
    toks, width = hid_ref.shape
    rows, cols = w_ref.shape
    seq = 2 * toks
    qcols = HEADS * HD
    chips = nz * SIDE
    chunks = cols // CHUNK
    span = n_inter // PIECES
    lanes = span * rows
    scale = HD ** (-0.5)
    f32, bf = jnp.float32, jnp.bfloat16

    def dev(zz, yy, cc, xx):
        return ((zz * SIDE + yy) * CORES + cc, xx)

    def slot(zz, yy, cc):
        return (zz * SIDE + yy) * CORES + cc

    def across(d):
        zz, bit = z, 1
        while bit < nz:
            if d & bit:
                zz = zz + bit - 2 * bit * lax.rem(z // bit, 2)
            bit *= 2
        return zz

    hops = list(range(1, nz))
    x_peer = dev(z, y, c, 1 - x)
    y_peer = dev(z, 1 - y, c, x)
    c_peer = dev(z, y, 1 - c, x)
    d_peer = dev(z, y, 1 - c, 1 - x)
    plane = [(d, yy, cc) for d in range(nz) for yy in (0, 1) for cc in (0, 1) if d or yy or cc]

    def plane_dev(e):
        d, yy, cc = e
        return (across(d), y + yy - 2 * yy * y, c + cc - 2 * cc * c)

    own = slot(z, y, c)
    here = pl.ds(pl.multiple_of(x * toks, toks), toks)
    there = pl.ds(pl.multiple_of((1 - x) * toks, toks), toks)

    def rcopy(src, dst, ss, rs, device):
        return pltpu.make_async_remote_copy(
            src_ref=src, dst_ref=dst, send_sem=ss, recv_sem=rs, device_id=device, device_id_type=MESH
        )

    barrier = pltpu.get_barrier_semaphore()
    peers = [dev(*plane_dev(e), x) for e in plane] + [x_peer, d_peer]
    for peer in peers:
        pl.semaphore_signal(barrier, inc=1, device_id=peer, device_id_type=MESH)

    def load(src, dst, k):
        pltpu.make_async_copy(src, dst, ld_sem.at[k]).start()

    def loaded(dst, k):
        pltpu.make_async_copy(dst, dst, ld_sem.at[k]).wait()

    for p in range(PIECES):
        for b in range(span):
            j = p * span + b
            mine = pl.ds(pl.multiple_of((2 * j + x) * rows, rows), rows)
            other = pl.ds(pl.multiple_of((2 * j + 1 - x) * rows, rows), rows)
            load(hid_ref.at[:, mine], hx.at[p, here, b * rows : (b + 1) * rows], 0)
            load(hid_ref.at[:, other], hs.at[p, :, b * rows : (b + 1) * rows], 1)
    load(w_ref.at[:, qcols:], wbuf.at[0, own], 2)
    half = HEADS // 2
    for n in range(half):
        for xx in range(2):
            first = (xx * half + n) * HD
            load(w_ref.at[:, first : first + HD], wbuf.at[1 + n, own, :, xx * HD : (xx + 1) * HD], 3 + n)
    nxt = 3 + half
    load(gain_ref, gain_in, nxt)
    load(ct_ref.at[:, pl.ds(pl.multiple_of(x * half * HD, HD), half * HD)], ctb.at[here], nxt + 1)
    load(ct_ref.at[:, pl.ds(pl.multiple_of((1 - x) * half * HD, HD), half * HD)], cts, nxt + 2)
    load(cos_hbm, cos_ref, nxt + 3)
    load(sin_hbm, sin_ref, nxt + 4)

    loaded(gain_in, nxt)
    gcol = lambda g: pl.ds(pl.multiple_of(g * rows, rows), rows)
    gbuf[:, gcol(own)] = gain_in[...].astype(f32)
    loaded(hx.at[:, here], 0)
    loaded(hs, 1)
    total = jnp.zeros((toks, 1), f32)
    for p in range(PIECES):
        a = hx[p, here, :].astype(f32)
        b = hs[p].astype(f32)
        total = total + jnp.sum(a * a + b * b, axis=1, keepdims=True)
    inv = jnp.broadcast_to(lax.rsqrt(total / width + eps_norm), (toks, HD))
    inv_all[here, :] = inv
    inv_s[...] = inv.T[:8, :]
    for q in range(chunks):
        loaded(wbuf.at[q, own], 2 + q)
    loaded(cts, nxt + 2)
    pl.semaphore_wait(barrier, len(peers))

    inner_z = jnp.logical_and(z > 0, z < nz - 1)
    far = nz - 1 if nz > 2 else None
    spare = chunks - 1

    def ag(q, g, link, device):
        return rcopy(wbuf.at[q, g], wbuf.at[q, g], ag_send.at[q, link], ag_recv.at[q, g], device)

    def arrive(q, g):
        ag(q, g, 0, x_peer).wait_recv()

    def x_copy(k, src, dst):
        return rcopy(src, dst, x_send.at[k], x_recv.at[k], x_peer)

    y_link = nz
    c_link = 2 * nz
    spare_link = 2 * nz + chips
    sent = []

    def push(q, g, link, device, cond=None):
        cp = ag(q, g, link, device)
        sent.append((cp, cond))
        if cond is None:
            cp.start()
        else:
            pl.when(cond)(cp.start)

    for n, e in enumerate(plane):
        rcopy(gbuf.at[:, gcol(own)], gbuf.at[:, gcol(own)], g_send.at[n], g_recv.at[own],
              dev(*plane_dev(e), x)).start()
    def own_z(q):
        for d in ([far] if far else []) + hops[::-1][1 if far else 0 :]:
            push(q, own, d, dev(across(d), y, c, x), inner_z if d == far and q else None)

    for q in range(chunks):
        if q < chunks - 1:
            own_z(q)
        push(q, own, y_link, y_peer)
        push(q, own, c_link, c_peer)
    messages = []

    def x_push(src, dst):
        cp = x_copy(len(messages), src, dst)
        cp.start()
        messages.append(cp)
        return cp

    inv_msg = x_push(inv_s, inv_r)
    hid_msg = [x_push(hs.at[p], hx.at[p, here]) for p in range(PIECES)]
    ct_msg = x_push(cts, ctb.at[here])

    def near(n):
        if n < 2:
            return across(n)
        return jnp.where(inner_z, across(nz + 1 - n), across(n))

    def z_arrival(q, n):
        g = slot(near(n), y, c)
        arrive(q, g)
        if n == far and q:
            push(q, g, 0, dev(across(1), y, c, x), inner_z)
        if q != spare or n != 1:
            push(q, g, y_link + n, y_peer)
        push(q, g, c_link + n, c_peer)

    def z_arrivals(q, ns):
        for n in ns:
            z_arrival(q, n)

    def y_arrival(q, d):
        g = slot(near(d), 1 - y, c)
        arrive(q, g)
        if q == spare and d == 0:
            push(q, g, spare_link, dev(across(1), y, c, x))
        push(q, g, c_link + nz + d, c_peer)

    def c_arrivals(q):
        for d in range(nz):
            for yy in (y, 1 - y):
                arrive(q, slot(across(d), yy, 1 - c))

    def norm(which):
        scaled = inv_all[which, :1]
        for p in range(PIECES):
            value = hx[p, which, :].astype(f32) * scaled * gbuf[:, p * lanes : (p + 1) * lanes]
            value = value.astype(bf)
            nbuf[p, which, :] = value
            ntr[p * lanes : (p + 1) * lanes, which] = value.T

    def partial(q):
        out = jnp.zeros((seq, CHUNK), f32)
        for p in range(PIECES):
            w = wbuf[q, p * span : (p + 1) * span].reshape(lanes, CHUNK)
            out = out + nn_dot(nbuf[p], w)
        mix[q] = out

    mycol = pl.ds(pl.multiple_of(x * HD, HD), HD)
    itscol = pl.ds(pl.multiple_of((1 - x) * HD, HD), HD)

    def finish(q):
        for d in hops:
            y_arrival(q, d)
        c_arrivals(q)
        partial(q)

    q_msg = []

    def finish_q(n):
        finish(1 + n)
        qm_s[n] = mix[1 + n, :, itscol].astype(bf)
        q_msg.append(x_push(qm_s.at[n], qm_r.at[n]))

    z_arrivals(0, hops)
    y_arrival(0, 0)
    y_arrival(1, 0)
    own_z(chunks - 1)
    y_arrival(2, 0)
    z_arrivals(1, hops)
    for n, e in enumerate(plane):
        g = slot(*plane_dev(e))
        rcopy(gbuf.at[:, gcol(g)], gbuf.at[:, gcol(g)], g_send.at[n], g_recv.at[g], x_peer).wait_recv()
    norm(here)
    inv_msg.wait_recv()
    for cp in hid_msg:
        cp.wait_recv()
    inv_all[there, :] = jnp.broadcast_to(inv_r[:1, :], (toks, toks)).T
    norm(there)
    finish(0)
    kv_s[...] = mix[0].astype(bf)
    kv_msg = x_push(kv_s, kv_r)
    z_arrivals(2, hops[:-1])
    finish_q(0)
    z_arrivals(2, hops[-1:])
    finish_q(1)

    loaded(cos_ref, nxt + 3)
    loaded(sin_ref, nxt + 4)
    loaded(ctb.at[here], nxt + 1)
    ct_msg.wait_recv()
    cosine, sine = cos_ref[...], sin_ref[...]

    def rope(u):
        return u * cosine + pltpu.roll(u, HD // 2, 1) * sine

    def unrope(u):
        return u * cosine - pltpu.roll(u, HD // 2, 1) * sine

    kv_msg.wait_recv()
    mix_kv = mix[0] + kv_r[...].astype(f32)
    mix[0] = mix_kv
    keys = rope(mix_kv[:, :HD]).astype(bf)
    values = mix_kv[:, HD:].astype(bf)
    allowed = lax.broadcasted_iota(jnp.int32, (seq, seq), 1) <= lax.broadcasted_iota(jnp.int32, (seq, seq), 0)
    inner = jnp.zeros((seq, 1), f32)
    grad_keys = jnp.zeros((seq, HD), f32)
    grad_values = jnp.zeros((seq, HD), f32)
    gq_msg = []

    def head(n, inner, grad_keys, grad_values):
        q_msg[n].wait_recv()
        mixed = mix[1 + n, :, mycol] + qm_r[n].astype(f32)
        query = (rope(mixed) * scale).astype(bf)
        grad = ctb[:, n * HD : (n + 1) * HD]
        scores = jnp.where(allowed, nt_dot(query, keys), -1e30)
        top = jnp.max(scores, axis=1, keepdims=True)
        numbers = jnp.where(allowed, jnp.exp(scores - top), 0.0)
        norm_sum = jnp.sum(numbers, axis=1, keepdims=True)
        high = numbers.astype(bf)
        low = (numbers - high.astype(f32)).astype(bf)
        attn = ((nn_dot(high, values) + nn_dot(low, values)) / norm_sum).astype(bf)
        at_s[n] = attn
        delta = jnp.sum(grad.astype(f32) * attn.astype(f32), axis=1, keepdims=True)
        probs = numbers / norm_sum
        grad_scores = (probs * (nt_dot(grad, values) - delta)).astype(bf)
        back = (unrope(nn_dot(grad_scores, keys)) * scale).astype(bf)
        gq[n, x] = back
        gq_msg.append(x_push(gq.at[n, x], gq.at[n, x]))
        inner = inner + jnp.sum(back.astype(f32) * mixed, axis=1, keepdims=True)
        grad_keys = grad_keys + tn_dot(grad_scores, query)
        grad_values = grad_values + tn_dot(probs.astype(bf), grad)
        return inner, grad_keys, grad_values

    def to_core(q, k):
        return rcopy(tbuf.at[q, (1 - c) * chips + k], rs1.at[q, k], c_send.at[q, k], c_recv.at[q, k], c_peer)

    def to_y(q, d):
        return rcopy(ybuf.at[q, d], rs2.at[q, d], y_send.at[q, d], y_recv.at[q, d], y_peer)

    def to_z(q, d):
        return rcopy(zbuf.at[q, d - 1], rs3.at[q, d - 1], z_send.at[q, d - 1], z_recv.at[q, d - 1],
                     dev(across(d), y, c, x))

    order = ([far] if far else []) + hops[:far - 1 if far else None] + [0]
    turn = 1

    def terms(q, grads, cc):
        part = nn_dot(ntr[pl.ds(pl.multiple_of(cc * chips * rows, rows), chips * rows), :], grads)
        tbuf[q, pl.ds(cc * chips, chips)] = part.astype(bf).reshape(chips, rows, CHUNK)

    def to_side(q, k, src):
        return rcopy(src, side.at[k, q], s_send.at[k, q], s_recv.at[k, q], dev(across(1), y, c, x))

    def core_sum(q, k):
        to_core(q, k).wait_recv()
        return tbuf[q, c * chips + k].astype(f32) + rs1[q, k].astype(f32)

    def rs_terms(q, grads):
        terms(q, grads, 1 - c)
        for yy in (1 - y, y):
            for d in order:
                to_core(q, across(d) * SIDE + yy).start()
        terms(q, grads, c)

    def rs_sums(q, ds):
        for d in ds:
            part = core_sum(q, across(d) * SIDE + 1 - y)
            if q == turn and d == 0:
                to_side(q, 0, ybuf.at[q, 1]).wait_recv()
                part = part + side[0, q].astype(f32)
            ybuf[q, d] = part.astype(bf)
            if q == turn and d == 1:
                to_side(q, 0, ybuf.at[q, d]).start()
            else:
                to_y(q, d).start()

    def rs_middle(q):
        for d in order:
            part = core_sum(q, across(d) * SIDE + y)
            if q != turn or d != 1:
                to_y(q, d).wait_recv()
                part = part + rs2[q, d].astype(f32)
            if d == 0:
                mix[q, :rows, :] = part
            elif d == far:
                zbuf[q, d - 1] = part.astype(bf)
                pl.when(inner_z)(to_z(q, d).start)
                pl.when(jnp.logical_not(inner_z))(to_side(q, 1, zbuf.at[q, d - 1]).start)
            elif d == 2:
                pl.when(inner_z)(to_side(q, 1, zbuf.at[q, d - 1]).wait_recv)
                extra = jnp.where(inner_z, side[1, q].astype(f32), 0.0)
                zbuf[q, d - 1] = (part + extra).astype(bf)
                to_z(q, d).start()
            else:
                zbuf[q, d - 1] = part.astype(bf)
                to_z(q, d).start()

    block = c * chips + z * SIDE + y
    cross = c != x
    sums = []

    def rs_end(q):
        result = mix[q, :rows, :]
        for d in hops:
            if d == far:
                pl.when(inner_z)(to_z(q, d).wait_recv)
                result = result + jnp.where(inner_z, rs3[q, d - 1].astype(f32), 0.0)
            else:
                to_z(q, d).wait_recv()
                result = result + rs3[q, d - 1].astype(f32)
        prod = wbuf[q, block].astype(f32) * result
        sums.append(prod[:, :HD] + prod[:, HD:])
        dg_s[q] = result.astype(bf)
        pl.when(cross)(lambda: to_diag(q).start())
        store(q, result)

    def store(q, result):
        if q == 0:
            wg_ref[:, qcols:] = result
        else:
            for xx in range(2):
                first = (xx * half + q - 1) * HD
                wg_ref[:, first : first + HD] = result[:, xx * HD : (xx + 1) * HD]

    def to_diag(q):
        return rcopy(dg_s.at[q], dg_r.at[q], d_send.at[q], d_recv.at[q], d_peer)

    gg_copy = rcopy(gg_s, gg_r, d_send.at[chunks], d_recv.at[chunks], d_peer)

    def rs_head(n):
        gq_msg[n].wait_recv()
        rs_terms(1 + n, jnp.concatenate([gq[n, 0], gq[n, 1]], axis=1))

    inner, grad_keys, grad_values = head(0, inner, grad_keys, grad_values)
    rs_head(0)
    inner, grad_keys, grad_values = head(1, inner, grad_keys, grad_values)
    grad_keys = unrope(grad_keys)
    gkv_s[:, :HD] = grad_keys.astype(bf)
    gkv_s[:, HD:] = grad_values.astype(bf)
    gkv_msg = x_push(gkv_s, gkv_r)
    inner_all = jnp.broadcast_to(inner, (seq, HD))
    in_s[...] = inner_all.T[:8, :]
    in_msg = x_push(in_s, in_r)
    for n in range(half):
        attn_ref[:, pl.ds(pl.multiple_of((x * half + n) * HD, HD), HD)] = at_s[n, here, :]

    rs_sums(1, [d for d in order if d == 1] + [d for d in order if d > 1])
    rs_head(1)
    rs_sums(1, [0])
    rs_sums(2, order)
    gkv_msg.wait_recv()
    keys_sum = gkv_s[:, :HD].astype(f32) + gkv_r[:, :HD].astype(f32)
    values_sum = gkv_s[:, HD:].astype(f32) + gkv_r[:, HD:].astype(f32)
    gkv_all = jnp.concatenate([keys_sum, values_sum], axis=1).astype(bf)
    rs_terms(0, gkv_all)
    rs_middle(1)
    rs_sums(0, order)
    in_msg.wait_recv()
    inner = inner + jnp.broadcast_to(in_r[:1, :], (HD, seq)).T[:, :1]
    inner = inner + jnp.sum(gkv_all.astype(f32) * mix[0], axis=1, keepdims=True)
    inv = inv_all[...]
    inv_all[...] = inner * (inv * inv / width)

    gqs = [jnp.concatenate([gq[n, 0], gq[n, 1]], axis=1) for n in range(half)]
    gi_msg = []
    for p in range(PIECES):
        out = jnp.zeros((seq, lanes), f32)
        for q in range(chunks):
            w = wbuf[q, p * span : (p + 1) * span].reshape(lanes, CHUNK)
            out = out + nt_dot(gkv_all if q == 0 else gqs[q - 1], w)
        gain = gbuf[:, p * lanes : (p + 1) * lanes]
        gi_s[p] = (gain * out * inv[:, :1] - hx[p].astype(f32) * inv_all[:, :1]).astype(bf)
        gi_msg.append(x_push(gi_s.at[p, there], gi_r.at[p]))
    at_msg = x_push(at_s.at[:, there], at_r)

    queue = list(range(1, chunks)) + [0]
    for p in range(PIECES):
        for b in range(span):
            j = p * span + b
            gin_ref[:, pl.ds(pl.multiple_of((2 * j + x) * rows, rows), rows)] = gi_s[p, here, b * rows : (b + 1) * rows]
    for n in range(1, chunks):
        rs_middle(queue[n])
        rs_end(queue[n - 1])
    rs_end(queue[-1])
    lanes_sum = sums[0]
    for part in sums[1:]:
        lanes_sum = lanes_sum + part
    gg = jnp.sum(lanes_sum.T, axis=0, keepdims=True) / gbuf[:, gcol(block)]
    gg_ref[...] = gg
    gg_s[...] = gg
    pl.when(cross)(lambda: gg_copy.start())

    at_msg.wait_recv()
    for n in range(half):
        attn_ref[:, pl.ds(pl.multiple_of(((1 - x) * half + n) * HD, HD), HD)] = at_r[n]
    for p in range(PIECES):
        gi_msg[p].wait_recv()
        for b in range(span):
            j = p * span + b
            gin_ref[:, pl.ds(pl.multiple_of((2 * j + 1 - x) * rows, rows), rows)] = gi_r[p, :, b * rows : (b + 1) * rows]

    for cp, cond in sent:
        if cond is None:
            cp.wait_send()
        else:
            pl.when(cond)(cp.wait_send)
    for cp in messages:
        cp.wait_send()
    for n, e in enumerate(plane):
        rcopy(gbuf.at[:, gcol(own)], gbuf.at[:, gcol(own)], g_send.at[n], g_recv.at[own], x_peer).wait_send()
    for q in range(chunks):
        for k in range(chips):
            to_core(q, k).wait_send()
        for d in range(nz):
            if q != turn or d != 1:
                to_y(q, d).wait_send()
            else:
                to_side(q, 0, ybuf.at[q, d]).wait_send()
        for d in hops:
            if d == far:
                pl.when(inner_z)(to_z(q, d).wait_send)
                pl.when(jnp.logical_not(inner_z))(to_side(q, 1, zbuf.at[q, d - 1]).wait_send)
            else:
                to_z(q, d).wait_send()

    @pl.when(cross)
    def _():
        for q in queue:
            to_diag(q).wait_recv()
            store(q, dg_r[q].astype(f32))
        gg_copy.wait_recv()
        gg_ref[...] = gg_r[...]
        for q in range(chunks):
            to_diag(q).wait_send()
        gg_copy.wait_send()


def copy_kernel(*refs):
    sems = refs[8]
    copies = [pltpu.make_async_copy(refs[k], refs[4 + k], sems.at[k]) for k in range(4)]
    for cp in copies:
        cp.start()
    for cp in copies:
        cp.wait()


def fused(n_inter, hidden_in, norm_gain, qkv_weight, attn_cotangent):
    toks, width = hidden_in.shape[1:]
    rows, cols = qkv_weight.shape
    nz = n_inter // (CORES * SIDE)
    chips = nz * SIDE
    seq, half, chunks = 2 * toks, HEADS // 2, cols // CHUNK
    lanes = n_inter // PIECES * rows
    freqs = rope_base ** (-np.arange(HD // 2, dtype=np.float32) / np.float32(HD // 2))
    angles = (np.arange(seq, dtype=np.float32)[:, None] * freqs.astype(np.float32)[None, :]).astype(np.float32)
    cosine = np.concatenate([np.cos(angles)] * 2, axis=1).astype(np.float32)
    sine = np.concatenate([-np.sin(angles), np.sin(angles)], axis=1).astype(np.float32)
    bf, f32, dma = jnp.bfloat16, jnp.float32, pltpu.SemaphoreType.DMA
    vmem = pl.BlockSpec(memory_space=pltpu.VMEM)
    hbm = pl.BlockSpec(memory_space=pltpu.HBM)
    V = pltpu.VMEM
    n_msgs = 2 * PIECES + 2 * half + 6
    ins = (hidden_in[0], norm_gain[None], qkv_weight, attn_cotangent[0], jnp.asarray(cosine), jnp.asarray(sine))
    attn, gin, wg, gg = pl.pallas_call(
        functools.partial(fused_kernel, n_inter),
        out_shape=(V((toks, HEADS * HD), bf), V((toks, width), bf), V((rows, cols), f32), V((1, rows), f32)),
        in_specs=[hbm] * 6,
        out_specs=(vmem,) * 4,
        scratch_shapes=[
            V((chunks, n_inter, rows, CHUNK), bf),
            V((1, n_inter * rows), f32),
            V((1, rows), bf),
            V((PIECES, seq, lanes), bf),
            V((PIECES, toks, lanes), bf),
            V((PIECES, seq, lanes), bf),
            V((n_inter * rows, seq), bf),
            V((seq, HD), f32),
            V((8, toks), f32),
            V((8, toks), f32),
            V((seq, half * HD), bf),
            V((toks, half * HD), bf),
            V((seq, HD), f32),
            V((seq, HD), f32),
            V((chunks, seq, CHUNK), f32),
            V((seq, CHUNK), bf),
            V((seq, CHUNK), bf),
            V((half, seq, HD), bf),
            V((half, seq, HD), bf),
            V((half, 2, seq, HD), bf),
            V((seq, CHUNK), bf),
            V((seq, CHUNK), bf),
            V((8, seq), f32),
            V((8, seq), f32),
            V((half, seq, HD), bf),
            V((half, toks, HD), bf),
            V((PIECES, seq, lanes), bf),
            V((PIECES, toks, lanes), bf),
            V((chunks, n_inter, rows, CHUNK), bf),
            V((chunks, chips, rows, CHUNK), bf),
            V((chunks, nz, rows, CHUNK), bf),
            V((chunks, nz, rows, CHUNK), bf),
            V((chunks, nz - 1, rows, CHUNK), bf),
            V((chunks, nz - 1, rows, CHUNK), bf),
            V((2, chunks, rows, CHUNK), bf),
            V((chunks, rows, CHUNK), bf),
            V((chunks, rows, CHUNK), bf),
            V((1, rows), f32),
            V((1, rows), f32),
            dma((8 + half,)),
            dma((chunks, 2 * nz + chips + 1)), dma((chunks, n_inter)),
            dma((n_inter,)), dma((n_inter,)),
            dma((n_msgs,)), dma((n_msgs,)),
            dma((chunks, chips)), dma((chunks, chips)),
            dma((chunks, nz)), dma((chunks, nz)),
            dma((chunks, nz - 1)), dma((chunks, nz - 1)),
            dma((2, chunks)), dma((2, chunks)),
            dma((chunks + 1,)), dma((chunks + 1,)),
        ],
        compiler_params=pltpu.CompilerParams(
            collective_id=0, has_side_effects=True, vmem_limit_bytes=32 * 2**20
        ),
    )(*[pltpu.with_memory_space_constraint(a, pltpu.HBM) for a in ins])
    outs = (attn, gin, wg, gg)
    attn, gin, wg, gg = pl.pallas_call(
        copy_kernel,
        out_shape=tuple(jax.ShapeDtypeStruct(o.shape, o.dtype) for o in outs),
        in_specs=[vmem] * 4,
        out_specs=(hbm,) * 4,
        scratch_shapes=[dma((4,))],
        compiler_params=pltpu.CompilerParams(vmem_limit_bytes=2**20),
    )(*[pltpu.with_memory_space_constraint(o, pltpu.VMEM) for o in outs])
    return attn[None], gin[None], wg, gg[0]


def solution(mesh):
    n_inter, n_intra = mesh.shape["inter"], mesh.shape["intra"]

    def body(hidden_in, norm_gain, qkv_weight, attn_cotangent):
        nz = n_inter // (CORES * SIDE)
        fits = n_intra == 2 and n_inter % (CORES * SIDE) == 0 and nz > 1 and nz & (nz - 1) == 0
        fits = fits and qkv_weight.shape[0] == HD and hidden_in.shape[0] == 1
        fits = fits and hidden_in.shape[1] == HD and n_inter % PIECES == 0 and HEADS == 4 and nz == 4
        if fits:
            return fused(n_inter, hidden_in, norm_gain, qkv_weight, attn_cotangent)
        return local(hidden_in, norm_gain, qkv_weight, attn_cotangent)

    return jax.shard_map(
        body,
        mesh=mesh,
        in_specs=(
            P("inter", "intra", None),
            P(("inter", "intra")),
            P(("inter", "intra"), None),
            P("inter", "intra", None),
        ),
        out_specs=(
            P("inter", "intra", None),
            P("inter", "intra", None),
            P(("intra", "inter"), None),
            P(("intra", "inter")),
        ),
        check_vma=False,
    )
```

```python
import functools
import jax
import jax.numpy as jnp
import numpy as np
from jax import lax
from jax.experimental import pallas as pl
from jax.experimental.pallas import tpu as pltpu
from jax.sharding import PartitionSpec as P

HD = 128
HEADS = 4


eps_norm = 1e-05
rope_base = 500000.0


def rope_tables(positions, head_size):
    half_size = head_size // 2
    freqs = rope_base ** (-jnp.arange(half_size, dtype=jnp.float32) / half_size)
    angles = positions.astype(jnp.float32)[:, None] * freqs[None, :]
    return (jnp.cos(angles), jnp.sin(angles))


def rotate(values_in, cosine, sine):
    half_size = values_in.shape[-1] // 2
    first, second = (values_in[..., :half_size], values_in[..., half_size:])
    return jnp.concatenate(
        [first * cosine - second * sine, second * cosine + first * sine], axis=-1
    )


def unrotate(grad_out, cosine, sine):
    half_size = grad_out.shape[-1] // 2
    first, second = (grad_out[..., :half_size], grad_out[..., half_size:])
    return jnp.concatenate(
        [first * cosine + second * sine, second * cosine - first * sine], axis=-1
    )


def forward_fold(query_rows, row_pos):

    def forward_advance(carry, piece, start):
        row_top, row_total, weighted = carry
        key_part, value_part = piece
        scores = jnp.einsum("qd,kd->qk", query_rows, key_part, preferred_element_type=jnp.float32)
        key_pos = jnp.arange(key_part.shape[0], dtype=jnp.int32)
        allowed = key_pos[None, :] <= row_pos[:, None]
        scores = jnp.where(allowed, scores, -1e30)
        new_top = jnp.maximum(row_top, jnp.max(scores, axis=1))
        numbers = jnp.where(allowed, jnp.exp(scores - new_top[:, None]), 0.0)
        row_total = jnp.sum(numbers, axis=1)
        weighted = jnp.dot(
            numbers,
            value_part.astype(jnp.float32),
            precision=lax.Precision.HIGHEST,
            preferred_element_type=jnp.float32,
        )
        return (new_top, row_total, weighted)

    return forward_advance


def query_grad_fold(query_rows, row_pos, grad_flat, log_total, row_delta):

    def query_advance(grad_query, piece, start):
        key_part, value_part = piece
        scores = jnp.einsum("qd,kd->qk", query_rows, key_part, preferred_element_type=jnp.float32)
        key_pos = jnp.arange(key_part.shape[0], dtype=jnp.int32)
        allowed = key_pos[None, :] <= row_pos[:, None]
        probs = jnp.where(
            allowed, jnp.exp(jnp.where(allowed, scores, -1e30) - log_total[:, None]), 0.0
        )
        grad_probs = jnp.einsum(
            "qd,kd->qk", grad_flat, value_part, preferred_element_type=jnp.float32
        )
        grad_scores = (probs * (grad_probs - row_delta[:, None])).astype(jnp.bfloat16)
        return jnp.dot(grad_scores, key_part, preferred_element_type=jnp.float32)

    return query_advance


def key_grad_fold(key_rows, value_rows, key_pos, log_all, delta_all, heads_count):

    def key_advance(carry, piece, start):
        query_part, attn_grad_part = piece
        count = query_part.shape[0]
        scores = jnp.einsum("qd,kd->qk", query_part, key_rows, preferred_element_type=jnp.float32)
        query_pos = jnp.arange(count, dtype=jnp.int32) // heads_count
        allowed = key_pos[None, :] <= query_pos[:, None]
        probs = jnp.where(
            allowed, jnp.exp(jnp.where(allowed, scores, -1e30) - log_all[:, None]), 0.0
        )
        grad_values = jnp.einsum(
            "qk,qd->kd",
            probs.astype(jnp.bfloat16),
            attn_grad_part,
            preferred_element_type=jnp.float32,
        )
        grad_probs = jnp.einsum(
            "qd,kd->qk", attn_grad_part, value_rows, preferred_element_type=jnp.float32
        )
        grad_scores = (probs * (grad_probs - delta_all[:, None])).astype(jnp.bfloat16)
        grad_keys = jnp.einsum(
            "qk,qd->kd", grad_scores, query_part, preferred_element_type=jnp.float32
        )
        return (grad_keys, grad_values)

    return key_advance


def local(hidden_in, norm_gain, qkv_weight, attn_cotangent):
    rows_in = hidden_in[0]
    grad_attn = attn_cotangent[0]
    tokens_here = rows_in.shape[0]
    width = rows_in.shape[1]
    head_size = HD
    heads_count = HEADS
    qcols = heads_count * head_size
    scale = head_size ** (-0.5)
    weight_group, gain_group = (
        lax.all_gather(qkv_weight, "intra", axis=0, tiled=True),
        lax.all_gather(norm_gain, "intra", axis=0, tiled=True),
    )
    weight_full, gain_full = (
        lax.all_gather(weight_group, "inter", axis=0, tiled=True),
        lax.all_gather(gain_group, "inter", axis=0, tiled=True),
    )
    query_pos = lax.axis_index("intra") * tokens_here + jnp.arange(tokens_here, dtype=jnp.int32)
    row_pos = jnp.broadcast_to(query_pos[:, None], (tokens_here, heads_count)).reshape(
        tokens_here * heads_count
    )
    cosine, sine = rope_tables(query_pos, head_size)
    wide_rows = rows_in.astype(jnp.float32)
    inv_rms = lax.rsqrt(jnp.mean(wide_rows * wide_rows, axis=1, keepdims=True) + eps_norm)
    normed = (wide_rows * inv_rms * gain_full.astype(jnp.float32)[None, :]).astype(jnp.bfloat16)
    mixed = jnp.dot(normed, weight_full, preferred_element_type=jnp.float32)
    query_rows = (
        (
            rotate(
                mixed[:, :qcols].reshape(tokens_here, heads_count, head_size),
                cosine[:, None, :],
                sine[:, None, :],
            )
            * scale
        )
        .astype(jnp.bfloat16)
        .reshape(tokens_here * heads_count, head_size)
    )
    key_rows = rotate(mixed[:, qcols : qcols + head_size], cosine, sine).astype(jnp.bfloat16)
    value_rows = mixed[:, qcols + head_size :].astype(jnp.bfloat16)
    grad_flat = grad_attn.reshape(tokens_here * heads_count, head_size)
    flat_rows = tokens_here * heads_count
    forward_step = forward_fold(query_rows, row_pos)
    start_carry = (
        jnp.full((flat_rows,), -1e30, jnp.float32),
        jnp.zeros((flat_rows,), jnp.float32),
        jnp.zeros((flat_rows, head_size), jnp.float32),
    )
    row_top, row_total, weighted = forward_step(
        start_carry,
        (
            lax.all_gather(key_rows, "intra", axis=0, tiled=True),
            lax.all_gather(value_rows, "intra", axis=0, tiled=True),
        ),
        jnp.int32(0),
    )
    attn_flat = (weighted / row_total[:, None]).astype(jnp.bfloat16)
    log_total = row_top + jnp.log(row_total)
    row_delta = jnp.sum(grad_flat.astype(jnp.float32) * attn_flat.astype(jnp.float32), axis=1)
    query_step = query_grad_fold(query_rows, row_pos, grad_flat, log_total, row_delta)
    grad_query = query_step(
        jnp.zeros((flat_rows, head_size), jnp.float32),
        (
            lax.all_gather(key_rows, "intra", axis=0, tiled=True),
            lax.all_gather(value_rows, "intra", axis=0, tiled=True),
        ),
        jnp.int32(0),
    )
    log_all, delta_all = (
        lax.all_gather(log_total, "intra", axis=0, tiled=True),
        lax.all_gather(row_delta, "intra", axis=0, tiled=True),
    )
    key_step = key_grad_fold(key_rows, value_rows, query_pos, log_all, delta_all, heads_count)
    grad_keys, grad_values = key_step(
        (
            jnp.zeros((tokens_here, head_size), jnp.float32),
            jnp.zeros((tokens_here, head_size), jnp.float32),
        ),
        (
            lax.all_gather(query_rows, "intra", axis=0, tiled=True),
            lax.all_gather(grad_flat, "intra", axis=0, tiled=True),
        ),
        jnp.int32(0),
    )
    query_back = (
        unrotate(
            grad_query.reshape(tokens_here, heads_count, head_size),
            cosine[:, None, :],
            sine[:, None, :],
        )
        * scale
    ).reshape(tokens_here, qcols)
    grad_mixed = jnp.concatenate(
        [query_back, unrotate(grad_keys, cosine, sine), grad_values], axis=1
    ).astype(jnp.bfloat16)
    weight_back, gain_back = (weight_full, gain_full)
    gain_wide = gain_back.astype(jnp.float32)[None, :]
    grad_normed = jnp.einsum(
        "tc,dc->td", grad_mixed, weight_back, preferred_element_type=jnp.float32
    )
    inner = jnp.sum(grad_normed * gain_wide * wide_rows, axis=1, keepdims=True)
    grad_rows = (
        gain_wide * grad_normed * inv_rms - wide_rows * inv_rms**3 / width * inner
    ).astype(jnp.bfloat16)
    gain_term = jnp.sum(grad_normed * wide_rows * inv_rms, axis=0)
    normed_cols = lax.all_to_all(normed, "intra", split_axis=1, concat_axis=0, tiled=True)
    group_term = lax.dot_general(
        normed_cols,
        lax.all_gather(grad_mixed, "intra", axis=0, tiled=True),
        (((0,), (0,)), ((), ())),
        preferred_element_type=jnp.float32,
    )
    term_low = lax.optimization_barrier(group_term.astype(jnp.bfloat16))
    gain_sums = lax.psum_scatter(gain_term, "intra", scatter_dimension=0, tiled=True)
    weight_grad, gain_grad = (
        lax.psum_scatter(term_low.astype(jnp.float32), "inter", scatter_dimension=0, tiled=True),
        lax.psum_scatter(gain_sums, "inter", scatter_dimension=0, tiled=True),
    )
    return (attn_flat.reshape(tokens_here, qcols)[None], grad_rows[None], weight_grad, gain_grad)

MESH = pl.DeviceIdType.MESH
CORES = 2
SIDE = 2
PIECES = 4
CHUNK = 2 * HD
SPLIT = 1
LAG = 1
Z_AHEAD = 3
Y_AHEAD = 3
RELAYED = (0, 1, 2)
MERGED = (1, 2)


def nt_dot(a, b):
    return lax.dot_general(a, b, (((1,), (1,)), ((), ())), preferred_element_type=jnp.float32)


def tn_dot(a, b):
    return lax.dot_general(a, b, (((0,), (0,)), ((), ())), preferred_element_type=jnp.float32)


def nn_dot(a, b):
    return jnp.dot(a, b, preferred_element_type=jnp.float32)


def fused_kernel(
    n_inter,
    hid_ref, gain_ref, w_ref, ct_ref, cos_hbm, sin_hbm,
    attn_ref, gin_ref, wg_ref, gg_ref,
    wbuf, gbuf, gain_in, hx, hs, nbuf, ntr, inv_all, inv_s, inv_r, ctb, cts, cos_ref, sin_ref,
    mix, kv_s, kv_r, qm_s, qm_r, gq, gkv_s, gkv_r, in_s, in_r, at_s, at_r, gi_s, gi_r,
    tbuf, rs1, ybuf, rs2, zbuf, rs3, side, dg_s, dg_r, gg_s, gg_r,
    ld_sem, ag_send, ag_recv, g_send, g_recv, x_send, x_recv,
    c_send, c_recv, y_send, y_recv, z_send, z_recv, s_send, s_recv, d_send, d_recv,
):
    i = lax.axis_index("inter")
    x = lax.axis_index("intra")
    nz = n_inter // (CORES * SIDE)
    c = lax.rem(i, CORES)
    y = lax.rem(i // CORES, SIDE)
    z = i // (CORES * SIDE)
    toks, width = hid_ref.shape
    rows, cols = w_ref.shape
    seq = 2 * toks
    qcols = HEADS * HD
    chips = nz * SIDE
    chunks = cols // CHUNK
    span = n_inter // PIECES
    lanes = span * rows
    scale = HD ** (-0.5)
    f32, bf = jnp.float32, jnp.bfloat16

    def dev(zz, yy, cc, xx):
        return ((zz * SIDE + yy) * CORES + cc, xx)

    def slot(zz, yy, cc):
        return (zz * SIDE + yy) * CORES + cc

    def across(d):
        zz, bit = z, 1
        while bit < nz:
            if d & bit:
                zz = zz + bit - 2 * bit * lax.rem(z // bit, 2)
            bit *= 2
        return zz

    hops = list(range(1, nz))
    x_peer = dev(z, y, c, 1 - x)
    y_peer = dev(z, 1 - y, c, x)
    c_peer = dev(z, y, 1 - c, x)
    d_peer = dev(z, y, 1 - c, 1 - x)
    plane = [(d, yy, cc) for d in range(nz) for yy in (0, 1) for cc in (0, 1) if d or yy or cc]

    def plane_dev(e):
        d, yy, cc = e
        return (across(d), y + yy - 2 * yy * y, c + cc - 2 * cc * c)

    own = slot(z, y, c)
    here = pl.ds(pl.multiple_of(x * toks, toks), toks)
    there = pl.ds(pl.multiple_of((1 - x) * toks, toks), toks)

    def rcopy(src, dst, ss, rs, device):
        return pltpu.make_async_remote_copy(
            src_ref=src, dst_ref=dst, send_sem=ss, recv_sem=rs, device_id=device, device_id_type=MESH
        )

    barrier = pltpu.get_barrier_semaphore()
    peers = [dev(*plane_dev(e), x) for e in plane] + [x_peer, d_peer]
    for peer in peers:
        pl.semaphore_signal(barrier, inc=1, device_id=peer, device_id_type=MESH)

    def load(src, dst, k):
        pltpu.make_async_copy(src, dst, ld_sem.at[k]).start()

    def loaded(dst, k):
        pltpu.make_async_copy(dst, dst, ld_sem.at[k]).wait()

    for p in range(PIECES):
        for b in range(span):
            j = p * span + b
            mine = pl.ds(pl.multiple_of((2 * j + x) * rows, rows), rows)
            other = pl.ds(pl.multiple_of((2 * j + 1 - x) * rows, rows), rows)
            load(hid_ref.at[:, mine], hx.at[p, here, b * rows : (b + 1) * rows], 0)
            load(hid_ref.at[:, other], hs.at[p, :, b * rows : (b + 1) * rows], 1)
    load(w_ref.at[:, qcols:], wbuf.at[0, own], 2)
    half = HEADS // 2
    for n in range(half):
        for xx in range(2):
            first = (xx * half + n) * HD
            load(w_ref.at[:, first : first + HD], wbuf.at[1 + n, own, :, xx * HD : (xx + 1) * HD], 3 + n)
    nxt = 3 + half
    load(gain_ref, gain_in, nxt)
    load(ct_ref.at[:, pl.ds(pl.multiple_of(x * half * HD, HD), half * HD)], ctb.at[here], nxt + 1)
    load(ct_ref.at[:, pl.ds(pl.multiple_of((1 - x) * half * HD, HD), half * HD)], cts, nxt + 2)
    load(cos_hbm, cos_ref, nxt + 3)
    load(sin_hbm, sin_ref, nxt + 4)

    loaded(gain_in, nxt)
    gcol = lambda g: pl.ds(pl.multiple_of(g * rows, rows), rows)
    gbuf[:, gcol(own)] = gain_in[...].astype(f32)
    loaded(hx.at[:, here], 0)
    loaded(hs, 1)
    total = jnp.zeros((toks, 1), f32)
    for p in range(PIECES):
        a = hx[p, here, :].astype(f32)
        b = hs[p].astype(f32)
        total = total + jnp.sum(a * a + b * b, axis=1, keepdims=True)
    inv = jnp.broadcast_to(lax.rsqrt(total / width + eps_norm), (toks, HD))
    inv_all[here, :] = inv
    inv_s[...] = inv.T[:8, :]
    for q in range(chunks):
        loaded(wbuf.at[q, own], 2 + q)
    loaded(cts, nxt + 2)
    pl.semaphore_wait(barrier, len(peers))

    inner_z = jnp.logical_and(z > 0, z < nz - 1)
    far = nz - 1
    steps = chunks * SPLIT
    spare = steps - 1

    def ag(t, g, link, device):
        part = wbuf.at[t // SPLIT, g, pl.ds(t % SPLIT * (rows // SPLIT), rows // SPLIT)]
        return rcopy(part, part, ag_send.at[t, link], ag_recv.at[t, g], device)

    def arrive(t, g):
        ag(t, g, 0, x_peer).wait_recv()

    def x_copy(k, src, dst):
        return rcopy(src, dst, x_send.at[k], x_recv.at[k], x_peer)

    y_link = nz
    c_link = 2 * nz
    spare_link = 2 * nz + chips
    sent = []

    def push(t, g, link, device, cond=None):
        cp = ag(t, g, link, device)
        sent.append((cp, cond))
        if cond is None:
            cp.start()
        else:
            pl.when(cond)(cp.start)

    for n, e in enumerate(plane):
        rcopy(gbuf.at[:, gcol(own)], gbuf.at[:, gcol(own)], g_send.at[n], g_recv.at[own],
              dev(*plane_dev(e), x)).start()
    def own_z(t):
        if t < steps:
            for d in hops[::-1]:
                push(t, own, d, dev(across(d), y, c, x), inner_z if d == far and t // SPLIT in RELAYED else None)

    def own_y(t):
        if t < steps:
            push(t, own, y_link, y_peer)
            push(t, own, c_link, c_peer)

    for t in range(max(Z_AHEAD, Y_AHEAD)):
        if t < Z_AHEAD:
            own_z(t)
        if t < Y_AHEAD:
            own_y(t)
    messages = []

    def x_push(src, dst):
        cp = x_copy(len(messages), src, dst)
        cp.start()
        messages.append(cp)
        return cp

    inv_msg = x_push(inv_s, inv_r)
    hid_msg = [x_push(hs.at[p], hx.at[p, here]) for p in range(PIECES)]
    ct_msg = x_push(cts, ctb.at[here])

    def near(n):
        if n < 2:
            return across(n)
        return jnp.where(inner_z, across(nz + 1 - n), across(n))

    def z_arrivals(t):
        for n in hops:
            g = slot(near(n), y, c)
            arrive(t, g)
            if n == far and t // SPLIT in RELAYED:
                push(t, g, 0, dev(across(1), y, c, x), inner_z)
            if t != spare or n != 1:
                push(t, g, y_link + n, y_peer)
            push(t, g, c_link + n, c_peer)
        own_z(t + Z_AHEAD)
        own_y(t + Y_AHEAD)

    def y_own(t):
        g = slot(z, 1 - y, c)
        arrive(t, g)
        if t == spare:
            push(t, g, spare_link, dev(across(1), y, c, x))
        push(t, g, c_link + nz, c_peer)

    def y_arrivals(t):
        for n in hops:
            g = slot(near(n), 1 - y, c)
            arrive(t, g)
            push(t, g, c_link + nz + n, c_peer)

    def c_arrivals(q):
        for t in range(q * SPLIT, (q + 1) * SPLIT):
            for d in range(nz):
                for yy in (y, 1 - y):
                    arrive(t, slot(across(d), yy, 1 - c))

    def norm(which):
        scaled = inv_all[which, :1]
        for p in range(PIECES):
            value = hx[p, which, :].astype(f32) * scaled * gbuf[:, p * lanes : (p + 1) * lanes]
            value = value.astype(bf)
            nbuf[p, which, :] = value
            ntr[p * lanes : (p + 1) * lanes, which] = value.T

    def partial(q):
        out = [jnp.zeros((toks, CHUNK), f32)] * 2
        for p in range(PIECES):
            w = wbuf[q, p * span : (p + 1) * span].reshape(lanes, CHUNK)
            out = [o + nn_dot(nbuf[p, r * toks : (r + 1) * toks, :], w) for r, o in enumerate(out)]
        for r, o in enumerate(out):
            mix[q, r * toks : (r + 1) * toks, :] = o

    mycol = pl.ds(pl.multiple_of(x * HD, HD), HD)
    itscol = pl.ds(pl.multiple_of((1 - x) * HD, HD), HD)

    q_msg = []

    def send_q(n):
        c_arrivals(1 + n)
        partial(1 + n)
        qm_s[n] = mix[1 + n, :, itscol].astype(bf)
        q_msg.append(x_push(qm_s.at[n], qm_r.at[n]))

    for t in range(steps + LAG):
        if t < steps:
            z_arrivals(t)
            y_own(t)
        if t == LAG:
            for n, e in enumerate(plane):
                g = slot(*plane_dev(e))
                rcopy(gbuf.at[:, gcol(g)], gbuf.at[:, gcol(g)], g_send.at[n], g_recv.at[g], x_peer).wait_recv()
            norm(here)
        if t >= LAG:
            y_arrivals(t - LAG)
            if t - LAG == SPLIT - 1:
                inv_msg.wait_recv()
                for cp in hid_msg:
                    cp.wait_recv()
                inv_all[there, :] = jnp.broadcast_to(inv_r[:1, :], (toks, toks)).T
                norm(there)
                c_arrivals(0)
                partial(0)
                kv_s[...] = mix[0].astype(bf)
                kv_msg = x_push(kv_s, kv_r)
            if t - LAG == 2 * SPLIT - 1:
                send_q(0)

    loaded(cos_ref, nxt + 3)
    loaded(sin_ref, nxt + 4)
    loaded(ctb.at[here], nxt + 1)
    ct_msg.wait_recv()
    cosine, sine = cos_ref[...], sin_ref[...]

    def rope(u):
        return u * cosine + pltpu.roll(u, HD // 2, 1) * sine

    def unrope(u):
        return u * cosine - pltpu.roll(u, HD // 2, 1) * sine

    kv_msg.wait_recv()
    mix_kv = mix[0] + kv_r[...].astype(f32)
    mix[0] = mix_kv
    keys = rope(mix_kv[:, :HD]).astype(bf)
    values = mix_kv[:, HD:].astype(bf)
    allowed = lax.broadcasted_iota(jnp.int32, (seq, seq), 1) <= lax.broadcasted_iota(jnp.int32, (seq, seq), 0)
    inner = jnp.zeros((seq, 1), f32)
    grad_keys = jnp.zeros((seq, HD), f32)
    grad_values = jnp.zeros((seq, HD), f32)
    gq_msg = []

    def head(n, inner, grad_keys, grad_values):
        q_msg[n].wait_recv()
        mixed = mix[1 + n, :, mycol] + qm_r[n].astype(f32)
        query = (rope(mixed) * scale).astype(bf)
        grad = ctb[:, n * HD : (n + 1) * HD]
        scores = jnp.where(allowed, nt_dot(query, keys), -1e30)
        top = jnp.max(scores, axis=1, keepdims=True)
        numbers = jnp.where(allowed, jnp.exp(scores - top), 0.0)
        norm_sum = jnp.sum(numbers, axis=1, keepdims=True)
        high = numbers.astype(bf)
        low = (numbers - high.astype(f32)).astype(bf)
        attn = ((nn_dot(high, values) + nn_dot(low, values)) / norm_sum).astype(bf)
        at_s[n] = attn
        delta = jnp.sum(grad.astype(f32) * attn.astype(f32), axis=1, keepdims=True)
        probs = numbers / norm_sum
        grad_scores = (probs * (nt_dot(grad, values) - delta)).astype(bf)
        back = (unrope(nn_dot(grad_scores, keys)) * scale).astype(bf)
        gq[n, x] = back
        gq_msg.append(x_push(gq.at[n, x], gq.at[n, x]))
        inner = inner + jnp.sum(back.astype(f32) * mixed, axis=1, keepdims=True)
        grad_keys = grad_keys + tn_dot(grad_scores, query)
        grad_values = grad_values + tn_dot(probs.astype(bf), grad)
        return inner, grad_keys, grad_values

    def to_core(q, k):
        return rcopy(tbuf.at[q, (1 - c) * chips + k], rs1.at[q, k], c_send.at[q, k], c_recv.at[q, k], c_peer)

    def to_y(q, d):
        return rcopy(ybuf.at[q, d], rs2.at[q, d], y_send.at[q, d], y_recv.at[q, d], y_peer)

    def to_z(q, d):
        return rcopy(zbuf.at[q, d - 1], rs3.at[q, d - 1], z_send.at[q, d - 1], z_recv.at[q, d - 1],
                     dev(across(d), y, c, x))

    order = [far, 1, 2, 0]
    turn = 1

    def terms(q, grads, cc):
        part = nn_dot(ntr[pl.ds(pl.multiple_of(cc * chips * rows, rows), chips * rows), :], grads)
        tbuf[q, pl.ds(cc * chips, chips)] = part.astype(bf).reshape(chips, rows, CHUNK)

    def to_side(k, src):
        return rcopy(src, side.at[k], s_send.at[k], s_recv.at[k], dev(across(1), y, c, x))

    def core_sum(q, k):
        to_core(q, k).wait_recv()
        return tbuf[q, c * chips + k].astype(f32) + rs1[q, k].astype(f32)

    def rs_terms(q, grads):
        terms(q, grads, 1 - c)
        for yy in (1 - y, y):
            for d in order:
                to_core(q, across(d) * SIDE + yy).start()
        terms(q, grads, c)

    def rs_sums(q, ds):
        for d in ds:
            part = core_sum(q, across(d) * SIDE + 1 - y)
            if q == turn and d == 0:
                to_side(0, ybuf.at[q, 1]).wait_recv()
                part = part + side[0].astype(f32)
            ybuf[q, d] = part.astype(bf)
            if q == turn and d == 1:
                to_side(0, ybuf.at[q, d]).start()
            else:
                to_y(q, d).start()

    def rs_middle(q, ds):
        for d in ds:
            part = core_sum(q, across(d) * SIDE + y)
            if q != turn or d != 1:
                to_y(q, d).wait_recv()
                part = part + rs2[q, d].astype(f32)
            if d == 0:
                mix[q, :rows, :] = part
            elif d == far and q in MERGED:
                zbuf[q, d - 1] = part.astype(bf)
                pl.when(inner_z)(to_z(q, d).start)
                pl.when(jnp.logical_not(inner_z))(to_side(q, zbuf.at[q, d - 1]).start)
            elif d == 2 and q in MERGED:
                pl.when(inner_z)(to_side(q, zbuf.at[q, d - 1]).wait_recv)
                extra = jnp.where(inner_z, side[q].astype(f32), 0.0)
                zbuf[q, d - 1] = (part + extra).astype(bf)
                to_z(q, d).start()
            else:
                zbuf[q, d - 1] = part.astype(bf)
                to_z(q, d).start()

    block = c * chips + z * SIDE + y
    cross = c != x
    sums = []

    def rs_end(q):
        result = mix[q, :rows, :]
        for d in hops:
            if d == far and q in MERGED:
                pl.when(inner_z)(to_z(q, d).wait_recv)
                result = result + jnp.where(inner_z, rs3[q, d - 1].astype(f32), 0.0)
            else:
                to_z(q, d).wait_recv()
                result = result + rs3[q, d - 1].astype(f32)
        prod = wbuf[q, block].astype(f32) * result
        sums.append(prod[:, :HD] + prod[:, HD:])
        dg_s[q] = result.astype(bf)
        pl.when(cross)(lambda: to_diag(q).start())
        store(q, result)

    def store(q, result):
        if q == 0:
            wg_ref[:, qcols:] = result
        else:
            for xx in range(2):
                first = (xx * half + q - 1) * HD
                wg_ref[:, first : first + HD] = result[:, xx * HD : (xx + 1) * HD]

    def to_diag(q):
        return rcopy(dg_s.at[q], dg_r.at[q], d_send.at[q], d_recv.at[q], d_peer)

    gg_copy = rcopy(gg_s, gg_r, d_send.at[chunks], d_recv.at[chunks], d_peer)

    def rs_head(n):
        gq_msg[n].wait_recv()
        rs_terms(1 + n, jnp.concatenate([gq[n, 0], gq[n, 1]], axis=1))

    inner, grad_keys, grad_values = head(0, inner, grad_keys, grad_values)
    send_q(1)
    rs_head(0)
    inner, grad_keys, grad_values = head(1, inner, grad_keys, grad_values)
    grad_keys = unrope(grad_keys)
    gkv_s[:, :HD] = grad_keys.astype(bf)
    gkv_s[:, HD:] = grad_values.astype(bf)
    gkv_msg = x_push(gkv_s, gkv_r)
    inner_all = jnp.broadcast_to(inner, (seq, HD))
    in_s[...] = inner_all.T[:8, :]
    in_msg = x_push(in_s, in_r)
    at_msg = x_push(at_s.at[:, there], at_r)
    for n in range(half):
        attn_ref[:, pl.ds(pl.multiple_of((x * half + n) * HD, HD), HD)] = at_s[n, here, :]

    rs_sums(1, [d for d in order if d == 1] + [d for d in order if d > 1])
    rs_head(1)
    rs_sums(1, [0])
    rs_sums(2, order)
    gkv_msg.wait_recv()
    keys_sum = gkv_s[:, :HD].astype(f32) + gkv_r[:, :HD].astype(f32)
    values_sum = gkv_s[:, HD:].astype(f32) + gkv_r[:, HD:].astype(f32)
    gkv_all = jnp.concatenate([keys_sum, values_sum], axis=1).astype(bf)
    rs_terms(0, gkv_all)
    rs_middle(1, [far, 1])
    in_msg.wait_recv()
    inner = inner + jnp.broadcast_to(in_r[:1, :], (HD, seq)).T[:, :1]
    inner = inner + jnp.sum(gkv_all.astype(f32) * mix[0], axis=1, keepdims=True)
    inv = inv_all[...]
    inv_all[...] = inner * (inv * inv / width)

    gqs = [jnp.concatenate([gq[n, 0], gq[n, 1]], axis=1) for n in range(half)]
    gi_msg = []
    for p in range(PIECES):
        out = jnp.zeros((seq, lanes), f32)
        for q in range(chunks):
            w = wbuf[q, p * span : (p + 1) * span].reshape(lanes, CHUNK)
            out = out + nt_dot(gkv_all if q == 0 else gqs[q - 1], w)
        gain = gbuf[:, p * lanes : (p + 1) * lanes]
        gi_s[p] = (gain * out * inv[:, :1] - hx[p].astype(f32) * inv_all[:, :1]).astype(bf)
        gi_msg.append(x_push(gi_s.at[p, there], gi_r.at[p]))
    queue = list(range(1, chunks)) + [0]
    rs_middle(1, [2])
    rs_sums(0, order)
    rs_middle(1, [0])
    rs_middle(2, [far, 1])
    for p in range(PIECES):
        for b in range(span):
            j = p * span + b
            gin_ref[:, pl.ds(pl.multiple_of((2 * j + x) * rows, rows), rows)] = gi_s[p, here, b * rows : (b + 1) * rows]
    rs_middle(2, [2, 0])
    rs_end(1)
    rs_middle(0, order)
    rs_end(2)
    at_msg.wait_recv()
    for n in range(half):
        attn_ref[:, pl.ds(pl.multiple_of(((1 - x) * half + n) * HD, HD), HD)] = at_r[n]
    for p in range(PIECES):
        gi_msg[p].wait_recv()
        for b in range(span):
            j = p * span + b
            gin_ref[:, pl.ds(pl.multiple_of((2 * j + 1 - x) * rows, rows), rows)] = gi_r[p, :, b * rows : (b + 1) * rows]

    rs_end(0)
    lanes_sum = sums[0]
    for part in sums[1:]:
        lanes_sum = lanes_sum + part
    gg = jnp.sum(lanes_sum.T, axis=0, keepdims=True) / gbuf[:, gcol(block)]
    gg_ref[...] = gg
    gg_s[...] = gg
    pl.when(cross)(lambda: gg_copy.start())

    for cp, cond in sent:
        if cond is None:
            cp.wait_send()
        else:
            pl.when(cond)(cp.wait_send)
    for cp in messages:
        cp.wait_send()
    for n, e in enumerate(plane):
        rcopy(gbuf.at[:, gcol(own)], gbuf.at[:, gcol(own)], g_send.at[n], g_recv.at[own], x_peer).wait_send()
    for q in range(chunks):
        for k in range(chips):
            to_core(q, k).wait_send()
        for d in range(nz):
            if q != turn or d != 1:
                to_y(q, d).wait_send()
            else:
                to_side(0, ybuf.at[q, d]).wait_send()
        for d in hops:
            if d == far and q in MERGED:
                pl.when(inner_z)(to_z(q, d).wait_send)
                pl.when(jnp.logical_not(inner_z))(to_side(q, zbuf.at[q, d - 1]).wait_send)
            else:
                to_z(q, d).wait_send()

    @pl.when(cross)
    def _():
        for q in queue:
            to_diag(q).wait_recv()
            store(q, dg_r[q].astype(f32))
        gg_copy.wait_recv()
        gg_ref[...] = gg_r[...]
        for q in range(chunks):
            to_diag(q).wait_send()
        gg_copy.wait_send()


def copy_kernel(*refs):
    sems = refs[8]
    copies = [pltpu.make_async_copy(refs[k], refs[4 + k], sems.at[k]) for k in range(4)]
    for cp in copies:
        cp.start()
    for cp in copies:
        cp.wait()


def fused(n_inter, hidden_in, norm_gain, qkv_weight, attn_cotangent):
    toks, width = hidden_in.shape[1:]
    rows, cols = qkv_weight.shape
    nz = n_inter // (CORES * SIDE)
    chips = nz * SIDE
    seq, half, chunks = 2 * toks, HEADS // 2, cols // CHUNK
    lanes = n_inter // PIECES * rows
    freqs = rope_base ** (-np.arange(HD // 2, dtype=np.float32) / np.float32(HD // 2))
    angles = (np.arange(seq, dtype=np.float32)[:, None] * freqs.astype(np.float32)[None, :]).astype(np.float32)
    cosine = np.concatenate([np.cos(angles)] * 2, axis=1).astype(np.float32)
    sine = np.concatenate([-np.sin(angles), np.sin(angles)], axis=1).astype(np.float32)
    bf, f32, dma = jnp.bfloat16, jnp.float32, pltpu.SemaphoreType.DMA
    vmem = pl.BlockSpec(memory_space=pltpu.VMEM)
    hbm = pl.BlockSpec(memory_space=pltpu.HBM)
    V = pltpu.VMEM
    n_msgs = 2 * PIECES + 2 * half + 6
    ins = (hidden_in[0], norm_gain[None], qkv_weight, attn_cotangent[0], jnp.asarray(cosine), jnp.asarray(sine))
    attn, gin, wg, gg = pl.pallas_call(
        functools.partial(fused_kernel, n_inter),
        out_shape=(V((toks, HEADS * HD), bf), V((toks, width), bf), V((rows, cols), f32), V((1, rows), f32)),
        in_specs=[hbm] * 6,
        out_specs=(vmem,) * 4,
        scratch_shapes=[
            V((chunks, n_inter, rows, CHUNK), bf),
            V((1, n_inter * rows), f32),
            V((1, rows), bf),
            V((PIECES, seq, lanes), bf),
            V((PIECES, toks, lanes), bf),
            V((PIECES, seq, lanes), bf),
            V((n_inter * rows, seq), bf),
            V((seq, HD), f32),
            V((8, toks), f32),
            V((8, toks), f32),
            V((seq, half * HD), bf),
            V((toks, half * HD), bf),
            V((seq, HD), f32),
            V((seq, HD), f32),
            V((chunks, seq, CHUNK), f32),
            V((seq, CHUNK), bf),
            V((seq, CHUNK), bf),
            V((half, seq, HD), bf),
            V((half, seq, HD), bf),
            V((half, 2, seq, HD), bf),
            V((seq, CHUNK), bf),
            V((seq, CHUNK), bf),
            V((8, seq), f32),
            V((8, seq), f32),
            V((half, seq, HD), bf),
            V((half, toks, HD), bf),
            V((PIECES, seq, lanes), bf),
            V((PIECES, toks, lanes), bf),
            V((chunks, n_inter, rows, CHUNK), bf),
            V((chunks, chips, rows, CHUNK), bf),
            V((chunks, nz, rows, CHUNK), bf),
            V((chunks, nz, rows, CHUNK), bf),
            V((chunks, nz - 1, rows, CHUNK), bf),
            V((chunks, nz - 1, rows, CHUNK), bf),
            V((chunks, rows, CHUNK), bf),
            V((chunks, rows, CHUNK), bf),
            V((chunks, rows, CHUNK), bf),
            V((1, rows), f32),
            V((1, rows), f32),
            dma((8 + half,)),
            dma((chunks * SPLIT, 2 * nz + chips + 1)), dma((chunks * SPLIT, n_inter)),
            dma((n_inter,)), dma((n_inter,)),
            dma((n_msgs,)), dma((n_msgs,)),
            dma((chunks, chips)), dma((chunks, chips)),
            dma((chunks, nz)), dma((chunks, nz)),
            dma((chunks, nz - 1)), dma((chunks, nz - 1)),
            dma((chunks,)), dma((chunks,)),
            dma((chunks + 1,)), dma((chunks + 1,)),
        ],
        compiler_params=pltpu.CompilerParams(
            collective_id=0, has_side_effects=True, vmem_limit_bytes=32 * 2**20
        ),
    )(*[pltpu.with_memory_space_constraint(a, pltpu.HBM) for a in ins])
    outs = (attn, gin, wg, gg)
    attn, gin, wg, gg = pl.pallas_call(
        copy_kernel,
        out_shape=tuple(jax.ShapeDtypeStruct(o.shape, o.dtype) for o in outs),
        in_specs=[vmem] * 4,
        out_specs=(hbm,) * 4,
        scratch_shapes=[dma((4,))],
        compiler_params=pltpu.CompilerParams(vmem_limit_bytes=2**20),
    )(*[pltpu.with_memory_space_constraint(o, pltpu.VMEM) for o in outs])
    return attn[None], gin[None], wg, gg[0]


def solution(mesh):
    n_inter, n_intra = mesh.shape["inter"], mesh.shape["intra"]

    def body(hidden_in, norm_gain, qkv_weight, attn_cotangent):
        nz = n_inter // (CORES * SIDE)
        fits = n_intra == 2 and n_inter % (CORES * SIDE) == 0 and nz > 1 and nz & (nz - 1) == 0
        fits = fits and qkv_weight.shape[0] == HD and hidden_in.shape[0] == 1
        fits = fits and hidden_in.shape[1] == HD and n_inter % PIECES == 0 and HEADS == 4 and nz == 4
        if fits:
            return fused(n_inter, hidden_in, norm_gain, qkv_weight, attn_cotangent)
        return local(hidden_in, norm_gain, qkv_weight, attn_cotangent)

    return jax.shard_map(
        body,
        mesh=mesh,
        in_specs=(
            P("inter", "intra", None),
            P(("inter", "intra")),
            P(("inter", "intra"), None),
            P("inter", "intra", None),
        ),
        out_specs=(
            P("inter", "intra", None),
            P("inter", "intra", None),
            P(("intra", "inter"), None),
            P(("intra", "inter")),
        ),
        check_vma=False,
    )
```

```python
import functools
import jax
import jax.numpy as jnp
import numpy as np
from jax import lax
from jax.experimental import pallas as pl
from jax.experimental.pallas import tpu as pltpu
from jax.sharding import PartitionSpec as P

HD = 128
HEADS = 4


eps_norm = 1e-05
rope_base = 500000.0


def rope_tables(positions, head_size):
    half_size = head_size // 2
    freqs = rope_base ** (-jnp.arange(half_size, dtype=jnp.float32) / half_size)
    angles = positions.astype(jnp.float32)[:, None] * freqs[None, :]
    return (jnp.cos(angles), jnp.sin(angles))


def rotate(values_in, cosine, sine):
    half_size = values_in.shape[-1] // 2
    first, second = (values_in[..., :half_size], values_in[..., half_size:])
    return jnp.concatenate(
        [first * cosine - second * sine, second * cosine + first * sine], axis=-1
    )


def unrotate(grad_out, cosine, sine):
    half_size = grad_out.shape[-1] // 2
    first, second = (grad_out[..., :half_size], grad_out[..., half_size:])
    return jnp.concatenate(
        [first * cosine + second * sine, second * cosine - first * sine], axis=-1
    )


def forward_fold(query_rows, row_pos):

    def forward_advance(carry, piece, start):
        row_top, row_total, weighted = carry
        key_part, value_part = piece
        scores = jnp.einsum("qd,kd->qk", query_rows, key_part, preferred_element_type=jnp.float32)
        key_pos = jnp.arange(key_part.shape[0], dtype=jnp.int32)
        allowed = key_pos[None, :] <= row_pos[:, None]
        scores = jnp.where(allowed, scores, -1e30)
        new_top = jnp.maximum(row_top, jnp.max(scores, axis=1))
        numbers = jnp.where(allowed, jnp.exp(scores - new_top[:, None]), 0.0)
        row_total = jnp.sum(numbers, axis=1)
        weighted = jnp.dot(
            numbers,
            value_part.astype(jnp.float32),
            precision=lax.Precision.HIGHEST,
            preferred_element_type=jnp.float32,
        )
        return (new_top, row_total, weighted)

    return forward_advance


def query_grad_fold(query_rows, row_pos, grad_flat, log_total, row_delta):

    def query_advance(grad_query, piece, start):
        key_part, value_part = piece
        scores = jnp.einsum("qd,kd->qk", query_rows, key_part, preferred_element_type=jnp.float32)
        key_pos = jnp.arange(key_part.shape[0], dtype=jnp.int32)
        allowed = key_pos[None, :] <= row_pos[:, None]
        probs = jnp.where(
            allowed, jnp.exp(jnp.where(allowed, scores, -1e30) - log_total[:, None]), 0.0
        )
        grad_probs = jnp.einsum(
            "qd,kd->qk", grad_flat, value_part, preferred_element_type=jnp.float32
        )
        grad_scores = (probs * (grad_probs - row_delta[:, None])).astype(jnp.bfloat16)
        return jnp.dot(grad_scores, key_part, preferred_element_type=jnp.float32)

    return query_advance


def key_grad_fold(key_rows, value_rows, key_pos, log_all, delta_all, heads_count):

    def key_advance(carry, piece, start):
        query_part, attn_grad_part = piece
        count = query_part.shape[0]
        scores = jnp.einsum("qd,kd->qk", query_part, key_rows, preferred_element_type=jnp.float32)
        query_pos = jnp.arange(count, dtype=jnp.int32) // heads_count
        allowed = key_pos[None, :] <= query_pos[:, None]
        probs = jnp.where(
            allowed, jnp.exp(jnp.where(allowed, scores, -1e30) - log_all[:, None]), 0.0
        )
        grad_values = jnp.einsum(
            "qk,qd->kd",
            probs.astype(jnp.bfloat16),
            attn_grad_part,
            preferred_element_type=jnp.float32,
        )
        grad_probs = jnp.einsum(
            "qd,kd->qk", attn_grad_part, value_rows, preferred_element_type=jnp.float32
        )
        grad_scores = (probs * (grad_probs - delta_all[:, None])).astype(jnp.bfloat16)
        grad_keys = jnp.einsum(
            "qk,qd->kd", grad_scores, query_part, preferred_element_type=jnp.float32
        )
        return (grad_keys, grad_values)

    return key_advance


def local(hidden_in, norm_gain, qkv_weight, attn_cotangent):
    rows_in = hidden_in[0]
    grad_attn = attn_cotangent[0]
    tokens_here = rows_in.shape[0]
    width = rows_in.shape[1]
    head_size = HD
    heads_count = HEADS
    qcols = heads_count * head_size
    scale = head_size ** (-0.5)
    weight_group, gain_group = (
        lax.all_gather(qkv_weight, "intra", axis=0, tiled=True),
        lax.all_gather(norm_gain, "intra", axis=0, tiled=True),
    )
    weight_full, gain_full = (
        lax.all_gather(weight_group, "inter", axis=0, tiled=True),
        lax.all_gather(gain_group, "inter", axis=0, tiled=True),
    )
    query_pos = lax.axis_index("intra") * tokens_here + jnp.arange(tokens_here, dtype=jnp.int32)
    row_pos = jnp.broadcast_to(query_pos[:, None], (tokens_here, heads_count)).reshape(
        tokens_here * heads_count
    )
    cosine, sine = rope_tables(query_pos, head_size)
    wide_rows = rows_in.astype(jnp.float32)
    inv_rms = lax.rsqrt(jnp.mean(wide_rows * wide_rows, axis=1, keepdims=True) + eps_norm)
    normed = (wide_rows * inv_rms * gain_full.astype(jnp.float32)[None, :]).astype(jnp.bfloat16)
    mixed = jnp.dot(normed, weight_full, preferred_element_type=jnp.float32)
    query_rows = (
        (
            rotate(
                mixed[:, :qcols].reshape(tokens_here, heads_count, head_size),
                cosine[:, None, :],
                sine[:, None, :],
            )
            * scale
        )
        .astype(jnp.bfloat16)
        .reshape(tokens_here * heads_count, head_size)
    )
    key_rows = rotate(mixed[:, qcols : qcols + head_size], cosine, sine).astype(jnp.bfloat16)
    value_rows = mixed[:, qcols + head_size :].astype(jnp.bfloat16)
    grad_flat = grad_attn.reshape(tokens_here * heads_count, head_size)
    flat_rows = tokens_here * heads_count
    forward_step = forward_fold(query_rows, row_pos)
    start_carry = (
        jnp.full((flat_rows,), -1e30, jnp.float32),
        jnp.zeros((flat_rows,), jnp.float32),
        jnp.zeros((flat_rows, head_size), jnp.float32),
    )
    row_top, row_total, weighted = forward_step(
        start_carry,
        (
            lax.all_gather(key_rows, "intra", axis=0, tiled=True),
            lax.all_gather(value_rows, "intra", axis=0, tiled=True),
        ),
        jnp.int32(0),
    )
    attn_flat = (weighted / row_total[:, None]).astype(jnp.bfloat16)
    log_total = row_top + jnp.log(row_total)
    row_delta = jnp.sum(grad_flat.astype(jnp.float32) * attn_flat.astype(jnp.float32), axis=1)
    query_step = query_grad_fold(query_rows, row_pos, grad_flat, log_total, row_delta)
    grad_query = query_step(
        jnp.zeros((flat_rows, head_size), jnp.float32),
        (
            lax.all_gather(key_rows, "intra", axis=0, tiled=True),
            lax.all_gather(value_rows, "intra", axis=0, tiled=True),
        ),
        jnp.int32(0),
    )
    log_all, delta_all = (
        lax.all_gather(log_total, "intra", axis=0, tiled=True),
        lax.all_gather(row_delta, "intra", axis=0, tiled=True),
    )
    key_step = key_grad_fold(key_rows, value_rows, query_pos, log_all, delta_all, heads_count)
    grad_keys, grad_values = key_step(
        (
            jnp.zeros((tokens_here, head_size), jnp.float32),
            jnp.zeros((tokens_here, head_size), jnp.float32),
        ),
        (
            lax.all_gather(query_rows, "intra", axis=0, tiled=True),
            lax.all_gather(grad_flat, "intra", axis=0, tiled=True),
        ),
        jnp.int32(0),
    )
    query_back = (
        unrotate(
            grad_query.reshape(tokens_here, heads_count, head_size),
            cosine[:, None, :],
            sine[:, None, :],
        )
        * scale
    ).reshape(tokens_here, qcols)
    grad_mixed = jnp.concatenate(
        [query_back, unrotate(grad_keys, cosine, sine), grad_values], axis=1
    ).astype(jnp.bfloat16)
    weight_back, gain_back = (weight_full, gain_full)
    gain_wide = gain_back.astype(jnp.float32)[None, :]
    grad_normed = jnp.einsum(
        "tc,dc->td", grad_mixed, weight_back, preferred_element_type=jnp.float32
    )
    inner = jnp.sum(grad_normed * gain_wide * wide_rows, axis=1, keepdims=True)
    grad_rows = (
        gain_wide * grad_normed * inv_rms - wide_rows * inv_rms**3 / width * inner
    ).astype(jnp.bfloat16)
    gain_term = jnp.sum(grad_normed * wide_rows * inv_rms, axis=0)
    normed_cols = lax.all_to_all(normed, "intra", split_axis=1, concat_axis=0, tiled=True)
    group_term = lax.dot_general(
        normed_cols,
        lax.all_gather(grad_mixed, "intra", axis=0, tiled=True),
        (((0,), (0,)), ((), ())),
        preferred_element_type=jnp.float32,
    )
    term_low = lax.optimization_barrier(group_term.astype(jnp.bfloat16))
    gain_sums = lax.psum_scatter(gain_term, "intra", scatter_dimension=0, tiled=True)
    weight_grad, gain_grad = (
        lax.psum_scatter(term_low.astype(jnp.float32), "inter", scatter_dimension=0, tiled=True),
        lax.psum_scatter(gain_sums, "inter", scatter_dimension=0, tiled=True),
    )
    return (attn_flat.reshape(tokens_here, qcols)[None], grad_rows[None], weight_grad, gain_grad)

MESH = pl.DeviceIdType.MESH
CORES = 2
SIDE = 2
PIECES = 4
CHUNK = 2 * HD
SPLIT = 1
LAG = 1
HELD = 2
HELD_UNTIL = 0
MERGED = (1, 2)


def nt_dot(a, b):
    return lax.dot_general(a, b, (((1,), (1,)), ((), ())), preferred_element_type=jnp.float32)


def tn_dot(a, b):
    return lax.dot_general(a, b, (((0,), (0,)), ((), ())), preferred_element_type=jnp.float32)


def nn_dot(a, b):
    return jnp.dot(a, b, preferred_element_type=jnp.float32)


def fused_kernel(
    n_inter,
    hid_ref, gain_ref, w_ref, ct_ref, cos_hbm, sin_hbm,
    attn_ref, gin_ref, wg_ref, gg_ref,
    wbuf, gbuf, gain_in, hx, hs, nbuf, ntr, inv_all, inv_s, inv_r, ctb, cts, cos_ref, sin_ref,
    mix, kv_s, kv_r, qm_s, qm_r, gq, gkv_s, gkv_r, in_s, in_r, at_s, at_r, gi_s, gi_r,
    tbuf, rs1, ybuf, rs2, zbuf, rs3, side, dg_s, dg_r, gg_s, gg_r,
    ld_sem, ag_send, ag_recv, ag_core, g_sem, x_send, x_recv,
    c_send, c_recv, r_send, y_recv, z_recv, s_recv, d_send, d_recv,
):
    i = lax.axis_index("inter")
    x = lax.axis_index("intra")
    nz = n_inter // (CORES * SIDE)
    c = lax.rem(i, CORES)
    y = lax.rem(i // CORES, SIDE)
    z = i // (CORES * SIDE)
    toks, width = hid_ref.shape
    rows, cols = w_ref.shape
    seq = 2 * toks
    qcols = HEADS * HD
    chips = nz * SIDE
    chunks = cols // CHUNK
    span = n_inter // PIECES
    lanes = span * rows
    scale = HD ** (-0.5)
    f32, bf = jnp.float32, jnp.bfloat16

    def dev(zz, yy, cc, xx):
        return ((zz * SIDE + yy) * CORES + cc, xx)

    def slot(zz, yy, cc):
        return (zz * SIDE + yy) * CORES + cc

    def across(d):
        zz, bit = z, 1
        while bit < nz:
            if d & bit:
                zz = zz + bit - 2 * bit * lax.rem(z // bit, 2)
            bit *= 2
        return zz

    hops = list(range(1, nz))
    x_peer = dev(z, y, c, 1 - x)
    y_peer = dev(z, 1 - y, c, x)
    c_peer = dev(z, y, 1 - c, x)
    d_peer = dev(z, y, 1 - c, 1 - x)
    plane = [(d, yy, cc) for d in range(nz) for yy in (0, 1) for cc in (0, 1) if d or yy or cc]

    def plane_dev(e):
        d, yy, cc = e
        return (across(d), y + yy - 2 * yy * y, c + cc - 2 * cc * c)

    own = slot(z, y, c)
    here = pl.ds(pl.multiple_of(x * toks, toks), toks)
    there = pl.ds(pl.multiple_of((1 - x) * toks, toks), toks)

    def rcopy(src, dst, ss, rs, device):
        return pltpu.make_async_remote_copy(
            src_ref=src, dst_ref=dst, send_sem=ss, recv_sem=rs, device_id=device, device_id_type=MESH
        )

    barrier = pltpu.get_barrier_semaphore()
    peers = [dev(*plane_dev(e), x) for e in plane] + [x_peer, d_peer]
    for peer in peers:
        pl.semaphore_signal(barrier, inc=1, device_id=peer, device_id_type=MESH)

    def load(src, dst, k):
        pltpu.make_async_copy(src, dst, ld_sem.at[k]).start()

    def loaded(dst, k):
        pltpu.make_async_copy(dst, dst, ld_sem.at[k]).wait()

    for p in range(PIECES):
        for b in range(span):
            j = p * span + b
            mine = pl.ds(pl.multiple_of((2 * j + x) * rows, rows), rows)
            other = pl.ds(pl.multiple_of((2 * j + 1 - x) * rows, rows), rows)
            load(hid_ref.at[:, mine], hx.at[p, here, b * rows : (b + 1) * rows], 0)
            load(hid_ref.at[:, other], hs.at[p, :, b * rows : (b + 1) * rows], 1)
    load(w_ref.at[:, qcols:], wbuf.at[0, own], 2)
    half = HEADS // 2
    for n in range(half):
        for xx in range(2):
            first = (xx * half + n) * HD
            load(w_ref.at[:, first : first + HD], wbuf.at[1 + n, own, :, xx * HD : (xx + 1) * HD], 2)
    nxt = 3
    load(gain_ref, gain_in, nxt)
    load(ct_ref.at[:, pl.ds(pl.multiple_of(x * half * HD, HD), half * HD)], ctb.at[here], nxt + 1)
    load(ct_ref.at[:, pl.ds(pl.multiple_of((1 - x) * half * HD, HD), half * HD)], cts, nxt + 2)
    load(cos_hbm, cos_ref, nxt + 3)
    load(sin_hbm, sin_ref, nxt + 4)

    loaded(gain_in, nxt)
    gcol = lambda g: pl.ds(pl.multiple_of(g * rows, rows), rows)
    gbuf[:, gcol(own)] = gain_in[...].astype(f32)
    loaded(hx.at[:, here], 0)
    loaded(hs, 1)
    total = jnp.zeros((toks, 1), f32)
    for p in range(PIECES):
        a = hx[p, here, :].astype(f32)
        b = hs[p].astype(f32)
        total = total + jnp.sum(a * a + b * b, axis=1, keepdims=True)
    inv = jnp.broadcast_to(lax.rsqrt(total / width + eps_norm), (toks, HD))
    inv_all[here, :] = inv
    inv_s[...] = inv.T[:8, :]
    loaded(wbuf.at[:, own], 2)
    loaded(cts, nxt + 2)
    pl.semaphore_wait(barrier, len(peers))

    inner_z = jnp.logical_and(z > 0, z < nz - 1)
    far = nz - 1
    steps = chunks * SPLIT
    spare = steps - 1

    def ag(t, g, device, core=False):
        part = wbuf.at[t // SPLIT, g, pl.ds(t % SPLIT * (rows // SPLIT), rows // SPLIT)]
        rs = ag_core.at[t] if core else ag_recv.at[t, g // CORES]
        return rcopy(part, part, ag_send.at[t], rs, device)

    def arrive(t, g):
        ag(t, g, x_peer).wait_recv()

    def sent_all(ref, sem):
        rcopy(ref, ref, sem, d_recv.at[0], x_peer).wait_send()

    def got_all(ref, sem):
        rcopy(ref, ref, d_send.at[0], sem, x_peer).wait_recv()

    def push(t, g, device, core=False, cond=None):
        cp = ag(t, g, device, core)
        if cond is None:
            cp.start()
        else:
            pl.when(cond)(cp.start)

    for n, e in enumerate(plane):
        rcopy(gbuf.at[:, gcol(own)], gbuf.at[:, gcol(own)], g_sem.at[0], g_sem.at[1],
              dev(*plane_dev(e), x)).start()
    ends_z = jnp.logical_not(inner_z)

    def own_z(t, late=False):
        for d in hops[::-1]:
            if d == far:
                cond = inner_z
            else:
                cond = (inner_z if late else ends_z) if t >= HELD else None
            if d != far or not late:
                push(t, own, dev(across(d), y, c, x), cond=cond)

    def own_y(t):
        push(t, own, y_peer)
        push(t, own, c_peer, core=True)

    for t in range(steps):
        own_z(t)
        own_y(t)
    messages = []

    def x_push(src, dst, ss=0, rs=None):
        if rs is None:
            rs = len(messages) + 2
            messages.append(rs)
        cp = rcopy(src, dst, x_send.at[ss], x_recv.at[rs], x_peer)
        cp.start()
        return cp

    inv_msg = x_push(inv_s, inv_r, 1)
    for p in range(PIECES):
        x_push(hs.at[p], hx.at[p, here], 0, 0)
    ct_msg = x_push(cts, ctb.at[here])

    def near(n):
        if n < 2:
            return across(n)
        return jnp.where(inner_z, across(nz + 1 - n), across(n))

    def z_arrivals(t):
        for n in hops:
            g = slot(near(n), y, c)
            arrive(t, g)
            if n == far:
                push(t, g, dev(across(1), y, c, x), cond=inner_z)
            if t != spare or n != 1:
                push(t, g, y_peer)
            push(t, g, c_peer, core=True)
        if t == HELD_UNTIL:
            for k in range(HELD, steps):
                own_z(k, True)

    def y_own(t):
        g = slot(z, 1 - y, c)
        arrive(t, g)
        if t == spare:
            push(t, g, dev(across(1), y, c, x))
        push(t, g, c_peer, core=True)

    def y_arrivals(t):
        for n in hops:
            g = slot(near(n), 1 - y, c)
            arrive(t, g)
            push(t, g, c_peer, core=True)

    def c_arrivals(q):
        for t in range(q * SPLIT, (q + 1) * SPLIT):
            got_all(wbuf.at[q, :chips, pl.ds(t % SPLIT * (rows // SPLIT), rows // SPLIT)], ag_core.at[t])

    def norm(which):
        scaled = inv_all[which, :1]
        for p in range(PIECES):
            value = hx[p, which, :].astype(f32) * scaled * gbuf[:, p * lanes : (p + 1) * lanes]
            value = value.astype(bf)
            nbuf[p, which, :] = value
            ntr[p * lanes : (p + 1) * lanes, which] = value.T

    def partial(q):
        out = [jnp.zeros((toks, CHUNK), f32)] * 2
        for p in range(PIECES):
            w = wbuf[q, p * span : (p + 1) * span].reshape(lanes, CHUNK)
            out = [o + nn_dot(nbuf[p, r * toks : (r + 1) * toks, :], w) for r, o in enumerate(out)]
        for r, o in enumerate(out):
            mix[q, r * toks : (r + 1) * toks, :] = o

    mycol = pl.ds(pl.multiple_of(x * HD, HD), HD)
    itscol = pl.ds(pl.multiple_of((1 - x) * HD, HD), HD)

    q_msg = []

    def send_q(n):
        c_arrivals(1 + n)
        partial(1 + n)
        qm_s[n] = mix[1 + n, :, itscol].astype(bf)
        q_msg.append(x_push(qm_s.at[n], qm_r.at[n]))

    for t in range(steps + LAG):
        if t < steps:
            z_arrivals(t)
            y_own(t)
        if t == LAG:
            got_all(gbuf.at[:, : len(plane) * rows], g_sem.at[1])
            norm(here)
        if t >= LAG:
            y_arrivals(t - LAG)
            if t - LAG == SPLIT - 1:
                inv_msg.wait_recv()
                got_all(hs, x_recv.at[0])
                inv_all[there, :] = jnp.broadcast_to(inv_r[:1, :], (toks, toks)).T
                norm(there)
                c_arrivals(0)
                partial(0)
                kv_s[...] = mix[0].astype(bf)
                kv_msg = x_push(kv_s, kv_r)
            if t - LAG == 2 * SPLIT - 1:
                send_q(0)

    loaded(cos_ref, nxt + 3)
    loaded(sin_ref, nxt + 4)
    loaded(ctb.at[here], nxt + 1)
    ct_msg.wait_recv()
    cosine, sine = cos_ref[...], sin_ref[...]

    def rope(u):
        return u * cosine + pltpu.roll(u, HD // 2, 1) * sine

    def unrope(u):
        return u * cosine - pltpu.roll(u, HD // 2, 1) * sine

    kv_msg.wait_recv()
    mix_kv = mix[0] + kv_r[...].astype(f32)
    mix[0] = mix_kv
    keys = rope(mix_kv[:, :HD]).astype(bf)
    values = mix_kv[:, HD:].astype(bf)
    allowed = lax.broadcasted_iota(jnp.int32, (seq, seq), 1) <= lax.broadcasted_iota(jnp.int32, (seq, seq), 0)
    inner = jnp.zeros((seq, 1), f32)
    grad_keys = jnp.zeros((seq, HD), f32)
    grad_values = jnp.zeros((seq, HD), f32)
    gq_msg = []

    def head(n, inner, grad_keys, grad_values):
        q_msg[n].wait_recv()
        mixed = mix[1 + n, :, mycol] + qm_r[n].astype(f32)
        query = (rope(mixed) * scale).astype(bf)
        grad = ctb[:, n * HD : (n + 1) * HD]
        scores = jnp.where(allowed, nt_dot(query, keys), -1e30)
        top = jnp.max(scores, axis=1, keepdims=True)
        numbers = jnp.where(allowed, jnp.exp(scores - top), 0.0)
        norm_sum = jnp.sum(numbers, axis=1, keepdims=True)
        high = numbers.astype(bf)
        low = (numbers - high.astype(f32)).astype(bf)
        attn = ((nn_dot(high, values) + nn_dot(low, values)) / norm_sum).astype(bf)
        at_s[n] = attn
        delta = jnp.sum(grad.astype(f32) * attn.astype(f32), axis=1, keepdims=True)
        probs = numbers / norm_sum
        grad_scores = (probs * (nt_dot(grad, values) - delta)).astype(bf)
        back = (unrope(nn_dot(grad_scores, keys)) * scale).astype(bf)
        gq[n, x] = back
        gq_msg.append(x_push(gq.at[n, x], gq.at[n, x]))
        inner = inner + jnp.sum(back.astype(f32) * mixed, axis=1, keepdims=True)
        grad_keys = grad_keys + tn_dot(grad_scores, query)
        grad_values = grad_values + tn_dot(probs.astype(bf), grad)
        return inner, grad_keys, grad_values

    def to_core(q, k):
        return rcopy(tbuf.at[q, (1 - c) * chips + k], rs1.at[q, k], c_send, c_recv.at[q, lax.rem(k + y, 2)], c_peer)

    def to_y(q, d):
        return rcopy(ybuf.at[q, d], rs2.at[q, d], r_send, y_recv.at[q, d], y_peer)

    def to_z(q, d):
        return rcopy(zbuf.at[q, d - 1], rs3.at[q, d - 1], r_send, z_recv.at[q],
                     dev(across(d), y, c, x))

    order = [far, 1, 2, 0]
    turn = 1

    def terms(q, grads, cc):
        part = nn_dot(ntr[pl.ds(pl.multiple_of(cc * chips * rows, rows), chips * rows), :], grads)
        tbuf[q, pl.ds(cc * chips, chips)] = part.astype(bf).reshape(chips, rows, CHUNK)

    def to_side(k, src):
        return rcopy(src, side.at[k], r_send, s_recv.at[k], dev(across(1), y, c, x))

    def core_sum(q, k):
        return tbuf[q, c * chips + k].astype(f32) + rs1[q, k].astype(f32)

    def rs_terms(q, grads):
        terms(q, grads, 1 - c)
        for yy in (1 - y, y):
            for d in order:
                to_core(q, across(d) * SIDE + yy).start()
        terms(q, grads, c)

    def rs_sums(q, ds):
        if ds[0]:
            got_all(rs1.at[q, :nz], c_recv.at[q, 1])
        for d in ds:
            part = core_sum(q, across(d) * SIDE + 1 - y)
            if q == turn and d == 0:
                to_side(0, ybuf.at[q, 1]).wait_recv()
                part = part + side[0].astype(f32)
            ybuf[q, d] = part.astype(bf)
            if q == turn and d == 1:
                to_side(0, ybuf.at[q, d]).start()
            else:
                to_y(q, d).start()

    def rs_middle(q, ds):
        if ds[0] == far:
            got_all(rs1.at[q, :nz], c_recv.at[q, 0])
        for d in ds:
            part = core_sum(q, across(d) * SIDE + y)
            if q != turn or d != 1:
                to_y(q, d).wait_recv()
                part = part + rs2[q, d].astype(f32)
            if d == 0:
                mix[q, :rows, :] = part
            elif d == far and q in MERGED:
                zbuf[q, d - 1] = part.astype(bf)
                pl.when(inner_z)(to_z(q, d).start)
                pl.when(jnp.logical_not(inner_z))(to_side(q, zbuf.at[q, d - 1]).start)
            elif d == 2 and q in MERGED:
                pl.when(inner_z)(to_side(q, zbuf.at[q, d - 1]).wait_recv)
                extra = jnp.where(inner_z, side[q].astype(f32), 0.0)
                zbuf[q, d - 1] = (part + extra).astype(bf)
                to_z(q, d).start()
            else:
                zbuf[q, d - 1] = part.astype(bf)
                to_z(q, d).start()

    block = c * chips + z * SIDE + y
    cross = c != x
    sums = []

    def rs_end(q):
        result = mix[q, :rows, :]
        if q in MERGED:
            pl.when(inner_z)(lambda: got_all(rs3.at[q], z_recv.at[q]))
            pl.when(ends_z)(lambda: got_all(rs3.at[q, : far - 1], z_recv.at[q]))
        else:
            got_all(rs3.at[q], z_recv.at[q])
        for d in hops:
            part = rs3[q, d - 1].astype(f32)
            result = result + (jnp.where(inner_z, part, 0.0) if d == far and q in MERGED else part)
        prod = wbuf[q, block].astype(f32) * result
        sums.append(prod[:, :HD] + prod[:, HD:])
        dg_s[q] = result.astype(bf)
        pl.when(cross)(lambda: to_diag(q).start())
        store(q, result)

    def store(q, result):
        if q == 0:
            wg_ref[:, qcols:] = result
        else:
            for xx in range(2):
                first = (xx * half + q - 1) * HD
                wg_ref[:, first : first + HD] = result[:, xx * HD : (xx + 1) * HD]

    def to_diag(q):
        return rcopy(dg_s.at[q], dg_r.at[q], d_send.at[0], d_recv.at[0], d_peer)

    gg_copy = rcopy(gg_s, gg_r, d_send.at[1], d_recv.at[1], d_peer)

    def rs_head(n):
        gq_msg[n].wait_recv()
        rs_terms(1 + n, jnp.concatenate([gq[n, 0], gq[n, 1]], axis=1))

    inner, grad_keys, grad_values = head(0, inner, grad_keys, grad_values)
    send_q(1)
    rs_head(0)
    inner, grad_keys, grad_values = head(1, inner, grad_keys, grad_values)
    grad_keys = unrope(grad_keys)
    gkv_s[:, :HD] = grad_keys.astype(bf)
    gkv_s[:, HD:] = grad_values.astype(bf)
    gkv_msg = x_push(gkv_s, gkv_r)
    inner_all = jnp.broadcast_to(inner, (seq, HD))
    in_s[...] = inner_all.T[:8, :]
    in_msg = x_push(in_s, in_r, 2)
    at_msg = x_push(at_s.at[:, there], at_r)
    for n in range(half):
        attn_ref[:, pl.ds(pl.multiple_of((x * half + n) * HD, HD), HD)] = at_s[n, here, :]

    rs_sums(1, [d for d in order if d == 1] + [d for d in order if d > 1])
    rs_head(1)
    rs_sums(1, [0])
    rs_sums(2, order)
    gkv_msg.wait_recv()
    keys_sum = gkv_s[:, :HD].astype(f32) + gkv_r[:, :HD].astype(f32)
    values_sum = gkv_s[:, HD:].astype(f32) + gkv_r[:, HD:].astype(f32)
    gkv_all = jnp.concatenate([keys_sum, values_sum], axis=1).astype(bf)
    rs_terms(0, gkv_all)
    rs_middle(1, [far, 1])
    in_msg.wait_recv()
    inner = inner + jnp.broadcast_to(in_r[:1, :], (HD, seq)).T[:, :1]
    inner = inner + jnp.sum(gkv_all.astype(f32) * mix[0], axis=1, keepdims=True)
    inv = inv_all[...]
    inv_all[...] = inner * (inv * inv / width)

    gqs = [jnp.concatenate([gq[n, 0], gq[n, 1]], axis=1) for n in range(half)]
    for p in range(PIECES):
        out = jnp.zeros((seq, lanes), f32)
        for q in range(chunks):
            w = wbuf[q, p * span : (p + 1) * span].reshape(lanes, CHUNK)
            out = out + nt_dot(gkv_all if q == 0 else gqs[q - 1], w)
        gain = gbuf[:, p * lanes : (p + 1) * lanes]
        gi_s[p] = (gain * out * inv[:, :1] - hx[p].astype(f32) * inv_all[:, :1]).astype(bf)
        x_push(gi_s.at[p, there], gi_r.at[p], 0, 1)
    queue = list(range(1, chunks)) + [0]
    rs_middle(1, [2])
    rs_sums(0, order)
    rs_middle(1, [0])
    rs_middle(2, [far, 1])
    for p in range(PIECES):
        for b in range(span):
            j = p * span + b
            gin_ref[:, pl.ds(pl.multiple_of((2 * j + x) * rows, rows), rows)] = gi_s[p, here, b * rows : (b + 1) * rows]
    rs_middle(2, [2, 0])
    rs_end(1)
    rs_middle(0, order)
    rs_end(2)
    at_msg.wait_recv()
    for n in range(half):
        attn_ref[:, pl.ds(pl.multiple_of(((1 - x) * half + n) * HD, HD), HD)] = at_r[n]
    got_all(gi_r, x_recv.at[1])
    for p in range(PIECES):
        for b in range(span):
            j = p * span + b
            gin_ref[:, pl.ds(pl.multiple_of((2 * j + 1 - x) * rows, rows), rows)] = gi_r[p, :, b * rows : (b + 1) * rows]

    rs_end(0)
    lanes_sum = sums[0]
    for part in sums[1:]:
        lanes_sum = lanes_sum + part
    gg = jnp.sum(lanes_sum.T, axis=0, keepdims=True) / gbuf[:, gcol(block)]
    gg_ref[...] = gg
    gg_s[...] = gg
    pl.when(cross)(lambda: gg_copy.start())

    for t in range(steps):
        near_sends = wbuf.at[t // SPLIT, : n_inter - 2, pl.ds(0, rows // SPLIT)]
        all_sends = wbuf.at[t // SPLIT, :, pl.ds(0, rows // SPLIT)]
        pl.when(inner_z)(lambda: sent_all(all_sends, ag_send.at[t]))
        pl.when(ends_z)(lambda: sent_all(near_sends, ag_send.at[t]))
    sent_all(gbuf.at[:, : len(plane) * rows], g_sem.at[0])
    sent_all(wbuf.at[:2, :13], x_send.at[0])
    sent_all(inv_s, x_send.at[1])
    sent_all(in_s, x_send.at[2])
    sent_all(tbuf.at[:, :chips], c_send)
    sent_all(tbuf.at[:, :7], r_send)

    @pl.when(cross)
    def _():
        got_all(dg_r, d_recv.at[0])
        for q in range(chunks):
            store(q, dg_r[q].astype(f32))
        gg_copy.wait_recv()
        gg_ref[...] = gg_r[...]
        sent_all(dg_s, d_send.at[0])
        gg_copy.wait_send()


def copy_kernel(*refs):
    sems = refs[8]
    copies = [pltpu.make_async_copy(refs[k], refs[4 + k], sems.at[k]) for k in range(4)]
    for cp in copies:
        cp.start()
    for cp in copies:
        cp.wait()


def fused(n_inter, hidden_in, norm_gain, qkv_weight, attn_cotangent):
    toks, width = hidden_in.shape[1:]
    rows, cols = qkv_weight.shape
    nz = n_inter // (CORES * SIDE)
    chips = nz * SIDE
    seq, half, chunks = 2 * toks, HEADS // 2, cols // CHUNK
    lanes = n_inter // PIECES * rows
    freqs = rope_base ** (-np.arange(HD // 2, dtype=np.float32) / np.float32(HD // 2))
    angles = (np.arange(seq, dtype=np.float32)[:, None] * freqs.astype(np.float32)[None, :]).astype(np.float32)
    cosine = np.concatenate([np.cos(angles)] * 2, axis=1).astype(np.float32)
    sine = np.concatenate([-np.sin(angles), np.sin(angles)], axis=1).astype(np.float32)
    bf, f32, dma = jnp.bfloat16, jnp.float32, pltpu.SemaphoreType.DMA
    vmem = pl.BlockSpec(memory_space=pltpu.VMEM)
    hbm = pl.BlockSpec(memory_space=pltpu.HBM)
    V = pltpu.VMEM
    ins = (hidden_in[0], norm_gain[None], qkv_weight, attn_cotangent[0], jnp.asarray(cosine), jnp.asarray(sine))
    attn, gin, wg, gg = pl.pallas_call(
        functools.partial(fused_kernel, n_inter),
        out_shape=(V((toks, HEADS * HD), bf), V((toks, width), bf), V((rows, cols), f32), V((1, rows), f32)),
        in_specs=[hbm] * 6,
        out_specs=(vmem,) * 4,
        scratch_shapes=[
            V((chunks, n_inter, rows, CHUNK), bf),
            V((1, n_inter * rows), f32),
            V((1, rows), bf),
            V((PIECES, seq, lanes), bf),
            V((PIECES, toks, lanes), bf),
            V((PIECES, seq, lanes), bf),
            V((n_inter * rows, seq), bf),
            V((seq, HD), f32),
            V((8, toks), f32),
            V((8, toks), f32),
            V((seq, half * HD), bf),
            V((toks, half * HD), bf),
            V((seq, HD), f32),
            V((seq, HD), f32),
            V((chunks, seq, CHUNK), f32),
            V((seq, CHUNK), bf),
            V((seq, CHUNK), bf),
            V((half, seq, HD), bf),
            V((half, seq, HD), bf),
            V((half, 2, seq, HD), bf),
            V((seq, CHUNK), bf),
            V((seq, CHUNK), bf),
            V((8, seq), f32),
            V((8, seq), f32),
            V((half, seq, HD), bf),
            V((half, toks, HD), bf),
            V((PIECES, seq, lanes), bf),
            V((PIECES, toks, lanes), bf),
            V((chunks, n_inter, rows, CHUNK), bf),
            V((chunks, chips, rows, CHUNK), bf),
            V((chunks, nz, rows, CHUNK), bf),
            V((chunks, nz, rows, CHUNK), bf),
            V((chunks, nz - 1, rows, CHUNK), bf),
            V((chunks, nz - 1, rows, CHUNK), bf),
            V((chunks, rows, CHUNK), bf),
            V((chunks, rows, CHUNK), bf),
            V((chunks, rows, CHUNK), bf),
            V((1, rows), f32),
            V((1, rows), f32),
            dma((8,)),
            dma((chunks * SPLIT,)), dma((chunks * SPLIT, chips)), dma((chunks * SPLIT,)),
            dma((2,)), dma((3,)), dma((12,)),
            dma, dma((chunks, 2)), dma, dma((chunks, nz)), dma((chunks,)), dma((chunks,)),
            dma((2,)), dma((2,)),
        ],
        compiler_params=pltpu.CompilerParams(
            collective_id=0, has_side_effects=True, vmem_limit_bytes=32 * 2**20
        ),
    )(*[pltpu.with_memory_space_constraint(a, pltpu.HBM) for a in ins])
    outs = (attn, gin, wg, gg)
    attn, gin, wg, gg = pl.pallas_call(
        copy_kernel,
        out_shape=tuple(jax.ShapeDtypeStruct(o.shape, o.dtype) for o in outs),
        in_specs=[vmem] * 4,
        out_specs=(hbm,) * 4,
        scratch_shapes=[dma((4,))],
        compiler_params=pltpu.CompilerParams(vmem_limit_bytes=2**20),
    )(*[pltpu.with_memory_space_constraint(o, pltpu.VMEM) for o in outs])
    return attn[None], gin[None], wg, gg[0]


def solution(mesh):
    n_inter, n_intra = mesh.shape["inter"], mesh.shape["intra"]

    def body(hidden_in, norm_gain, qkv_weight, attn_cotangent):
        nz = n_inter // (CORES * SIDE)
        fits = n_intra == 2 and n_inter % (CORES * SIDE) == 0 and nz > 1 and nz & (nz - 1) == 0
        fits = fits and qkv_weight.shape[0] == HD and hidden_in.shape[0] == 1
        fits = fits and hidden_in.shape[1] == HD and n_inter % PIECES == 0 and HEADS == 4 and nz == 4
        if fits:
            return fused(n_inter, hidden_in, norm_gain, qkv_weight, attn_cotangent)
        return local(hidden_in, norm_gain, qkv_weight, attn_cotangent)

    return jax.shard_map(
        body,
        mesh=mesh,
        in_specs=(
            P("inter", "intra", None),
            P(("inter", "intra")),
            P(("inter", "intra"), None),
            P("inter", "intra", None),
        ),
        out_specs=(
            P("inter", "intra", None),
            P("inter", "intra", None),
            P(("intra", "inter"), None),
            P(("intra", "inter")),
        ),
        check_vma=False,
    )
```

```python
import functools
import jax
import jax.numpy as jnp
import numpy as np
from jax import lax
from jax.experimental import pallas as pl
from jax.experimental.pallas import tpu as pltpu
from jax.sharding import PartitionSpec as P

HD = 128
HEADS = 4


eps_norm = 1e-05
rope_base = 500000.0


def rope_tables(positions, head_size):
    half_size = head_size // 2
    freqs = rope_base ** (-jnp.arange(half_size, dtype=jnp.float32) / half_size)
    angles = positions.astype(jnp.float32)[:, None] * freqs[None, :]
    return (jnp.cos(angles), jnp.sin(angles))


def rotate(values_in, cosine, sine):
    half_size = values_in.shape[-1] // 2
    first, second = (values_in[..., :half_size], values_in[..., half_size:])
    return jnp.concatenate(
        [first * cosine - second * sine, second * cosine + first * sine], axis=-1
    )


def unrotate(grad_out, cosine, sine):
    half_size = grad_out.shape[-1] // 2
    first, second = (grad_out[..., :half_size], grad_out[..., half_size:])
    return jnp.concatenate(
        [first * cosine + second * sine, second * cosine - first * sine], axis=-1
    )


def forward_fold(query_rows, row_pos):

    def forward_advance(carry, piece, start):
        row_top, row_total, weighted = carry
        key_part, value_part = piece
        scores = jnp.einsum("qd,kd->qk", query_rows, key_part, preferred_element_type=jnp.float32)
        key_pos = jnp.arange(key_part.shape[0], dtype=jnp.int32)
        allowed = key_pos[None, :] <= row_pos[:, None]
        scores = jnp.where(allowed, scores, -1e30)
        new_top = jnp.maximum(row_top, jnp.max(scores, axis=1))
        numbers = jnp.where(allowed, jnp.exp(scores - new_top[:, None]), 0.0)
        row_total = jnp.sum(numbers, axis=1)
        weighted = jnp.dot(
            numbers,
            value_part.astype(jnp.float32),
            precision=lax.Precision.HIGHEST,
            preferred_element_type=jnp.float32,
        )
        return (new_top, row_total, weighted)

    return forward_advance


def query_grad_fold(query_rows, row_pos, grad_flat, log_total, row_delta):

    def query_advance(grad_query, piece, start):
        key_part, value_part = piece
        scores = jnp.einsum("qd,kd->qk", query_rows, key_part, preferred_element_type=jnp.float32)
        key_pos = jnp.arange(key_part.shape[0], dtype=jnp.int32)
        allowed = key_pos[None, :] <= row_pos[:, None]
        probs = jnp.where(
            allowed, jnp.exp(jnp.where(allowed, scores, -1e30) - log_total[:, None]), 0.0
        )
        grad_probs = jnp.einsum(
            "qd,kd->qk", grad_flat, value_part, preferred_element_type=jnp.float32
        )
        grad_scores = (probs * (grad_probs - row_delta[:, None])).astype(jnp.bfloat16)
        return jnp.dot(grad_scores, key_part, preferred_element_type=jnp.float32)

    return query_advance


def key_grad_fold(key_rows, value_rows, key_pos, log_all, delta_all, heads_count):

    def key_advance(carry, piece, start):
        query_part, attn_grad_part = piece
        count = query_part.shape[0]
        scores = jnp.einsum("qd,kd->qk", query_part, key_rows, preferred_element_type=jnp.float32)
        query_pos = jnp.arange(count, dtype=jnp.int32) // heads_count
        allowed = key_pos[None, :] <= query_pos[:, None]
        probs = jnp.where(
            allowed, jnp.exp(jnp.where(allowed, scores, -1e30) - log_all[:, None]), 0.0
        )
        grad_values = jnp.einsum(
            "qk,qd->kd",
            probs.astype(jnp.bfloat16),
            attn_grad_part,
            preferred_element_type=jnp.float32,
        )
        grad_probs = jnp.einsum(
            "qd,kd->qk", attn_grad_part, value_rows, preferred_element_type=jnp.float32
        )
        grad_scores = (probs * (grad_probs - delta_all[:, None])).astype(jnp.bfloat16)
        grad_keys = jnp.einsum(
            "qk,qd->kd", grad_scores, query_part, preferred_element_type=jnp.float32
        )
        return (grad_keys, grad_values)

    return key_advance


def local(hidden_in, norm_gain, qkv_weight, attn_cotangent):
    rows_in = hidden_in[0]
    grad_attn = attn_cotangent[0]
    tokens_here = rows_in.shape[0]
    width = rows_in.shape[1]
    head_size = HD
    heads_count = HEADS
    qcols = heads_count * head_size
    scale = head_size ** (-0.5)
    weight_group, gain_group = (
        lax.all_gather(qkv_weight, "intra", axis=0, tiled=True),
        lax.all_gather(norm_gain, "intra", axis=0, tiled=True),
    )
    weight_full, gain_full = (
        lax.all_gather(weight_group, "inter", axis=0, tiled=True),
        lax.all_gather(gain_group, "inter", axis=0, tiled=True),
    )
    query_pos = lax.axis_index("intra") * tokens_here + jnp.arange(tokens_here, dtype=jnp.int32)
    row_pos = jnp.broadcast_to(query_pos[:, None], (tokens_here, heads_count)).reshape(
        tokens_here * heads_count
    )
    cosine, sine = rope_tables(query_pos, head_size)
    wide_rows = rows_in.astype(jnp.float32)
    inv_rms = lax.rsqrt(jnp.mean(wide_rows * wide_rows, axis=1, keepdims=True) + eps_norm)
    normed = (wide_rows * inv_rms * gain_full.astype(jnp.float32)[None, :]).astype(jnp.bfloat16)
    mixed = jnp.dot(normed, weight_full, preferred_element_type=jnp.float32)
    query_rows = (
        (
            rotate(
                mixed[:, :qcols].reshape(tokens_here, heads_count, head_size),
                cosine[:, None, :],
                sine[:, None, :],
            )
            * scale
        )
        .astype(jnp.bfloat16)
        .reshape(tokens_here * heads_count, head_size)
    )
    key_rows = rotate(mixed[:, qcols : qcols + head_size], cosine, sine).astype(jnp.bfloat16)
    value_rows = mixed[:, qcols + head_size :].astype(jnp.bfloat16)
    grad_flat = grad_attn.reshape(tokens_here * heads_count, head_size)
    flat_rows = tokens_here * heads_count
    forward_step = forward_fold(query_rows, row_pos)
    start_carry = (
        jnp.full((flat_rows,), -1e30, jnp.float32),
        jnp.zeros((flat_rows,), jnp.float32),
        jnp.zeros((flat_rows, head_size), jnp.float32),
    )
    row_top, row_total, weighted = forward_step(
        start_carry,
        (
            lax.all_gather(key_rows, "intra", axis=0, tiled=True),
            lax.all_gather(value_rows, "intra", axis=0, tiled=True),
        ),
        jnp.int32(0),
    )
    attn_flat = (weighted / row_total[:, None]).astype(jnp.bfloat16)
    log_total = row_top + jnp.log(row_total)
    row_delta = jnp.sum(grad_flat.astype(jnp.float32) * attn_flat.astype(jnp.float32), axis=1)
    query_step = query_grad_fold(query_rows, row_pos, grad_flat, log_total, row_delta)
    grad_query = query_step(
        jnp.zeros((flat_rows, head_size), jnp.float32),
        (
            lax.all_gather(key_rows, "intra", axis=0, tiled=True),
            lax.all_gather(value_rows, "intra", axis=0, tiled=True),
        ),
        jnp.int32(0),
    )
    log_all, delta_all = (
        lax.all_gather(log_total, "intra", axis=0, tiled=True),
        lax.all_gather(row_delta, "intra", axis=0, tiled=True),
    )
    key_step = key_grad_fold(key_rows, value_rows, query_pos, log_all, delta_all, heads_count)
    grad_keys, grad_values = key_step(
        (
            jnp.zeros((tokens_here, head_size), jnp.float32),
            jnp.zeros((tokens_here, head_size), jnp.float32),
        ),
        (
            lax.all_gather(query_rows, "intra", axis=0, tiled=True),
            lax.all_gather(grad_flat, "intra", axis=0, tiled=True),
        ),
        jnp.int32(0),
    )
    query_back = (
        unrotate(
            grad_query.reshape(tokens_here, heads_count, head_size),
            cosine[:, None, :],
            sine[:, None, :],
        )
        * scale
    ).reshape(tokens_here, qcols)
    grad_mixed = jnp.concatenate(
        [query_back, unrotate(grad_keys, cosine, sine), grad_values], axis=1
    ).astype(jnp.bfloat16)
    weight_back, gain_back = (weight_full, gain_full)
    gain_wide = gain_back.astype(jnp.float32)[None, :]
    grad_normed = jnp.einsum(
        "tc,dc->td", grad_mixed, weight_back, preferred_element_type=jnp.float32
    )
    inner = jnp.sum(grad_normed * gain_wide * wide_rows, axis=1, keepdims=True)
    grad_rows = (
        gain_wide * grad_normed * inv_rms - wide_rows * inv_rms**3 / width * inner
    ).astype(jnp.bfloat16)
    gain_term = jnp.sum(grad_normed * wide_rows * inv_rms, axis=0)
    normed_cols = lax.all_to_all(normed, "intra", split_axis=1, concat_axis=0, tiled=True)
    group_term = lax.dot_general(
        normed_cols,
        lax.all_gather(grad_mixed, "intra", axis=0, tiled=True),
        (((0,), (0,)), ((), ())),
        preferred_element_type=jnp.float32,
    )
    term_low = lax.optimization_barrier(group_term.astype(jnp.bfloat16))
    gain_sums = lax.psum_scatter(gain_term, "intra", scatter_dimension=0, tiled=True)
    weight_grad, gain_grad = (
        lax.psum_scatter(term_low.astype(jnp.float32), "inter", scatter_dimension=0, tiled=True),
        lax.psum_scatter(gain_sums, "inter", scatter_dimension=0, tiled=True),
    )
    return (attn_flat.reshape(tokens_here, qcols)[None], grad_rows[None], weight_grad, gain_grad)

MESH = pl.DeviceIdType.MESH
CORES = 2
SIDE = 2
PIECES = 4
CHUNK = 2 * HD
SPLIT = 1
LAG = 1
HELD = 2
HELD_UNTIL = 0
MERGED = (1, 2)


def nt_dot(a, b):
    return lax.dot_general(a, b, (((1,), (1,)), ((), ())), preferred_element_type=jnp.float32)


def tn_dot(a, b):
    return lax.dot_general(a, b, (((0,), (0,)), ((), ())), preferred_element_type=jnp.float32)


def nn_dot(a, b):
    return jnp.dot(a, b, preferred_element_type=jnp.float32)


def fused_kernel(
    n_inter,
    hid_ref, gain_ref, w_ref, ct_ref, cos_hbm, sin_hbm,
    attn_ref, gin_ref, wg_ref, gg_ref,
    wbuf, gbuf, gain_in, hx, hs, nbuf, ntr, inv_all, inv_s, inv_r, ctb, cts, cos_ref, sin_ref,
    mix, kv_s, kv_r, qm_s, qm_r, gq, gkv_s, gkv_r, in_s, in_r, at_s, at_r, gi_s, gi_r,
    tbuf, rs1, ybuf, rs2, zbuf, rs3, side, dg_s, dg_r, gg_s, gg_r, w_own, gain_own,
    ld_sem, ag_send, ag_recv, ag_core, g_sem, x_send, x_recv,
    c_send, c_recv, r_send, y_recv, z_recv, s_recv, d_send, d_recv,
):
    i = lax.axis_index("inter")
    x = lax.axis_index("intra")
    nz = n_inter // (CORES * SIDE)
    c = lax.rem(i, CORES)
    y = lax.rem(i // CORES, SIDE)
    z = i // (CORES * SIDE)
    toks, width = hid_ref.shape
    rows, cols = w_ref.shape
    seq = 2 * toks
    qcols = HEADS * HD
    chips = nz * SIDE
    chunks = cols // CHUNK
    span = n_inter // PIECES
    lanes = span * rows
    scale = HD ** (-0.5)
    f32, bf = jnp.float32, jnp.bfloat16

    def dev(zz, yy, cc, xx):
        return ((zz * SIDE + yy) * CORES + cc, xx)

    def slot(zz, yy, cc):
        return (zz * SIDE + yy) * CORES + cc

    def across(d):
        zz, bit = z, 1
        while bit < nz:
            if d & bit:
                zz = zz + bit - 2 * bit * lax.rem(z // bit, 2)
            bit *= 2
        return zz

    hops = list(range(1, nz))
    x_peer = dev(z, y, c, 1 - x)
    y_peer = dev(z, 1 - y, c, x)
    c_peer = dev(z, y, 1 - c, x)
    d_peer = dev(z, y, 1 - c, 1 - x)
    plane = [(d, yy, cc) for d in range(nz) for yy in (0, 1) for cc in (0, 1) if d or yy or cc]

    def plane_dev(e):
        d, yy, cc = e
        return (across(d), y + yy - 2 * yy * y, c + cc - 2 * cc * c)

    own = slot(z, y, c)
    here = pl.ds(pl.multiple_of(x * toks, toks), toks)
    there = pl.ds(pl.multiple_of((1 - x) * toks, toks), toks)

    def rcopy(src, dst, ss, rs, device):
        return pltpu.make_async_remote_copy(
            src_ref=src, dst_ref=dst, send_sem=ss, recv_sem=rs, device_id=device, device_id_type=MESH
        )

    barrier = pltpu.get_barrier_semaphore()
    peers = [dev(*plane_dev(e), x) for e in plane] + [x_peer, d_peer]
    for peer in peers:
        pl.semaphore_signal(barrier, inc=1, device_id=peer, device_id_type=MESH)

    def load(src, dst, k):
        pltpu.make_async_copy(src, dst, ld_sem.at[k]).start()

    def loaded(dst, k):
        pltpu.make_async_copy(dst, dst, ld_sem.at[k]).wait()

    for p in range(PIECES):
        for b in range(span):
            j = p * span + b
            mine = pl.ds(pl.multiple_of((2 * j + x) * rows, rows), rows)
            other = pl.ds(pl.multiple_of((2 * j + 1 - x) * rows, rows), rows)
            load(hid_ref.at[:, mine], hx.at[p, here, b * rows : (b + 1) * rows], 0)
            load(hid_ref.at[:, other], hs.at[p, :, b * rows : (b + 1) * rows], 1)
    load(w_ref.at[:, qcols:], wbuf.at[0, own], 2)
    half = HEADS // 2
    for n in range(half):
        for xx in range(2):
            first = (xx * half + n) * HD
            load(w_ref.at[:, first : first + HD], wbuf.at[1 + n, own, :, xx * HD : (xx + 1) * HD], 2)
    nxt = 3
    load(gain_ref, gain_in, nxt)
    load(ct_ref.at[:, pl.ds(pl.multiple_of(x * half * HD, HD), half * HD)], ctb.at[here], nxt + 1)
    load(ct_ref.at[:, pl.ds(pl.multiple_of((1 - x) * half * HD, HD), half * HD)], cts, nxt + 2)
    load(cos_hbm, cos_ref, nxt + 3)
    load(sin_hbm, sin_ref, nxt + 4)

    loaded(gain_in, nxt)
    gcol = lambda g: pl.ds(pl.multiple_of(g * rows, rows), rows)
    gbuf[:, gcol(own)] = gain_in[...].astype(f32)
    loaded(hx.at[:, here], 0)
    loaded(hs, 1)
    total = jnp.zeros((toks, 1), f32)
    for p in range(PIECES):
        a = hx[p, here, :].astype(f32)
        b = hs[p].astype(f32)
        total = total + jnp.sum(a * a + b * b, axis=1, keepdims=True)
    inv = jnp.broadcast_to(lax.rsqrt(total / width + eps_norm), (toks, HD))
    inv_all[here, :] = inv
    inv_s[...] = inv.T[:8, :]
    loaded(wbuf.at[:, own], 2)
    loaded(cts, nxt + 2)
    pl.semaphore_wait(barrier, len(peers))

    inner_z = jnp.logical_and(z > 0, z < nz - 1)
    far = nz - 1
    steps = chunks * SPLIT
    spare = steps - 1

    def ag(t, g, device, core=False):
        part = wbuf.at[t // SPLIT, g, pl.ds(t % SPLIT * (rows // SPLIT), rows // SPLIT)]
        rs = ag_core.at[t] if core else ag_recv.at[t, g // CORES]
        return rcopy(part, part, ag_send.at[t], rs, device)

    def arrive(t, g):
        ag(t, g, x_peer).wait_recv()

    def sent_all(ref, sem):
        rcopy(ref, ref, sem, d_recv.at[0], x_peer).wait_send()

    def got_all(ref, sem):
        rcopy(ref, ref, d_send.at[0], sem, x_peer).wait_recv()

    def push(t, g, device, core=False, cond=None):
        cp = ag(t, g, device, core)
        if cond is None:
            cp.start()
        else:
            pl.when(cond)(cp.start)

    for n, e in enumerate(plane):
        rcopy(gbuf.at[:, gcol(own)], gbuf.at[:, gcol(own)], g_sem.at[0], g_sem.at[1],
              dev(*plane_dev(e), x)).start()
    ends_z = jnp.logical_not(inner_z)

    def own_z(t, late=False):
        for d in hops[::-1]:
            if d == far:
                cond = inner_z
            else:
                cond = (inner_z if late else ends_z) if t >= HELD else None
            if d != far or not late:
                push(t, own, dev(across(d), y, c, x), cond=cond)

    def own_y(t):
        push(t, own, y_peer)
        push(t, own, c_peer, core=True)

    for t in range(steps):
        own_z(t)
        own_y(t)
    messages = []

    def x_push(src, dst, ss=0, rs=None):
        if rs is None:
            rs = len(messages) + 2
            messages.append(rs)
        cp = rcopy(src, dst, x_send.at[ss], x_recv.at[rs], x_peer)
        cp.start()
        return cp

    inv_msg = x_push(inv_s, inv_r, 1)
    for p in range(PIECES):
        x_push(hs.at[p], hx.at[p, here], 0, 0)
    ct_msg = x_push(cts, ctb.at[here])

    def near(n):
        if n < 2:
            return across(n)
        return jnp.where(inner_z, across(nz + 1 - n), across(n))

    def z_arrivals(t):
        for n in hops:
            g = slot(near(n), y, c)
            arrive(t, g)
            if n == far:
                push(t, g, dev(across(1), y, c, x), cond=inner_z)
            if t != spare or n != 1:
                push(t, g, y_peer)
            push(t, g, c_peer, core=True)
        if t == HELD_UNTIL:
            for k in range(HELD, steps):
                own_z(k, True)

    def y_own(t):
        g = slot(z, 1 - y, c)
        arrive(t, g)
        if t == spare:
            push(t, g, dev(across(1), y, c, x))
        push(t, g, c_peer, core=True)

    def y_arrivals(t):
        for n in hops:
            g = slot(near(n), 1 - y, c)
            arrive(t, g)
            push(t, g, c_peer, core=True)

    def c_arrivals(q):
        for t in range(q * SPLIT, (q + 1) * SPLIT):
            got_all(wbuf.at[q, :chips, pl.ds(t % SPLIT * (rows // SPLIT), rows // SPLIT)], ag_core.at[t])

    def norm(which):
        scaled = inv_all[which, :1]
        for p in range(PIECES):
            value = hx[p, which, :].astype(f32) * scaled * gbuf[:, p * lanes : (p + 1) * lanes]
            value = value.astype(bf)
            nbuf[p, which, :] = value
            ntr[p * lanes : (p + 1) * lanes, which] = value.T

    def partial(q):
        out = [jnp.zeros((toks, CHUNK), f32)] * 2
        for p in range(PIECES):
            w = wbuf[q, p * span : (p + 1) * span].reshape(lanes, CHUNK)
            out = [o + nn_dot(nbuf[p, r * toks : (r + 1) * toks, :], w) for r, o in enumerate(out)]
        for r, o in enumerate(out):
            mix[q, r * toks : (r + 1) * toks, :] = o

    mycol = pl.ds(pl.multiple_of(x * HD, HD), HD)
    itscol = pl.ds(pl.multiple_of((1 - x) * HD, HD), HD)

    q_msg = []

    def send_q(n):
        c_arrivals(1 + n)
        partial(1 + n)
        qm_s[n] = mix[1 + n, :, itscol].astype(bf)
        q_msg.append(x_push(qm_s.at[n], qm_r.at[n]))

    for t in range(steps + LAG):
        if t < steps:
            z_arrivals(t)
            y_own(t)
        if t == LAG:
            got_all(gbuf.at[:, : len(plane) * rows], g_sem.at[1])
            norm(here)
        if t >= LAG:
            y_arrivals(t - LAG)
            if t - LAG == SPLIT - 1:
                inv_msg.wait_recv()
                got_all(hs, x_recv.at[0])
                inv_all[there, :] = jnp.broadcast_to(inv_r[:1, :], (toks, toks)).T
                norm(there)
                c_arrivals(0)
                partial(0)
                kv_s[...] = mix[0].astype(bf)
                kv_msg = x_push(kv_s, kv_r)
            if t - LAG == 2 * SPLIT - 1:
                send_q(0)

    loaded(cos_ref, nxt + 3)
    loaded(sin_ref, nxt + 4)
    loaded(ctb.at[here], nxt + 1)
    ct_msg.wait_recv()
    cosine, sine = cos_ref[...], sin_ref[...]

    def rope(u):
        return u * cosine + pltpu.roll(u, HD // 2, 1) * sine

    def unrope(u):
        return u * cosine - pltpu.roll(u, HD // 2, 1) * sine

    kv_msg.wait_recv()
    mix_kv = mix[0] + kv_r[...].astype(f32)
    mix[0] = mix_kv
    keys = rope(mix_kv[:, :HD]).astype(bf)
    values = mix_kv[:, HD:].astype(bf)
    allowed = lax.broadcasted_iota(jnp.int32, (seq, seq), 1) <= lax.broadcasted_iota(jnp.int32, (seq, seq), 0)
    inner = jnp.zeros((seq, 1), f32)
    grad_keys = jnp.zeros((seq, HD), f32)
    grad_values = jnp.zeros((seq, HD), f32)
    gq_msg = []

    def head(n, inner, grad_keys, grad_values):
        q_msg[n].wait_recv()
        mixed = mix[1 + n, :, mycol] + qm_r[n].astype(f32)
        query = (rope(mixed) * scale).astype(bf)
        grad = ctb[:, n * HD : (n + 1) * HD]
        scores = jnp.where(allowed, nt_dot(query, keys), -1e30)
        top = jnp.max(scores, axis=1, keepdims=True)
        numbers = jnp.where(allowed, jnp.exp(scores - top), 0.0)
        norm_sum = jnp.sum(numbers, axis=1, keepdims=True)
        high = numbers.astype(bf)
        low = (numbers - high.astype(f32)).astype(bf)
        attn = ((nn_dot(high, values) + nn_dot(low, values)) / norm_sum).astype(bf)
        at_s[n] = attn
        delta = jnp.sum(grad.astype(f32) * attn.astype(f32), axis=1, keepdims=True)
        probs = numbers / norm_sum
        grad_scores = (probs * (nt_dot(grad, values) - delta)).astype(bf)
        back = (unrope(nn_dot(grad_scores, keys)) * scale).astype(bf)
        gq[n, x] = back
        gq_msg.append(x_push(gq.at[n, x], gq.at[n, x]))
        inner = inner + jnp.sum(back.astype(f32) * mixed, axis=1, keepdims=True)
        grad_keys = grad_keys + tn_dot(grad_scores, query)
        grad_values = grad_values + tn_dot(probs.astype(bf), grad)
        return inner, grad_keys, grad_values

    def to_core(q, k):
        return rcopy(tbuf.at[q, (1 - c) * chips + k], rs1.at[q, k], c_send, c_recv.at[q, lax.rem(k + y, 2)], c_peer)

    def to_y(q, d):
        return rcopy(ybuf.at[q, d], rs2.at[q, d], r_send, y_recv.at[q, d], y_peer)

    def to_z(q, d):
        return rcopy(zbuf.at[q, d - 1], rs3.at[q, d - 1], r_send, z_recv.at[q],
                     dev(across(d), y, x, c) if q == 0 else dev(across(d), y, c, x))

    order = [far, 1, 2, 0]
    turn = 1

    def terms(q, grads, cc):
        part = nn_dot(ntr[pl.ds(pl.multiple_of(cc * chips * rows, rows), chips * rows), :], grads)
        tbuf[q, pl.ds(cc * chips, chips)] = part.astype(bf).reshape(chips, rows, CHUNK)

    def to_side(k, src):
        return rcopy(src, side.at[k], r_send, s_recv.at[k], dev(across(1), y, c, x))

    def core_sum(q, k):
        return tbuf[q, c * chips + k].astype(f32) + rs1[q, k].astype(f32)

    def rs_terms(q, grads):
        terms(q, grads, 1 - c)
        for yy in (1 - y, y):
            for d in order:
                to_core(q, across(d) * SIDE + yy).start()
        terms(q, grads, c)

    def rs_sums(q, ds):
        if ds[0]:
            got_all(rs1.at[q, :nz], c_recv.at[q, 1])
        for d in ds:
            part = core_sum(q, across(d) * SIDE + 1 - y)
            if q == turn and d == 0:
                to_side(0, ybuf.at[q, 1]).wait_recv()
                part = part + side[0].astype(f32)
            ybuf[q, d] = part.astype(bf)
            if q == turn and d == 1:
                to_side(0, ybuf.at[q, d]).start()
            else:
                to_y(q, d).start()

    def rs_middle(q, ds):
        if ds[0] == far:
            got_all(rs1.at[q, :nz], c_recv.at[q, 0])
        for d in ds:
            part = core_sum(q, across(d) * SIDE + y)
            if q != turn or d != 1:
                to_y(q, d).wait_recv()
                part = part + rs2[q, d].astype(f32)
            if d == 0:
                mix[q, :rows, :] = part
                if q == 0:
                    dg_s[q] = part.astype(bf)
                    pl.when(cross)(to_diag(q).start)
            elif d == far and q in MERGED:
                zbuf[q, d - 1] = part.astype(bf)
                pl.when(inner_z)(to_z(q, d).start)
                pl.when(jnp.logical_not(inner_z))(to_side(q, zbuf.at[q, d - 1]).start)
            elif d == 2 and q in MERGED:
                pl.when(inner_z)(to_side(q, zbuf.at[q, d - 1]).wait_recv)
                extra = jnp.where(inner_z, side[q].astype(f32), 0.0)
                zbuf[q, d - 1] = (part + extra).astype(bf)
                to_z(q, d).start()
            else:
                zbuf[q, d - 1] = part.astype(bf)
                to_z(q, d).start()

    sums = []

    def gain_term(parts, gain):
        lanes_sum = parts[0]
        for part in parts[1:]:
            lanes_sum = lanes_sum + part
        return jnp.sum(lanes_sum.T, axis=0, keepdims=True) / gain

    def rs_end(q):
        result = mix[q, :rows, :]
        if q == 0:
            pl.when(cross)(to_diag(q).wait_recv)
            result = jnp.where(cross, dg_r[q].astype(f32), result)
        if q in MERGED:
            pl.when(inner_z)(lambda: got_all(rs3.at[q], z_recv.at[q]))
            pl.when(ends_z)(lambda: got_all(rs3.at[q, : far - 1], z_recv.at[q]))
        else:
            got_all(rs3.at[q], z_recv.at[q])
        for d in hops:
            part = rs3[q, d - 1].astype(f32)
            result = result + (jnp.where(inner_z, part, 0.0) if d == far and q in MERGED else part)
        store(q, result)
        if q:
            prod = wbuf[q, block].astype(f32) * result
            sums.append(prod[:, :HD] + prod[:, HD:])
            dg_s[q] = result.astype(bf)
            pl.when(cross)(to_diag(q).start)
            return
        prod = jnp.where(cross, w_own[...], wbuf[q, block]).astype(f32) * result
        gain = jnp.where(cross, gain_own[...], gbuf[:, gcol(block)])
        gg_ref[...] = gain_term([prod[:, :HD] + prod[:, HD:]], gain) + jnp.where(cross, gg_r[...], gg_s[...])

    def store(q, result):
        if q == 0:
            wg_ref[:, qcols:] = result
        else:
            for xx in range(2):
                first = (xx * half + q - 1) * HD
                wg_ref[:, first : first + HD] = result[:, xx * HD : (xx + 1) * HD]

    def rs_head(n):
        gq_msg[n].wait_recv()
        rs_terms(1 + n, jnp.concatenate([gq[n, 0], gq[n, 1]], axis=1))

    inner, grad_keys, grad_values = head(0, inner, grad_keys, grad_values)
    send_q(1)
    rs_head(0)
    inner, grad_keys, grad_values = head(1, inner, grad_keys, grad_values)
    grad_keys = unrope(grad_keys)
    gkv_s[:, :HD] = grad_keys.astype(bf)
    gkv_s[:, HD:] = grad_values.astype(bf)
    gkv_msg = x_push(gkv_s, gkv_r)
    inner_all = jnp.broadcast_to(inner, (seq, HD))
    in_s[...] = inner_all.T[:8, :]
    in_msg = x_push(in_s, in_r, 2)
    at_msg = x_push(at_s.at[:, there], at_r)
    block = c * chips + z * SIDE + y
    cross = c != x

    def to_diag(q):
        return rcopy(dg_s.at[q], dg_r.at[q], d_send.at[0], d_recv.at[min(q, 1)], d_peer)

    w_copy = rcopy(wbuf.at[0, block], w_own, d_send.at[0], d_recv.at[2], d_peer)
    gain_copy = rcopy(gbuf.at[:, gcol(block)], gain_own, d_send.at[1], d_recv.at[3], d_peer)
    gg_copy = rcopy(gg_s, gg_r, d_send.at[1], d_recv.at[4], d_peer)
    pl.when(cross)(w_copy.start)
    pl.when(cross)(gain_copy.start)
    for n in range(half):
        attn_ref[:, pl.ds(pl.multiple_of((x * half + n) * HD, HD), HD)] = at_s[n, here, :]

    rs_sums(1, [d for d in order if d == 1] + [d for d in order if d > 1])
    rs_head(1)
    rs_sums(1, [0])
    rs_sums(2, order)
    gkv_msg.wait_recv()
    keys_sum = gkv_s[:, :HD].astype(f32) + gkv_r[:, :HD].astype(f32)
    values_sum = gkv_s[:, HD:].astype(f32) + gkv_r[:, HD:].astype(f32)
    gkv_all = jnp.concatenate([keys_sum, values_sum], axis=1).astype(bf)
    rs_terms(0, gkv_all)
    rs_middle(1, [far, 1])
    in_msg.wait_recv()
    inner = inner + jnp.broadcast_to(in_r[:1, :], (HD, seq)).T[:, :1]
    inner = inner + jnp.sum(gkv_all.astype(f32) * mix[0], axis=1, keepdims=True)
    inv = inv_all[...]
    inv_all[...] = inner * (inv * inv / width)

    gqs = [jnp.concatenate([gq[n, 0], gq[n, 1]], axis=1) for n in range(half)]
    for p in range(PIECES):
        out = jnp.zeros((seq, lanes), f32)
        for q in range(chunks):
            w = wbuf[q, p * span : (p + 1) * span].reshape(lanes, CHUNK)
            out = out + nt_dot(gkv_all if q == 0 else gqs[q - 1], w)
        gain = gbuf[:, p * lanes : (p + 1) * lanes]
        gi_s[p] = (gain * out * inv[:, :1] - hx[p].astype(f32) * inv_all[:, :1]).astype(bf)
        x_push(gi_s.at[p, there], gi_r.at[p], 0, 1)
    queue = list(range(1, chunks)) + [0]
    rs_middle(1, [2])
    rs_sums(0, order)
    rs_middle(1, [0])
    rs_middle(2, [far, 1])
    for p in range(PIECES):
        for b in range(span):
            j = p * span + b
            gin_ref[:, pl.ds(pl.multiple_of((2 * j + x) * rows, rows), rows)] = gi_s[p, here, b * rows : (b + 1) * rows]
    rs_middle(2, [2, 0])
    rs_end(1)
    rs_middle(0, order)
    rs_end(2)
    gg_s[...] = gain_term(sums, gbuf[:, gcol(block)])
    pl.when(cross)(gg_copy.start)
    at_msg.wait_recv()
    for n in range(half):
        attn_ref[:, pl.ds(pl.multiple_of(((1 - x) * half + n) * HD, HD), HD)] = at_r[n]
    got_all(gi_r, x_recv.at[1])
    for p in range(PIECES):
        for b in range(span):
            j = p * span + b
            gin_ref[:, pl.ds(pl.multiple_of((2 * j + 1 - x) * rows, rows), rows)] = gi_r[p, :, b * rows : (b + 1) * rows]


    @pl.when(cross)
    def _():
        w_copy.wait_recv()
        gain_copy.wait_recv()
        gg_copy.wait_recv()
        got_all(dg_r.at[1:], d_recv.at[1])
        for q in range(1, chunks):
            store(q, dg_r[q].astype(f32))

    rs_end(0)
    for t in range(steps):
        near_sends = wbuf.at[t // SPLIT, : n_inter - 2, pl.ds(0, rows // SPLIT)]
        all_sends = wbuf.at[t // SPLIT, :, pl.ds(0, rows // SPLIT)]
        pl.when(inner_z)(lambda: sent_all(all_sends, ag_send.at[t]))
        pl.when(ends_z)(lambda: sent_all(near_sends, ag_send.at[t]))
    sent_all(gbuf.at[:, : len(plane) * rows], g_sem.at[0])
    sent_all(wbuf.at[:2, :13], x_send.at[0])
    sent_all(inv_s, x_send.at[1])
    sent_all(in_s, x_send.at[2])
    sent_all(tbuf.at[:, :chips], c_send)
    sent_all(tbuf.at[:, :7], r_send)

    @pl.when(cross)
    def _():
        sent_all(wbuf.at[0, : chunks + 1], d_send.at[0])
        sent_all(gbuf.at[:, : 2 * rows], d_send.at[1])


def copy_kernel(*refs):
    sems = refs[8]
    copies = [pltpu.make_async_copy(refs[k], refs[4 + k], sems.at[k]) for k in range(4)]
    for cp in copies:
        cp.start()
    for cp in copies:
        cp.wait()


def fused(n_inter, hidden_in, norm_gain, qkv_weight, attn_cotangent):
    toks, width = hidden_in.shape[1:]
    rows, cols = qkv_weight.shape
    nz = n_inter // (CORES * SIDE)
    chips = nz * SIDE
    seq, half, chunks = 2 * toks, HEADS // 2, cols // CHUNK
    lanes = n_inter // PIECES * rows
    freqs = rope_base ** (-np.arange(HD // 2, dtype=np.float32) / np.float32(HD // 2))
    angles = (np.arange(seq, dtype=np.float32)[:, None] * freqs.astype(np.float32)[None, :]).astype(np.float32)
    cosine = np.concatenate([np.cos(angles)] * 2, axis=1).astype(np.float32)
    sine = np.concatenate([-np.sin(angles), np.sin(angles)], axis=1).astype(np.float32)
    bf, f32, dma = jnp.bfloat16, jnp.float32, pltpu.SemaphoreType.DMA
    vmem = pl.BlockSpec(memory_space=pltpu.VMEM)
    hbm = pl.BlockSpec(memory_space=pltpu.HBM)
    V = pltpu.VMEM
    ins = (hidden_in[0], norm_gain[None], qkv_weight, attn_cotangent[0], jnp.asarray(cosine), jnp.asarray(sine))
    attn, gin, wg, gg = pl.pallas_call(
        functools.partial(fused_kernel, n_inter),
        out_shape=(V((toks, HEADS * HD), bf), V((toks, width), bf), V((rows, cols), f32), V((1, rows), f32)),
        in_specs=[hbm] * 6,
        out_specs=(vmem,) * 4,
        scratch_shapes=[
            V((chunks, n_inter, rows, CHUNK), bf),
            V((1, n_inter * rows), f32),
            V((1, rows), bf),
            V((PIECES, seq, lanes), bf),
            V((PIECES, toks, lanes), bf),
            V((PIECES, seq, lanes), bf),
            V((n_inter * rows, seq), bf),
            V((seq, HD), f32),
            V((8, toks), f32),
            V((8, toks), f32),
            V((seq, half * HD), bf),
            V((toks, half * HD), bf),
            V((seq, HD), f32),
            V((seq, HD), f32),
            V((chunks, seq, CHUNK), f32),
            V((seq, CHUNK), bf),
            V((seq, CHUNK), bf),
            V((half, seq, HD), bf),
            V((half, seq, HD), bf),
            V((half, 2, seq, HD), bf),
            V((seq, CHUNK), bf),
            V((seq, CHUNK), bf),
            V((8, seq), f32),
            V((8, seq), f32),
            V((half, seq, HD), bf),
            V((half, toks, HD), bf),
            V((PIECES, seq, lanes), bf),
            V((PIECES, toks, lanes), bf),
            V((chunks, n_inter, rows, CHUNK), bf),
            V((chunks, chips, rows, CHUNK), bf),
            V((chunks, nz, rows, CHUNK), bf),
            V((chunks, nz, rows, CHUNK), bf),
            V((chunks, nz - 1, rows, CHUNK), bf),
            V((chunks, nz - 1, rows, CHUNK), bf),
            V((chunks, rows, CHUNK), bf),
            V((chunks, rows, CHUNK), bf),
            V((chunks, rows, CHUNK), bf),
            V((1, rows), f32),
            V((1, rows), f32),
            V((rows, CHUNK), bf),
            V((1, rows), f32),
            dma((8,)),
            dma((chunks * SPLIT,)), dma((chunks * SPLIT, chips)), dma((chunks * SPLIT,)),
            dma((2,)), dma((3,)), dma((12,)),
            dma, dma((chunks, 2)), dma, dma((chunks, nz)), dma((chunks,)), dma((chunks,)),
            dma((2,)), dma((5,)),
        ],
        compiler_params=pltpu.CompilerParams(
            collective_id=0, has_side_effects=True, vmem_limit_bytes=32 * 2**20
        ),
    )(*[pltpu.with_memory_space_constraint(a, pltpu.HBM) for a in ins])
    outs = (attn, gin, wg, gg)
    attn, gin, wg, gg = pl.pallas_call(
        copy_kernel,
        out_shape=tuple(jax.ShapeDtypeStruct(o.shape, o.dtype) for o in outs),
        in_specs=[vmem] * 4,
        out_specs=(hbm,) * 4,
        scratch_shapes=[dma((4,))],
        compiler_params=pltpu.CompilerParams(vmem_limit_bytes=2**20),
    )(*[pltpu.with_memory_space_constraint(o, pltpu.VMEM) for o in outs])
    return attn[None], gin[None], wg, gg[0]


def solution(mesh):
    n_inter, n_intra = mesh.shape["inter"], mesh.shape["intra"]

    def body(hidden_in, norm_gain, qkv_weight, attn_cotangent):
        nz = n_inter // (CORES * SIDE)
        fits = n_intra == 2 and n_inter % (CORES * SIDE) == 0 and nz > 1 and nz & (nz - 1) == 0
        fits = fits and qkv_weight.shape[0] == HD and hidden_in.shape[0] == 1
        fits = fits and hidden_in.shape[1] == HD and n_inter % PIECES == 0 and HEADS == 4 and nz == 4
        if fits:
            return fused(n_inter, hidden_in, norm_gain, qkv_weight, attn_cotangent)
        return local(hidden_in, norm_gain, qkv_weight, attn_cotangent)

    return jax.shard_map(
        body,
        mesh=mesh,
        in_specs=(
            P("inter", "intra", None),
            P(("inter", "intra")),
            P(("inter", "intra"), None),
            P("inter", "intra", None),
        ),
        out_specs=(
            P("inter", "intra", None),
            P("inter", "intra", None),
            P(("intra", "inter"), None),
            P(("intra", "inter")),
        ),
        check_vma=False,
    )
```

```python
import functools
import jax
import jax.numpy as jnp
import numpy as np
from jax import lax
from jax.experimental import pallas as pl
from jax.experimental.pallas import tpu as pltpu
from jax.sharding import PartitionSpec as P

HD = 128
HEADS = 4


eps_norm = 1e-05
rope_base = 500000.0


def rope_tables(positions, head_size):
    half_size = head_size // 2
    freqs = rope_base ** (-jnp.arange(half_size, dtype=jnp.float32) / half_size)
    angles = positions.astype(jnp.float32)[:, None] * freqs[None, :]
    return (jnp.cos(angles), jnp.sin(angles))


def rotate(values_in, cosine, sine):
    half_size = values_in.shape[-1] // 2
    first, second = (values_in[..., :half_size], values_in[..., half_size:])
    return jnp.concatenate(
        [first * cosine - second * sine, second * cosine + first * sine], axis=-1
    )


def unrotate(grad_out, cosine, sine):
    half_size = grad_out.shape[-1] // 2
    first, second = (grad_out[..., :half_size], grad_out[..., half_size:])
    return jnp.concatenate(
        [first * cosine + second * sine, second * cosine - first * sine], axis=-1
    )


def forward_fold(query_rows, row_pos):

    def forward_advance(carry, piece, start):
        row_top, row_total, weighted = carry
        key_part, value_part = piece
        scores = jnp.einsum("qd,kd->qk", query_rows, key_part, preferred_element_type=jnp.float32)
        key_pos = jnp.arange(key_part.shape[0], dtype=jnp.int32)
        allowed = key_pos[None, :] <= row_pos[:, None]
        scores = jnp.where(allowed, scores, -1e30)
        new_top = jnp.maximum(row_top, jnp.max(scores, axis=1))
        numbers = jnp.where(allowed, jnp.exp(scores - new_top[:, None]), 0.0)
        row_total = jnp.sum(numbers, axis=1)
        weighted = jnp.dot(
            numbers,
            value_part.astype(jnp.float32),
            precision=lax.Precision.HIGHEST,
            preferred_element_type=jnp.float32,
        )
        return (new_top, row_total, weighted)

    return forward_advance


def query_grad_fold(query_rows, row_pos, grad_flat, log_total, row_delta):

    def query_advance(grad_query, piece, start):
        key_part, value_part = piece
        scores = jnp.einsum("qd,kd->qk", query_rows, key_part, preferred_element_type=jnp.float32)
        key_pos = jnp.arange(key_part.shape[0], dtype=jnp.int32)
        allowed = key_pos[None, :] <= row_pos[:, None]
        probs = jnp.where(
            allowed, jnp.exp(jnp.where(allowed, scores, -1e30) - log_total[:, None]), 0.0
        )
        grad_probs = jnp.einsum(
            "qd,kd->qk", grad_flat, value_part, preferred_element_type=jnp.float32
        )
        grad_scores = (probs * (grad_probs - row_delta[:, None])).astype(jnp.bfloat16)
        return jnp.dot(grad_scores, key_part, preferred_element_type=jnp.float32)

    return query_advance


def key_grad_fold(key_rows, value_rows, key_pos, log_all, delta_all, heads_count):

    def key_advance(carry, piece, start):
        query_part, attn_grad_part = piece
        count = query_part.shape[0]
        scores = jnp.einsum("qd,kd->qk", query_part, key_rows, preferred_element_type=jnp.float32)
        query_pos = jnp.arange(count, dtype=jnp.int32) // heads_count
        allowed = key_pos[None, :] <= query_pos[:, None]
        probs = jnp.where(
            allowed, jnp.exp(jnp.where(allowed, scores, -1e30) - log_all[:, None]), 0.0
        )
        grad_values = jnp.einsum(
            "qk,qd->kd",
            probs.astype(jnp.bfloat16),
            attn_grad_part,
            preferred_element_type=jnp.float32,
        )
        grad_probs = jnp.einsum(
            "qd,kd->qk", attn_grad_part, value_rows, preferred_element_type=jnp.float32
        )
        grad_scores = (probs * (grad_probs - delta_all[:, None])).astype(jnp.bfloat16)
        grad_keys = jnp.einsum(
            "qk,qd->kd", grad_scores, query_part, preferred_element_type=jnp.float32
        )
        return (grad_keys, grad_values)

    return key_advance


def local(hidden_in, norm_gain, qkv_weight, attn_cotangent):
    rows_in = hidden_in[0]
    grad_attn = attn_cotangent[0]
    tokens_here = rows_in.shape[0]
    width = rows_in.shape[1]
    head_size = HD
    heads_count = HEADS
    qcols = heads_count * head_size
    scale = head_size ** (-0.5)
    weight_group, gain_group = (
        lax.all_gather(qkv_weight, "intra", axis=0, tiled=True),
        lax.all_gather(norm_gain, "intra", axis=0, tiled=True),
    )
    weight_full, gain_full = (
        lax.all_gather(weight_group, "inter", axis=0, tiled=True),
        lax.all_gather(gain_group, "inter", axis=0, tiled=True),
    )
    query_pos = lax.axis_index("intra") * tokens_here + jnp.arange(tokens_here, dtype=jnp.int32)
    row_pos = jnp.broadcast_to(query_pos[:, None], (tokens_here, heads_count)).reshape(
        tokens_here * heads_count
    )
    cosine, sine = rope_tables(query_pos, head_size)
    wide_rows = rows_in.astype(jnp.float32)
    inv_rms = lax.rsqrt(jnp.mean(wide_rows * wide_rows, axis=1, keepdims=True) + eps_norm)
    normed = (wide_rows * inv_rms * gain_full.astype(jnp.float32)[None, :]).astype(jnp.bfloat16)
    mixed = jnp.dot(normed, weight_full, preferred_element_type=jnp.float32)
    query_rows = (
        (
            rotate(
                mixed[:, :qcols].reshape(tokens_here, heads_count, head_size),
                cosine[:, None, :],
                sine[:, None, :],
            )
            * scale
        )
        .astype(jnp.bfloat16)
        .reshape(tokens_here * heads_count, head_size)
    )
    key_rows = rotate(mixed[:, qcols : qcols + head_size], cosine, sine).astype(jnp.bfloat16)
    value_rows = mixed[:, qcols + head_size :].astype(jnp.bfloat16)
    grad_flat = grad_attn.reshape(tokens_here * heads_count, head_size)
    flat_rows = tokens_here * heads_count
    forward_step = forward_fold(query_rows, row_pos)
    start_carry = (
        jnp.full((flat_rows,), -1e30, jnp.float32),
        jnp.zeros((flat_rows,), jnp.float32),
        jnp.zeros((flat_rows, head_size), jnp.float32),
    )
    row_top, row_total, weighted = forward_step(
        start_carry,
        (
            lax.all_gather(key_rows, "intra", axis=0, tiled=True),
            lax.all_gather(value_rows, "intra", axis=0, tiled=True),
        ),
        jnp.int32(0),
    )
    attn_flat = (weighted / row_total[:, None]).astype(jnp.bfloat16)
    log_total = row_top + jnp.log(row_total)
    row_delta = jnp.sum(grad_flat.astype(jnp.float32) * attn_flat.astype(jnp.float32), axis=1)
    query_step = query_grad_fold(query_rows, row_pos, grad_flat, log_total, row_delta)
    grad_query = query_step(
        jnp.zeros((flat_rows, head_size), jnp.float32),
        (
            lax.all_gather(key_rows, "intra", axis=0, tiled=True),
            lax.all_gather(value_rows, "intra", axis=0, tiled=True),
        ),
        jnp.int32(0),
    )
    log_all, delta_all = (
        lax.all_gather(log_total, "intra", axis=0, tiled=True),
        lax.all_gather(row_delta, "intra", axis=0, tiled=True),
    )
    key_step = key_grad_fold(key_rows, value_rows, query_pos, log_all, delta_all, heads_count)
    grad_keys, grad_values = key_step(
        (
            jnp.zeros((tokens_here, head_size), jnp.float32),
            jnp.zeros((tokens_here, head_size), jnp.float32),
        ),
        (
            lax.all_gather(query_rows, "intra", axis=0, tiled=True),
            lax.all_gather(grad_flat, "intra", axis=0, tiled=True),
        ),
        jnp.int32(0),
    )
    query_back = (
        unrotate(
            grad_query.reshape(tokens_here, heads_count, head_size),
            cosine[:, None, :],
            sine[:, None, :],
        )
        * scale
    ).reshape(tokens_here, qcols)
    grad_mixed = jnp.concatenate(
        [query_back, unrotate(grad_keys, cosine, sine), grad_values], axis=1
    ).astype(jnp.bfloat16)
    weight_back, gain_back = (weight_full, gain_full)
    gain_wide = gain_back.astype(jnp.float32)[None, :]
    grad_normed = jnp.einsum(
        "tc,dc->td", grad_mixed, weight_back, preferred_element_type=jnp.float32
    )
    inner = jnp.sum(grad_normed * gain_wide * wide_rows, axis=1, keepdims=True)
    grad_rows = (
        gain_wide * grad_normed * inv_rms - wide_rows * inv_rms**3 / width * inner
    ).astype(jnp.bfloat16)
    gain_term = jnp.sum(grad_normed * wide_rows * inv_rms, axis=0)
    normed_cols = lax.all_to_all(normed, "intra", split_axis=1, concat_axis=0, tiled=True)
    group_term = lax.dot_general(
        normed_cols,
        lax.all_gather(grad_mixed, "intra", axis=0, tiled=True),
        (((0,), (0,)), ((), ())),
        preferred_element_type=jnp.float32,
    )
    term_low = lax.optimization_barrier(group_term.astype(jnp.bfloat16))
    gain_sums = lax.psum_scatter(gain_term, "intra", scatter_dimension=0, tiled=True)
    weight_grad, gain_grad = (
        lax.psum_scatter(term_low.astype(jnp.float32), "inter", scatter_dimension=0, tiled=True),
        lax.psum_scatter(gain_sums, "inter", scatter_dimension=0, tiled=True),
    )
    return (attn_flat.reshape(tokens_here, qcols)[None], grad_rows[None], weight_grad, gain_grad)

MESH = pl.DeviceIdType.MESH
CORES = 2
SIDE = 2
PIECES = 4
CHUNK = 2 * HD
SPLIT = 1
LAG = 1
HELD = 2
HELD_UNTIL = 0
MERGED = (1, 2)


def nt_dot(a, b):
    return lax.dot_general(a, b, (((1,), (1,)), ((), ())), preferred_element_type=jnp.float32)


def tn_dot(a, b):
    return lax.dot_general(a, b, (((0,), (0,)), ((), ())), preferred_element_type=jnp.float32)


def nn_dot(a, b):
    return jnp.dot(a, b, preferred_element_type=jnp.float32)


def fused_kernel(
    n_inter,
    hid_ref, gain_ref, w_ref, ct_ref, cos_hbm, sin_hbm,
    attn_ref, gin_ref, wg_ref, gg_ref,
    wbuf, gbuf, gain_in, hx, hs, nbuf, ntr, inv_all, inv_s, inv_r, ctb, cts, cos_ref, sin_ref,
    mix, kv_s, kv_r, qm_s, qm_r, gq, gkv_s, gkv_r, in_s, in_r, at_s, at_r, gi_s, gi_r,
    tbuf, rs1, ybuf, rs2, zbuf, rs3, side, dg_s, dg_r, gg_s, gg_r, w_own, gain_own,
    ld_sem, ag_send, ag_recv, ag_core, g_sem, x_send, x_recv,
    c_send, c_recv, r_send, y_recv, z_recv, s_recv, d_send, d_recv,
):
    i = lax.axis_index("inter")
    x = lax.axis_index("intra")
    nz = n_inter // (CORES * SIDE)
    c = lax.rem(i, CORES)
    y = lax.rem(i // CORES, SIDE)
    z = i // (CORES * SIDE)
    toks, width = hid_ref.shape
    rows, cols = w_ref.shape
    seq = 2 * toks
    qcols = HEADS * HD
    chips = nz * SIDE
    chunks = cols // CHUNK
    span = n_inter // PIECES
    lanes = span * rows
    scale = HD ** (-0.5)
    f32, bf = jnp.float32, jnp.bfloat16

    def dev(zz, yy, cc, xx):
        return ((zz * SIDE + yy) * CORES + cc, xx)

    def slot(zz, yy, cc):
        return (zz * SIDE + yy) * CORES + cc

    def across(d):
        zz, bit = z, 1
        while bit < nz:
            if d & bit:
                zz = zz + bit - 2 * bit * lax.rem(z // bit, 2)
            bit *= 2
        return zz

    hops = list(range(1, nz))
    x_peer = dev(z, y, c, 1 - x)
    y_peer = dev(z, 1 - y, c, x)
    c_peer = dev(z, y, 1 - c, x)
    d_peer = dev(z, y, 1 - c, 1 - x)
    plane = [(d, yy, cc) for d in range(nz) for yy in (0, 1) for cc in (0, 1) if d or yy or cc]

    def plane_dev(e):
        d, yy, cc = e
        return (across(d), y + yy - 2 * yy * y, c + cc - 2 * cc * c)

    own = slot(z, y, c)
    here = pl.ds(pl.multiple_of(x * toks, toks), toks)
    there = pl.ds(pl.multiple_of((1 - x) * toks, toks), toks)

    def rcopy(src, dst, ss, rs, device):
        return pltpu.make_async_remote_copy(
            src_ref=src, dst_ref=dst, send_sem=ss, recv_sem=rs, device_id=device, device_id_type=MESH
        )

    barrier = pltpu.get_barrier_semaphore()
    peers = [dev(*plane_dev(e), x) for e in plane] + [x_peer, d_peer]
    for peer in peers:
        pl.semaphore_signal(barrier, inc=1, device_id=peer, device_id_type=MESH)

    def load(src, dst, k):
        pltpu.make_async_copy(src, dst, ld_sem.at[k]).start()

    def loaded(dst, k):
        pltpu.make_async_copy(dst, dst, ld_sem.at[k]).wait()

    for p in range(PIECES):
        for b in range(span):
            j = p * span + b
            mine = pl.ds(pl.multiple_of((2 * j + x) * rows, rows), rows)
            other = pl.ds(pl.multiple_of((2 * j + 1 - x) * rows, rows), rows)
            load(hid_ref.at[:, mine], hx.at[p, here, b * rows : (b + 1) * rows], 0)
            load(hid_ref.at[:, other], hs.at[p, :, b * rows : (b + 1) * rows], 1)
    load(w_ref.at[:, qcols:], wbuf.at[0, own], 2)
    half = HEADS // 2
    for n in range(half):
        for xx in range(2):
            first = (xx * half + n) * HD
            load(w_ref.at[:, first : first + HD], wbuf.at[1 + n, own, :, xx * HD : (xx + 1) * HD], 2)
    nxt = 3
    load(gain_ref, gain_in, nxt)
    load(ct_ref.at[:, pl.ds(pl.multiple_of(x * half * HD, HD), half * HD)], ctb.at[here], nxt + 1)
    load(ct_ref.at[:, pl.ds(pl.multiple_of((1 - x) * half * HD, HD), half * HD)], cts, nxt + 2)
    load(cos_hbm, cos_ref, nxt + 3)
    load(sin_hbm, sin_ref, nxt + 4)

    loaded(gain_in, nxt)
    gcol = lambda g: pl.ds(pl.multiple_of(g * rows, rows), rows)
    gbuf[:, gcol(own)] = gain_in[...].astype(f32)
    loaded(hx.at[:, here], 0)
    loaded(hs, 1)
    total = jnp.zeros((toks, 1), f32)
    for p in range(PIECES):
        a = hx[p, here, :].astype(f32)
        b = hs[p].astype(f32)
        total = total + jnp.sum(a * a + b * b, axis=1, keepdims=True)
    inv = jnp.broadcast_to(lax.rsqrt(total / width + eps_norm), (toks, HD))
    inv_all[here, :] = inv
    inv_s[...] = inv.T[:8, :]
    loaded(wbuf.at[:, own], 2)
    loaded(cts, nxt + 2)
    pl.semaphore_wait(barrier, len(peers))

    inner_z = jnp.logical_and(z > 0, z < nz - 1)
    far = nz - 1
    steps = chunks * SPLIT
    spare = steps - 1

    def ag(t, g, device, core=False):
        part = wbuf.at[t // SPLIT, g, pl.ds(t % SPLIT * (rows // SPLIT), rows // SPLIT)]
        rs = ag_core.at[t] if core else ag_recv.at[t, g // CORES]
        return rcopy(part, part, ag_send.at[t], rs, device)

    def arrive(t, g):
        ag(t, g, x_peer).wait_recv()

    def sent_all(ref, sem):
        rcopy(ref, ref, sem, d_recv.at[0], x_peer).wait_send()

    def got_all(ref, sem):
        rcopy(ref, ref, d_send.at[0], sem, x_peer).wait_recv()

    def push(t, g, device, core=False, cond=None):
        cp = ag(t, g, device, core)
        if cond is None:
            cp.start()
        else:
            pl.when(cond)(cp.start)

    for n, e in enumerate(plane):
        rcopy(gbuf.at[:, gcol(own)], gbuf.at[:, gcol(own)], g_sem.at[0], g_sem.at[1],
              dev(*plane_dev(e), x)).start()
    ends_z = jnp.logical_not(inner_z)

    def own_z(t, late=False):
        for d in hops[::-1]:
            if d == far:
                cond = inner_z
            else:
                cond = (inner_z if late else ends_z) if t >= HELD else None
            if d != far or not late:
                push(t, own, dev(across(d), y, c, x), cond=cond)

    def own_y(t):
        push(t, own, y_peer)
        push(t, own, c_peer, core=True)

    for t in range(steps):
        own_z(t)
        own_y(t)
    messages = []

    def x_push(src, dst, ss=0, rs=None):
        if rs is None:
            rs = len(messages) + 2
            messages.append(rs)
        cp = rcopy(src, dst, x_send.at[ss], x_recv.at[rs], x_peer)
        cp.start()
        return cp

    inv_msg = x_push(inv_s, inv_r, 1)
    for p in range(PIECES):
        x_push(hs.at[p], hx.at[p, here], 0, 0)
    ct_msg = x_push(cts, ctb.at[here])

    def near(n):
        if n < 2:
            return across(n)
        return jnp.where(inner_z, across(nz + 1 - n), across(n))

    def z_arrivals(t):
        for n in hops:
            g = slot(near(n), y, c)
            arrive(t, g)
            if n == far:
                push(t, g, dev(across(1), y, c, x), cond=inner_z)
            if t != spare or n != 1:
                push(t, g, y_peer)
            push(t, g, c_peer, core=True)
        if t == HELD_UNTIL:
            for k in range(HELD, steps):
                own_z(k, True)

    def y_own(t):
        g = slot(z, 1 - y, c)
        arrive(t, g)
        if t == spare:
            push(t, g, dev(across(1), y, c, x))
        push(t, g, c_peer, core=True)

    def y_arrivals(t):
        for n in hops:
            g = slot(near(n), 1 - y, c)
            arrive(t, g)
            push(t, g, c_peer, core=True)

    def c_arrivals(q):
        for t in range(q * SPLIT, (q + 1) * SPLIT):
            got_all(wbuf.at[q, :chips, pl.ds(t % SPLIT * (rows // SPLIT), rows // SPLIT)], ag_core.at[t])

    def norm(which):
        scaled = inv_all[which, :1]
        for p in range(PIECES):
            value = hx[p, which, :].astype(f32) * scaled * gbuf[:, p * lanes : (p + 1) * lanes]
            value = value.astype(bf)
            nbuf[p, which, :] = value
            ntr[p * lanes : (p + 1) * lanes, which] = value.T

    def partial(q):
        out = [jnp.zeros((toks, CHUNK), f32)] * 2
        for p in range(PIECES):
            w = wbuf[q, p * span : (p + 1) * span].reshape(lanes, CHUNK)
            out = [o + nn_dot(nbuf[p, r * toks : (r + 1) * toks, :], w) for r, o in enumerate(out)]
        for r, o in enumerate(out):
            mix[q, r * toks : (r + 1) * toks, :] = o

    mycol = pl.ds(pl.multiple_of(x * HD, HD), HD)
    itscol = pl.ds(pl.multiple_of((1 - x) * HD, HD), HD)

    q_msg = []

    def send_q(n):
        c_arrivals(1 + n)
        partial(1 + n)
        qm_s[n] = mix[1 + n, :, itscol].astype(bf)
        q_msg.append(x_push(qm_s.at[n], qm_r.at[n]))

    for t in range(steps + LAG):
        if t < steps:
            z_arrivals(t)
            y_own(t)
        if t == LAG:
            got_all(gbuf.at[:, : len(plane) * rows], g_sem.at[1])
            norm(here)
        if t >= LAG:
            y_arrivals(t - LAG)
            if t - LAG == SPLIT - 1:
                inv_msg.wait_recv()
                got_all(hs, x_recv.at[0])
                inv_all[there, :] = jnp.broadcast_to(inv_r[:1, :], (toks, toks)).T
                norm(there)
                c_arrivals(0)
                partial(0)
                kv_s[...] = mix[0].astype(bf)
                kv_msg = x_push(kv_s, kv_r)
            if t - LAG == 2 * SPLIT - 1:
                send_q(0)

    loaded(cos_ref, nxt + 3)
    loaded(sin_ref, nxt + 4)
    loaded(ctb.at[here], nxt + 1)
    ct_msg.wait_recv()
    cosine, sine = cos_ref[...], sin_ref[...]

    def rope(u):
        return u * cosine + pltpu.roll(u, HD // 2, 1) * sine

    def unrope(u):
        return u * cosine - pltpu.roll(u, HD // 2, 1) * sine

    kv_msg.wait_recv()
    mix_kv = mix[0] + kv_r[...].astype(f32)
    mix[0] = mix_kv
    keys = rope(mix_kv[:, :HD]).astype(bf)
    values = mix_kv[:, HD:].astype(bf)
    allowed = lax.broadcasted_iota(jnp.int32, (seq, seq), 1) <= lax.broadcasted_iota(jnp.int32, (seq, seq), 0)
    inner = jnp.zeros((seq, 1), f32)
    grad_keys = jnp.zeros((seq, HD), f32)
    grad_values = jnp.zeros((seq, HD), f32)
    gq_msg = []

    def head(n, inner, grad_keys, grad_values):
        grad = ctb[:, n * HD : (n + 1) * HD]
        grad_probs = nt_dot(grad, values)
        q_msg[n].wait_recv()
        mixed = mix[1 + n, :, mycol] + qm_r[n].astype(f32)
        query = (rope(mixed) * scale).astype(bf)
        scores = jnp.where(allowed, nt_dot(query, keys), -1e30)
        top = jnp.max(scores, axis=1, keepdims=True)
        numbers = jnp.where(allowed, jnp.exp(scores - top), 0.0)
        share = 1.0 / jnp.sum(numbers, axis=1, keepdims=True)
        probs = numbers * share
        delta = jnp.sum(probs * grad_probs, axis=1, keepdims=True)
        grad_scores = (probs * (grad_probs - delta)).astype(bf)
        back = (unrope(nn_dot(grad_scores, keys)) * scale).astype(bf)
        gq[n, x] = back
        gq_msg.append(x_push(gq.at[n, x], gq.at[n, x]))
        high = numbers.astype(bf)
        low = (numbers - high.astype(f32)).astype(bf)
        at_s[n] = ((nn_dot(high, values) + nn_dot(low, values)) * share).astype(bf)
        inner = inner + jnp.sum(back.astype(f32) * mixed, axis=1, keepdims=True)
        grad_keys = grad_keys + tn_dot(grad_scores, query)
        grad_values = grad_values + tn_dot(probs.astype(bf), grad)
        return inner, grad_keys, grad_values

    def to_core(q, k):
        return rcopy(tbuf.at[q, (1 - c) * chips + k], rs1.at[q, k], c_send, c_recv.at[q, lax.rem(k + y, 2)], c_peer)

    def to_y(q, d):
        return rcopy(ybuf.at[q, d], rs2.at[q, d], r_send, y_recv.at[q, d], y_peer)

    def to_z(q, d):
        return rcopy(zbuf.at[q, d - 1], rs3.at[q, d - 1], r_send, z_recv.at[q],
                     dev(across(d), y, x, c) if q == 0 else dev(across(d), y, c, x))

    order = [far, 1, 2, 0]
    turn = 1

    def terms(q, grads, cc):
        group = chips // 4
        for r in range(4):
            first = cc * chips + r * group
            part = nn_dot(ntr[pl.ds(pl.multiple_of(first * rows, rows), group * rows), :], grads)
            tbuf[q, pl.ds(first, group)] = part.astype(bf).reshape(group, rows, CHUNK)

    def to_side(k, src):
        return rcopy(src, side.at[k], r_send, s_recv.at[k], dev(across(1), y, c, x))

    def core_sum(q, k):
        return tbuf[q, c * chips + k].astype(f32) + rs1[q, k].astype(f32)

    def rs_terms(q, grads):
        terms(q, grads, 1 - c)
        for yy in (1 - y, y):
            for d in order:
                to_core(q, across(d) * SIDE + yy).start()
        terms(q, grads, c)

    def rs_sums(q, ds):
        if ds[0]:
            got_all(rs1.at[q, :nz], c_recv.at[q, 1])
        for d in ds:
            part = core_sum(q, across(d) * SIDE + 1 - y)
            if q == turn and d == 0:
                to_side(0, ybuf.at[q, 1]).wait_recv()
                part = part + side[0].astype(f32)
            ybuf[q, d] = part.astype(bf)
            if q == turn and d == 1:
                to_side(0, ybuf.at[q, d]).start()
            else:
                to_y(q, d).start()

    def rs_middle(q, ds):
        if ds[0] == far:
            got_all(rs1.at[q, :nz], c_recv.at[q, 0])
        for d in ds:
            part = core_sum(q, across(d) * SIDE + y)
            if q != turn or d != 1:
                to_y(q, d).wait_recv()
                part = part + rs2[q, d].astype(f32)
            if d == 0:
                mix[q, :rows, :] = part
                if q == 0:
                    dg_s[q] = part.astype(bf)
                    pl.when(cross)(to_diag(q).start)
            elif d == far and q in MERGED:
                zbuf[q, d - 1] = part.astype(bf)
                pl.when(inner_z)(to_z(q, d).start)
                pl.when(jnp.logical_not(inner_z))(to_side(q, zbuf.at[q, d - 1]).start)
            elif d == 2 and q in MERGED:
                pl.when(inner_z)(to_side(q, zbuf.at[q, d - 1]).wait_recv)
                extra = jnp.where(inner_z, side[q].astype(f32), 0.0)
                zbuf[q, d - 1] = (part + extra).astype(bf)
                to_z(q, d).start()
            else:
                zbuf[q, d - 1] = part.astype(bf)
                to_z(q, d).start()

    sums = []

    def gain_term(parts, gain):
        lanes_sum = parts[0]
        for part in parts[1:]:
            lanes_sum = lanes_sum + part
        return jnp.sum(lanes_sum.T, axis=0, keepdims=True) / gain

    def rs_end(q):
        result = mix[q, :rows, :]
        if q == 0:
            pl.when(cross)(to_diag(q).wait_recv)
            result = jnp.where(cross, dg_r[q].astype(f32), result)
        if q in MERGED:
            pl.when(inner_z)(lambda: got_all(rs3.at[q], z_recv.at[q]))
            pl.when(ends_z)(lambda: got_all(rs3.at[q, : far - 1], z_recv.at[q]))
        else:
            got_all(rs3.at[q], z_recv.at[q])
        for d in hops:
            part = rs3[q, d - 1].astype(f32)
            result = result + (jnp.where(inner_z, part, 0.0) if d == far and q in MERGED else part)
        store(q, result)
        if q:
            prod = wbuf[q, block].astype(f32) * result
            sums.append(prod[:, :HD] + prod[:, HD:])
            dg_s[q] = result.astype(bf)
            pl.when(cross)(to_diag(q).start)
            return
        prod = jnp.where(cross, w_own[...], wbuf[q, block]).astype(f32) * result
        gain = jnp.where(cross, gain_own[...], gbuf[:, gcol(block)])
        gg_ref[...] = gain_term([prod[:, :HD] + prod[:, HD:]], gain) + jnp.where(cross, gg_r[...], gg_s[...])

    def store(q, result):
        if q == 0:
            wg_ref[:, qcols:] = result
        else:
            for xx in range(2):
                first = (xx * half + q - 1) * HD
                wg_ref[:, first : first + HD] = result[:, xx * HD : (xx + 1) * HD]

    def rs_head(n):
        gq_msg[n].wait_recv()
        rs_terms(1 + n, jnp.concatenate([gq[n, 0], gq[n, 1]], axis=1))

    send_q(1)
    inner, grad_keys, grad_values = head(0, inner, grad_keys, grad_values)
    at_msg = [x_push(at_s.at[0, there], at_r.at[0])]
    block = c * chips + z * SIDE + y
    cross = c != x

    def to_diag(q):
        return rcopy(dg_s.at[q], dg_r.at[q], d_send.at[0], d_recv.at[min(q, 1)], d_peer)

    w_copy = rcopy(wbuf.at[0, block], w_own, d_send.at[0], d_recv.at[2], d_peer)
    gain_copy = rcopy(gbuf.at[:, gcol(block)], gain_own, d_send.at[1], d_recv.at[3], d_peer)
    gg_copy = rcopy(gg_s, gg_r, d_send.at[1], d_recv.at[4], d_peer)
    pl.when(cross)(w_copy.start)
    pl.when(cross)(gain_copy.start)
    rs_head(0)
    inner, grad_keys, grad_values = head(1, inner, grad_keys, grad_values)
    grad_keys = unrope(grad_keys)
    gkv_s[:, :HD] = grad_keys.astype(bf)
    gkv_s[:, HD:] = grad_values.astype(bf)
    gkv_msg = x_push(gkv_s, gkv_r)
    inner_all = jnp.broadcast_to(inner, (seq, HD))
    in_s[...] = inner_all.T[:8, :]
    in_msg = x_push(in_s, in_r, 2)
    at_msg.append(x_push(at_s.at[1, there], at_r.at[1]))
    for n in range(half):
        attn_ref[:, pl.ds(pl.multiple_of((x * half + n) * HD, HD), HD)] = at_s[n, here, :]

    rs_sums(1, [d for d in order if d == 1] + [d for d in order if d > 1])
    rs_head(1)
    rs_sums(1, [0])
    rs_sums(2, order)
    gkv_msg.wait_recv()
    keys_sum = gkv_s[:, :HD].astype(f32) + gkv_r[:, :HD].astype(f32)
    values_sum = gkv_s[:, HD:].astype(f32) + gkv_r[:, HD:].astype(f32)
    gkv_all = jnp.concatenate([keys_sum, values_sum], axis=1).astype(bf)
    rs_middle(1, [far, 1])
    in_msg.wait_recv()
    inner = inner + jnp.broadcast_to(in_r[:1, :], (HD, seq)).T[:, :1]
    inner = inner + jnp.sum(gkv_all.astype(f32) * mix[0], axis=1, keepdims=True)
    inv = inv_all[...]
    inv_all[...] = inner * (inv * inv / width)

    gqs = [jnp.concatenate([gq[n, 0], gq[n, 1]], axis=1) for n in range(half)]
    for p in range(PIECES):
        out = jnp.zeros((seq, lanes), f32)
        for q in range(chunks):
            w = wbuf[q, p * span : (p + 1) * span].reshape(lanes, CHUNK)
            out = out + nt_dot(gkv_all if q == 0 else gqs[q - 1], w)
        gain = gbuf[:, p * lanes : (p + 1) * lanes]
        gi_s[p] = (gain * out * inv[:, :1] - hx[p].astype(f32) * inv_all[:, :1]).astype(bf)
        x_push(gi_s.at[p, there], gi_r.at[p], 0, 1)
    queue = list(range(1, chunks)) + [0]
    rs_terms(0, gkv_all)
    rs_middle(1, [2])
    rs_sums(0, order)
    rs_middle(1, [0])
    rs_middle(2, [far, 1])
    for p in range(PIECES):
        for b in range(span):
            j = p * span + b
            gin_ref[:, pl.ds(pl.multiple_of((2 * j + x) * rows, rows), rows)] = gi_s[p, here, b * rows : (b + 1) * rows]
    rs_middle(2, [2, 0])
    rs_end(1)
    rs_middle(0, order)
    rs_end(2)
    gg_s[...] = gain_term(sums, gbuf[:, gcol(block)])
    pl.when(cross)(gg_copy.start)
    for n in range(half):
        at_msg[n].wait_recv()
        attn_ref[:, pl.ds(pl.multiple_of(((1 - x) * half + n) * HD, HD), HD)] = at_r[n]
    got_all(gi_r, x_recv.at[1])
    for p in range(PIECES):
        for b in range(span):
            j = p * span + b
            gin_ref[:, pl.ds(pl.multiple_of((2 * j + 1 - x) * rows, rows), rows)] = gi_r[p, :, b * rows : (b + 1) * rows]


    @pl.when(cross)
    def _():
        w_copy.wait_recv()
        gain_copy.wait_recv()
        gg_copy.wait_recv()
        got_all(dg_r.at[1:], d_recv.at[1])
        for q in range(1, chunks):
            store(q, dg_r[q].astype(f32))

    rs_end(0)
    for t in range(steps):
        near_sends = wbuf.at[t // SPLIT, : n_inter - 2, pl.ds(0, rows // SPLIT)]
        all_sends = wbuf.at[t // SPLIT, :, pl.ds(0, rows // SPLIT)]
        pl.when(inner_z)(lambda: sent_all(all_sends, ag_send.at[t]))
        pl.when(ends_z)(lambda: sent_all(near_sends, ag_send.at[t]))
    sent_all(gbuf.at[:, : len(plane) * rows], g_sem.at[0])
    sent_all(wbuf.at[:2, :13], x_send.at[0])
    sent_all(inv_s, x_send.at[1])
    sent_all(in_s, x_send.at[2])
    sent_all(tbuf.at[:, :chips], c_send)
    sent_all(tbuf.at[:, :7], r_send)

    @pl.when(cross)
    def _():
        sent_all(wbuf.at[0, : chunks + 1], d_send.at[0])
        sent_all(gbuf.at[:, : 2 * rows], d_send.at[1])


def copy_kernel(*refs):
    sems = refs[8]
    copies = [pltpu.make_async_copy(refs[k], refs[4 + k], sems.at[k]) for k in range(4)]
    for cp in copies:
        cp.start()
    for cp in copies:
        cp.wait()


def fused(n_inter, hidden_in, norm_gain, qkv_weight, attn_cotangent):
    toks, width = hidden_in.shape[1:]
    rows, cols = qkv_weight.shape
    nz = n_inter // (CORES * SIDE)
    chips = nz * SIDE
    seq, half, chunks = 2 * toks, HEADS // 2, cols // CHUNK
    lanes = n_inter // PIECES * rows
    freqs = rope_base ** (-np.arange(HD // 2, dtype=np.float32) / np.float32(HD // 2))
    angles = (np.arange(seq, dtype=np.float32)[:, None] * freqs.astype(np.float32)[None, :]).astype(np.float32)
    cosine = np.concatenate([np.cos(angles)] * 2, axis=1).astype(np.float32)
    sine = np.concatenate([-np.sin(angles), np.sin(angles)], axis=1).astype(np.float32)
    bf, f32, dma = jnp.bfloat16, jnp.float32, pltpu.SemaphoreType.DMA
    vmem = pl.BlockSpec(memory_space=pltpu.VMEM)
    hbm = pl.BlockSpec(memory_space=pltpu.HBM)
    V = pltpu.VMEM
    ins = (hidden_in[0], norm_gain[None], qkv_weight, attn_cotangent[0], jnp.asarray(cosine), jnp.asarray(sine))
    attn, gin, wg, gg = pl.pallas_call(
        functools.partial(fused_kernel, n_inter),
        out_shape=(V((toks, HEADS * HD), bf), V((toks, width), bf), V((rows, cols), f32), V((1, rows), f32)),
        in_specs=[hbm] * 6,
        out_specs=(vmem,) * 4,
        scratch_shapes=[
            V((chunks, n_inter, rows, CHUNK), bf),
            V((1, n_inter * rows), f32),
            V((1, rows), bf),
            V((PIECES, seq, lanes), bf),
            V((PIECES, toks, lanes), bf),
            V((PIECES, seq, lanes), bf),
            V((n_inter * rows, seq), bf),
            V((seq, HD), f32),
            V((8, toks), f32),
            V((8, toks), f32),
            V((seq, half * HD), bf),
            V((toks, half * HD), bf),
            V((seq, HD), f32),
            V((seq, HD), f32),
            V((chunks, seq, CHUNK), f32),
            V((seq, CHUNK), bf),
            V((seq, CHUNK), bf),
            V((half, seq, HD), bf),
            V((half, seq, HD), bf),
            V((half, 2, seq, HD), bf),
            V((seq, CHUNK), bf),
            V((seq, CHUNK), bf),
            V((8, seq), f32),
            V((8, seq), f32),
            V((half, seq, HD), bf),
            V((half, toks, HD), bf),
            V((PIECES, seq, lanes), bf),
            V((PIECES, toks, lanes), bf),
            V((chunks, n_inter, rows, CHUNK), bf),
            V((chunks, chips, rows, CHUNK), bf),
            V((chunks, nz, rows, CHUNK), bf),
            V((chunks, nz, rows, CHUNK), bf),
            V((chunks, nz - 1, rows, CHUNK), bf),
            V((chunks, nz - 1, rows, CHUNK), bf),
            V((chunks, rows, CHUNK), bf),
            V((chunks, rows, CHUNK), bf),
            V((chunks, rows, CHUNK), bf),
            V((1, rows), f32),
            V((1, rows), f32),
            V((rows, CHUNK), bf),
            V((1, rows), f32),
            dma((8,)),
            dma((chunks * SPLIT,)), dma((chunks * SPLIT, chips)), dma((chunks * SPLIT,)),
            dma((2,)), dma((3,)), dma((13,)),
            dma, dma((chunks, 2)), dma, dma((chunks, nz)), dma((chunks,)), dma((chunks,)),
            dma((2,)), dma((5,)),
        ],
        compiler_params=pltpu.CompilerParams(
            collective_id=0, has_side_effects=True, vmem_limit_bytes=32 * 2**20
        ),
    )(*[pltpu.with_memory_space_constraint(a, pltpu.HBM) for a in ins])
    outs = (attn, gin, wg, gg)
    attn, gin, wg, gg = pl.pallas_call(
        copy_kernel,
        out_shape=tuple(jax.ShapeDtypeStruct(o.shape, o.dtype) for o in outs),
        in_specs=[vmem] * 4,
        out_specs=(hbm,) * 4,
        scratch_shapes=[dma((4,))],
        compiler_params=pltpu.CompilerParams(vmem_limit_bytes=2**20),
    )(*[pltpu.with_memory_space_constraint(o, pltpu.VMEM) for o in outs])
    return attn[None], gin[None], wg, gg[0]


def solution(mesh):
    n_inter, n_intra = mesh.shape["inter"], mesh.shape["intra"]

    def body(hidden_in, norm_gain, qkv_weight, attn_cotangent):
        nz = n_inter // (CORES * SIDE)
        fits = n_intra == 2 and n_inter % (CORES * SIDE) == 0 and nz > 1 and nz & (nz - 1) == 0
        fits = fits and qkv_weight.shape[0] == HD and hidden_in.shape[0] == 1
        fits = fits and hidden_in.shape[1] == HD and n_inter % PIECES == 0 and HEADS == 4 and nz == 4
        if fits:
            return fused(n_inter, hidden_in, norm_gain, qkv_weight, attn_cotangent)
        return local(hidden_in, norm_gain, qkv_weight, attn_cotangent)

    return jax.shard_map(
        body,
        mesh=mesh,
        in_specs=(
            P("inter", "intra", None),
            P(("inter", "intra")),
            P(("inter", "intra"), None),
            P("inter", "intra", None),
        ),
        out_specs=(
            P("inter", "intra", None),
            P("inter", "intra", None),
            P(("intra", "inter"), None),
            P(("intra", "inter")),
        ),
        check_vma=False,
    )
```

```python
import functools
import jax
import jax.numpy as jnp
import numpy as np
from jax import lax
from jax.experimental import pallas as pl
from jax.experimental.pallas import tpu as pltpu
from jax.sharding import PartitionSpec as P

HD = 128
HEADS = 4


eps_norm = 1e-05
rope_base = 500000.0


def rope_tables(positions, head_size):
    half_size = head_size // 2
    freqs = rope_base ** (-jnp.arange(half_size, dtype=jnp.float32) / half_size)
    angles = positions.astype(jnp.float32)[:, None] * freqs[None, :]
    return (jnp.cos(angles), jnp.sin(angles))


def rotate(values_in, cosine, sine):
    half_size = values_in.shape[-1] // 2
    first, second = (values_in[..., :half_size], values_in[..., half_size:])
    return jnp.concatenate(
        [first * cosine - second * sine, second * cosine + first * sine], axis=-1
    )


def unrotate(grad_out, cosine, sine):
    half_size = grad_out.shape[-1] // 2
    first, second = (grad_out[..., :half_size], grad_out[..., half_size:])
    return jnp.concatenate(
        [first * cosine + second * sine, second * cosine - first * sine], axis=-1
    )


def forward_fold(query_rows, row_pos):

    def forward_advance(carry, piece, start):
        row_top, row_total, weighted = carry
        key_part, value_part = piece
        scores = jnp.einsum("qd,kd->qk", query_rows, key_part, preferred_element_type=jnp.float32)
        key_pos = jnp.arange(key_part.shape[0], dtype=jnp.int32)
        allowed = key_pos[None, :] <= row_pos[:, None]
        scores = jnp.where(allowed, scores, -1e30)
        new_top = jnp.maximum(row_top, jnp.max(scores, axis=1))
        numbers = jnp.where(allowed, jnp.exp(scores - new_top[:, None]), 0.0)
        row_total = jnp.sum(numbers, axis=1)
        weighted = jnp.dot(
            numbers,
            value_part.astype(jnp.float32),
            precision=lax.Precision.HIGHEST,
            preferred_element_type=jnp.float32,
        )
        return (new_top, row_total, weighted)

    return forward_advance


def query_grad_fold(query_rows, row_pos, grad_flat, log_total, row_delta):

    def query_advance(grad_query, piece, start):
        key_part, value_part = piece
        scores = jnp.einsum("qd,kd->qk", query_rows, key_part, preferred_element_type=jnp.float32)
        key_pos = jnp.arange(key_part.shape[0], dtype=jnp.int32)
        allowed = key_pos[None, :] <= row_pos[:, None]
        probs = jnp.where(
            allowed, jnp.exp(jnp.where(allowed, scores, -1e30) - log_total[:, None]), 0.0
        )
        grad_probs = jnp.einsum(
            "qd,kd->qk", grad_flat, value_part, preferred_element_type=jnp.float32
        )
        grad_scores = (probs * (grad_probs - row_delta[:, None])).astype(jnp.bfloat16)
        return jnp.dot(grad_scores, key_part, preferred_element_type=jnp.float32)

    return query_advance


def key_grad_fold(key_rows, value_rows, key_pos, log_all, delta_all, heads_count):

    def key_advance(carry, piece, start):
        query_part, attn_grad_part = piece
        count = query_part.shape[0]
        scores = jnp.einsum("qd,kd->qk", query_part, key_rows, preferred_element_type=jnp.float32)
        query_pos = jnp.arange(count, dtype=jnp.int32) // heads_count
        allowed = key_pos[None, :] <= query_pos[:, None]
        probs = jnp.where(
            allowed, jnp.exp(jnp.where(allowed, scores, -1e30) - log_all[:, None]), 0.0
        )
        grad_values = jnp.einsum(
            "qk,qd->kd",
            probs.astype(jnp.bfloat16),
            attn_grad_part,
            preferred_element_type=jnp.float32,
        )
        grad_probs = jnp.einsum(
            "qd,kd->qk", attn_grad_part, value_rows, preferred_element_type=jnp.float32
        )
        grad_scores = (probs * (grad_probs - delta_all[:, None])).astype(jnp.bfloat16)
        grad_keys = jnp.einsum(
            "qk,qd->kd", grad_scores, query_part, preferred_element_type=jnp.float32
        )
        return (grad_keys, grad_values)

    return key_advance


def local(hidden_in, norm_gain, qkv_weight, attn_cotangent):
    rows_in = hidden_in[0]
    grad_attn = attn_cotangent[0]
    tokens_here = rows_in.shape[0]
    width = rows_in.shape[1]
    head_size = HD
    heads_count = HEADS
    qcols = heads_count * head_size
    scale = head_size ** (-0.5)
    weight_group, gain_group = (
        lax.all_gather(qkv_weight, "intra", axis=0, tiled=True),
        lax.all_gather(norm_gain, "intra", axis=0, tiled=True),
    )
    weight_full, gain_full = (
        lax.all_gather(weight_group, "inter", axis=0, tiled=True),
        lax.all_gather(gain_group, "inter", axis=0, tiled=True),
    )
    query_pos = lax.axis_index("intra") * tokens_here + jnp.arange(tokens_here, dtype=jnp.int32)
    row_pos = jnp.broadcast_to(query_pos[:, None], (tokens_here, heads_count)).reshape(
        tokens_here * heads_count
    )
    cosine, sine = rope_tables(query_pos, head_size)
    wide_rows = rows_in.astype(jnp.float32)
    inv_rms = lax.rsqrt(jnp.mean(wide_rows * wide_rows, axis=1, keepdims=True) + eps_norm)
    normed = (wide_rows * inv_rms * gain_full.astype(jnp.float32)[None, :]).astype(jnp.bfloat16)
    mixed = jnp.dot(normed, weight_full, preferred_element_type=jnp.float32)
    query_rows = (
        (
            rotate(
                mixed[:, :qcols].reshape(tokens_here, heads_count, head_size),
                cosine[:, None, :],
                sine[:, None, :],
            )
            * scale
        )
        .astype(jnp.bfloat16)
        .reshape(tokens_here * heads_count, head_size)
    )
    key_rows = rotate(mixed[:, qcols : qcols + head_size], cosine, sine).astype(jnp.bfloat16)
    value_rows = mixed[:, qcols + head_size :].astype(jnp.bfloat16)
    grad_flat = grad_attn.reshape(tokens_here * heads_count, head_size)
    flat_rows = tokens_here * heads_count
    forward_step = forward_fold(query_rows, row_pos)
    start_carry = (
        jnp.full((flat_rows,), -1e30, jnp.float32),
        jnp.zeros((flat_rows,), jnp.float32),
        jnp.zeros((flat_rows, head_size), jnp.float32),
    )
    row_top, row_total, weighted = forward_step(
        start_carry,
        (
            lax.all_gather(key_rows, "intra", axis=0, tiled=True),
            lax.all_gather(value_rows, "intra", axis=0, tiled=True),
        ),
        jnp.int32(0),
    )
    attn_flat = (weighted / row_total[:, None]).astype(jnp.bfloat16)
    log_total = row_top + jnp.log(row_total)
    row_delta = jnp.sum(grad_flat.astype(jnp.float32) * attn_flat.astype(jnp.float32), axis=1)
    query_step = query_grad_fold(query_rows, row_pos, grad_flat, log_total, row_delta)
    grad_query = query_step(
        jnp.zeros((flat_rows, head_size), jnp.float32),
        (
            lax.all_gather(key_rows, "intra", axis=0, tiled=True),
            lax.all_gather(value_rows, "intra", axis=0, tiled=True),
        ),
        jnp.int32(0),
    )
    log_all, delta_all = (
        lax.all_gather(log_total, "intra", axis=0, tiled=True),
        lax.all_gather(row_delta, "intra", axis=0, tiled=True),
    )
    key_step = key_grad_fold(key_rows, value_rows, query_pos, log_all, delta_all, heads_count)
    grad_keys, grad_values = key_step(
        (
            jnp.zeros((tokens_here, head_size), jnp.float32),
            jnp.zeros((tokens_here, head_size), jnp.float32),
        ),
        (
            lax.all_gather(query_rows, "intra", axis=0, tiled=True),
            lax.all_gather(grad_flat, "intra", axis=0, tiled=True),
        ),
        jnp.int32(0),
    )
    query_back = (
        unrotate(
            grad_query.reshape(tokens_here, heads_count, head_size),
            cosine[:, None, :],
            sine[:, None, :],
        )
        * scale
    ).reshape(tokens_here, qcols)
    grad_mixed = jnp.concatenate(
        [query_back, unrotate(grad_keys, cosine, sine), grad_values], axis=1
    ).astype(jnp.bfloat16)
    weight_back, gain_back = (weight_full, gain_full)
    gain_wide = gain_back.astype(jnp.float32)[None, :]
    grad_normed = jnp.einsum(
        "tc,dc->td", grad_mixed, weight_back, preferred_element_type=jnp.float32
    )
    inner = jnp.sum(grad_normed * gain_wide * wide_rows, axis=1, keepdims=True)
    grad_rows = (
        gain_wide * grad_normed * inv_rms - wide_rows * inv_rms**3 / width * inner
    ).astype(jnp.bfloat16)
    gain_term = jnp.sum(grad_normed * wide_rows * inv_rms, axis=0)
    normed_cols = lax.all_to_all(normed, "intra", split_axis=1, concat_axis=0, tiled=True)
    group_term = lax.dot_general(
        normed_cols,
        lax.all_gather(grad_mixed, "intra", axis=0, tiled=True),
        (((0,), (0,)), ((), ())),
        preferred_element_type=jnp.float32,
    )
    term_low = lax.optimization_barrier(group_term.astype(jnp.bfloat16))
    gain_sums = lax.psum_scatter(gain_term, "intra", scatter_dimension=0, tiled=True)
    weight_grad, gain_grad = (
        lax.psum_scatter(term_low.astype(jnp.float32), "inter", scatter_dimension=0, tiled=True),
        lax.psum_scatter(gain_sums, "inter", scatter_dimension=0, tiled=True),
    )
    return (attn_flat.reshape(tokens_here, qcols)[None], grad_rows[None], weight_grad, gain_grad)

MESH = pl.DeviceIdType.MESH
CORES = 2
SIDE = 2
PIECES = 4
CHUNK = 2 * HD
SPLIT = 1
LAG = 1
HELD = 2
HELD_UNTIL = 0
MERGED = (1, 2)


def nt_dot(a, b):
    return lax.dot_general(a, b, (((1,), (1,)), ((), ())), preferred_element_type=jnp.float32)


def tn_dot(a, b):
    return lax.dot_general(a, b, (((0,), (0,)), ((), ())), preferred_element_type=jnp.float32)


def nn_dot(a, b):
    return jnp.dot(a, b, preferred_element_type=jnp.float32)


def fused_kernel(
    n_inter,
    hid_ref, gain_ref, w_ref, ct_ref, cos_hbm, sin_hbm,
    attn_ref, gin_ref, wg_ref, gg_ref,
    wbuf, gbuf, gain_in, hx, hs, nbuf, ntr, inv_all, inv_s, inv_r, ctb, cts, cos_ref, sin_ref,
    mix, kv_s, kv_r, qm_s, qm_r, gq, gkv_s, gkv_r, in_s, in_r, at_s, at_r, gi_s, gi_r,
    tbuf, rs1, ybuf, rs2, zbuf, rs3, side, dg_s, dg_r, gg_s, gg_r, w_own, gain_own,
    ld_sem, ag_send, ag_recv, ag_core, g_sem, x_send, x_recv,
    c_send, c_recv, r_send, y_recv, z_recv, s_recv, d_send, d_recv,
):
    i = lax.axis_index("inter")
    x = lax.axis_index("intra")
    nz = n_inter // (CORES * SIDE)
    c = lax.rem(i, CORES)
    y = lax.rem(i // CORES, SIDE)
    z = i // (CORES * SIDE)
    toks, width = hid_ref.shape
    rows, cols = w_ref.shape
    seq = 2 * toks
    qcols = HEADS * HD
    chips = nz * SIDE
    chunks = cols // CHUNK
    span = n_inter // PIECES
    lanes = span * rows
    scale = HD ** (-0.5)
    f32, bf = jnp.float32, jnp.bfloat16

    def dev(zz, yy, cc, xx):
        return ((zz * SIDE + yy) * CORES + cc, xx)

    def slot(zz, yy, cc):
        return (zz * SIDE + yy) * CORES + cc

    def across(d):
        zz, bit = z, 1
        while bit < nz:
            if d & bit:
                zz = zz + bit - 2 * bit * lax.rem(z // bit, 2)
            bit *= 2
        return zz

    hops = list(range(1, nz))
    x_peer = dev(z, y, c, 1 - x)
    y_peer = dev(z, 1 - y, c, x)
    c_peer = dev(z, y, 1 - c, x)
    d_peer = dev(z, y, 1 - c, 1 - x)
    plane = [(d, yy, cc) for d in range(nz) for yy in (0, 1) for cc in (0, 1) if d or yy or cc]

    def plane_dev(e):
        d, yy, cc = e
        return (across(d), y + yy - 2 * yy * y, c + cc - 2 * cc * c)

    own = slot(z, y, c)
    here = pl.ds(pl.multiple_of(x * toks, toks), toks)
    there = pl.ds(pl.multiple_of((1 - x) * toks, toks), toks)

    def rcopy(src, dst, ss, rs, device):
        return pltpu.make_async_remote_copy(
            src_ref=src, dst_ref=dst, send_sem=ss, recv_sem=rs, device_id=device, device_id_type=MESH
        )

    barrier = pltpu.get_barrier_semaphore()
    peers = [dev(*plane_dev(e), x) for e in plane] + [x_peer, d_peer]
    for peer in peers:
        pl.semaphore_signal(barrier, inc=1, device_id=peer, device_id_type=MESH)

    def load(src, dst, k):
        pltpu.make_async_copy(src, dst, ld_sem.at[k]).start()

    def loaded(dst, k):
        pltpu.make_async_copy(dst, dst, ld_sem.at[k]).wait()

    load(w_ref.at[:, qcols:], wbuf.at[0, own], 2)
    half = HEADS // 2
    for n in range(half):
        for xx in range(2):
            first = (xx * half + n) * HD
            load(w_ref.at[:, first : first + HD], wbuf.at[1 + n, own, :, xx * HD : (xx + 1) * HD], 2)
    nxt = 3
    load(gain_ref, gain_in, nxt)
    for p in range(PIECES):
        for b in range(span):
            other = pl.ds(pl.multiple_of((2 * (p * span + b) + 1 - x) * rows, rows), rows)
            load(hid_ref.at[:, other], hs.at[p, :, b * rows : (b + 1) * rows], 1)
    for p in range(PIECES):
        for b in range(span):
            mine = pl.ds(pl.multiple_of((2 * (p * span + b) + x) * rows, rows), rows)
            load(hid_ref.at[:, mine], hx.at[p, here, b * rows : (b + 1) * rows], 0)
    load(ct_ref.at[:, pl.ds(pl.multiple_of(x * half * HD, HD), half * HD)], ctb.at[here], nxt + 1)
    load(ct_ref.at[:, pl.ds(pl.multiple_of((1 - x) * half * HD, HD), half * HD)], cts, nxt + 2)
    load(cos_hbm, cos_ref, nxt + 3)
    load(sin_hbm, sin_ref, nxt + 4)

    loaded(gain_in, nxt)
    gcol = lambda g: pl.ds(pl.multiple_of(g * rows, rows), rows)
    gbuf[:, gcol(own)] = gain_in[...].astype(f32)
    loaded(wbuf.at[:, own], 2)
    pl.semaphore_wait(barrier, len(peers))

    inner_z = jnp.logical_and(z > 0, z < nz - 1)
    far = nz - 1
    steps = chunks * SPLIT
    spare = steps - 1

    def ag(t, g, device, core=False):
        part = wbuf.at[t // SPLIT, g, pl.ds(t % SPLIT * (rows // SPLIT), rows // SPLIT)]
        rs = ag_core.at[t] if core else ag_recv.at[t, g // CORES]
        return rcopy(part, part, ag_send.at[t], rs, device)

    def arrive(t, g):
        ag(t, g, x_peer).wait_recv()

    def sent_all(ref, sem):
        rcopy(ref, ref, sem, d_recv.at[0], x_peer).wait_send()

    def got_all(ref, sem):
        rcopy(ref, ref, d_send.at[0], sem, x_peer).wait_recv()

    def push(t, g, device, core=False, cond=None):
        cp = ag(t, g, device, core)
        if cond is None:
            cp.start()
        else:
            pl.when(cond)(cp.start)

    for n, e in enumerate(plane):
        rcopy(gbuf.at[:, gcol(own)], gbuf.at[:, gcol(own)], g_sem.at[0], g_sem.at[1],
              dev(*plane_dev(e), x)).start()
    ends_z = jnp.logical_not(inner_z)

    def own_z(t, late=False):
        for d in hops[::-1]:
            if d == far:
                cond = inner_z
            else:
                cond = (inner_z if late else ends_z) if t >= HELD else None
            if d != far or not late:
                push(t, own, dev(across(d), y, c, x), cond=cond)

    def own_y(t):
        push(t, own, y_peer)
        push(t, own, c_peer, core=True)

    for t in range(steps):
        own_z(t)
        own_y(t)
    messages = []

    def x_push(src, dst, ss=0, rs=None):
        if rs is None:
            rs = len(messages) + 2
            messages.append(rs)
        cp = rcopy(src, dst, x_send.at[ss], x_recv.at[rs], x_peer)
        cp.start()
        return cp

    loaded(hs, 1)
    x_push(hs.at[0], hx.at[0, here], 0, 0)
    loaded(hx.at[:, here], 0)
    total = jnp.zeros((toks, 1), f32)
    for p in range(PIECES):
        a = hx[p, here, :].astype(f32)
        b = hs[p].astype(f32)
        total = total + jnp.sum(a * a + b * b, axis=1, keepdims=True)
    inv = jnp.broadcast_to(lax.rsqrt(total / width + eps_norm), (toks, HD))
    inv_all[here, :] = inv
    inv_s[...] = inv.T[:8, :]
    inv_msg = x_push(inv_s, inv_r, 1)
    for p in range(1, PIECES):
        x_push(hs.at[p], hx.at[p, here], 0, 0)
    loaded(cts, nxt + 2)
    ct_msg = x_push(cts, ctb.at[here])

    def near(n):
        if n < 2:
            return across(n)
        return jnp.where(inner_z, across(nz + 1 - n), across(n))

    def z_arrivals(t):
        for n in hops:
            g = slot(near(n), y, c)
            arrive(t, g)
            if n == far:
                push(t, g, dev(across(1), y, c, x), cond=inner_z)
            if t != spare or n != 1:
                push(t, g, y_peer)
            push(t, g, c_peer, core=True)
        if t == HELD_UNTIL:
            for k in range(HELD, steps):
                own_z(k, True)

    def y_own(t):
        g = slot(z, 1 - y, c)
        arrive(t, g)
        if t == spare:
            push(t, g, dev(across(1), y, c, x))
        push(t, g, c_peer, core=True)

    def y_arrivals(t):
        for n in hops:
            g = slot(near(n), 1 - y, c)
            arrive(t, g)
            push(t, g, c_peer, core=True)

    def c_arrivals(q):
        for t in range(q * SPLIT, (q + 1) * SPLIT):
            got_all(wbuf.at[q, :chips, pl.ds(t % SPLIT * (rows // SPLIT), rows // SPLIT)], ag_core.at[t])

    def norm(which):
        scaled = inv_all[which, :1]
        for p in range(PIECES):
            value = hx[p, which, :].astype(f32) * scaled * gbuf[:, p * lanes : (p + 1) * lanes]
            value = value.astype(bf)
            nbuf[p, which, :] = value
            ntr[p * lanes : (p + 1) * lanes, which] = value.T

    def partial(q):
        out = [jnp.zeros((toks, CHUNK), f32)] * 2
        for p in range(PIECES):
            w = wbuf[q, p * span : (p + 1) * span].reshape(lanes, CHUNK)
            out = [o + nn_dot(nbuf[p, r * toks : (r + 1) * toks, :], w) for r, o in enumerate(out)]
        for r, o in enumerate(out):
            mix[q, r * toks : (r + 1) * toks, :] = o

    mycol = pl.ds(pl.multiple_of(x * HD, HD), HD)
    itscol = pl.ds(pl.multiple_of((1 - x) * HD, HD), HD)

    q_msg = []

    def send_q(n):
        c_arrivals(1 + n)
        partial(1 + n)
        qm_s[n] = mix[1 + n, :, itscol].astype(bf)
        q_msg.append(x_push(qm_s.at[n], qm_r.at[n]))

    for t in range(steps + LAG):
        if t < steps:
            z_arrivals(t)
            y_own(t)
        if t == LAG:
            got_all(gbuf.at[:, : len(plane) * rows], g_sem.at[1])
            norm(here)
        if t >= LAG:
            y_arrivals(t - LAG)
            if t - LAG == SPLIT - 1:
                inv_msg.wait_recv()
                got_all(hs, x_recv.at[0])
                inv_all[there, :] = jnp.broadcast_to(inv_r[:1, :], (toks, toks)).T
                norm(there)
                c_arrivals(0)
                partial(0)
                kv_s[...] = mix[0].astype(bf)
                kv_msg = x_push(kv_s, kv_r)
            if t - LAG == 2 * SPLIT - 1:
                send_q(0)

    loaded(cos_ref, nxt + 3)
    loaded(sin_ref, nxt + 4)
    loaded(ctb.at[here], nxt + 1)
    ct_msg.wait_recv()
    cosine, sine = cos_ref[...], sin_ref[...]

    def rope(u):
        return u * cosine + pltpu.roll(u, HD // 2, 1) * sine

    def unrope(u):
        return u * cosine - pltpu.roll(u, HD // 2, 1) * sine

    kv_msg.wait_recv()
    mix_kv = mix[0] + kv_r[...].astype(f32)
    mix[0] = mix_kv
    keys = rope(mix_kv[:, :HD]).astype(bf)
    values = mix_kv[:, HD:].astype(bf)
    allowed = lax.broadcasted_iota(jnp.int32, (seq, seq), 1) <= lax.broadcasted_iota(jnp.int32, (seq, seq), 0)
    inner = jnp.zeros((seq, 1), f32)
    grad_keys = jnp.zeros((seq, HD), f32)
    grad_values = jnp.zeros((seq, HD), f32)
    gq_msg = []

    def head(n, inner, grad_keys, grad_values):
        grad = ctb[:, n * HD : (n + 1) * HD]
        grad_probs = nt_dot(grad, values)
        q_msg[n].wait_recv()
        mixed = mix[1 + n, :, mycol] + qm_r[n].astype(f32)
        query = (rope(mixed) * scale).astype(bf)
        scores = jnp.where(allowed, nt_dot(query, keys), -1e30)
        top = jnp.max(scores, axis=1, keepdims=True)
        numbers = jnp.where(allowed, jnp.exp(scores - top), 0.0)
        share = 1.0 / jnp.sum(numbers, axis=1, keepdims=True)
        probs = numbers * share
        delta = jnp.sum(probs * grad_probs, axis=1, keepdims=True)
        grad_scores = (probs * (grad_probs - delta)).astype(bf)
        back = (unrope(nn_dot(grad_scores, keys)) * scale).astype(bf)
        gq[n, x] = back
        gq_msg.append(x_push(gq.at[n, x], gq.at[n, x]))
        high = numbers.astype(bf)
        low = (numbers - high.astype(f32)).astype(bf)
        at_s[n] = ((nn_dot(high, values) + nn_dot(low, values)) * share).astype(bf)
        inner = inner + jnp.sum(back.astype(f32) * mixed, axis=1, keepdims=True)
        grad_keys = grad_keys + tn_dot(grad_scores, query)
        grad_values = grad_values + tn_dot(probs.astype(bf), grad)
        return inner, grad_keys, grad_values

    def to_core(q, k):
        return rcopy(tbuf.at[q, (1 - c) * chips + k], rs1.at[q, k], c_send, c_recv.at[q, lax.rem(k + y, 2)], c_peer)

    def to_y(q, d):
        return rcopy(ybuf.at[q, d], rs2.at[q, d], r_send, y_recv.at[q, d], y_peer)

    def to_z(q, d):
        return rcopy(zbuf.at[q, d - 1], rs3.at[q, d - 1], r_send, z_recv.at[q],
                     dev(across(d), y, x, c) if q == 0 else dev(across(d), y, c, x))

    order = [far, 1, 2, 0]
    turn = 1

    def terms(q, grads, cc):
        group = chips // 4
        for r in range(4):
            first = cc * chips + r * group
            part = nn_dot(ntr[pl.ds(pl.multiple_of(first * rows, rows), group * rows), :], grads)
            tbuf[q, pl.ds(first, group)] = part.astype(bf).reshape(group, rows, CHUNK)

    def to_side(k, src):
        return rcopy(src, side.at[k], r_send, s_recv.at[k], dev(across(1), y, c, x))

    def core_sum(q, k):
        return tbuf[q, c * chips + k].astype(f32) + rs1[q, k].astype(f32)

    def rs_terms(q, grads):
        terms(q, grads, 1 - c)
        for yy in (1 - y, y):
            for d in order:
                to_core(q, across(d) * SIDE + yy).start()
        terms(q, grads, c)

    def rs_sums(q, ds):
        if ds[0]:
            got_all(rs1.at[q, :nz], c_recv.at[q, 1])
        for d in ds:
            part = core_sum(q, across(d) * SIDE + 1 - y)
            if q == turn and d == 0:
                to_side(0, ybuf.at[q, 1]).wait_recv()
                part = part + side[0].astype(f32)
            ybuf[q, d] = part.astype(bf)
            if q == turn and d == 1:
                to_side(0, ybuf.at[q, d]).start()
            else:
                to_y(q, d).start()

    def rs_middle(q, ds):
        if ds[0] == far:
            got_all(rs1.at[q, :nz], c_recv.at[q, 0])
        for d in ds:
            part = core_sum(q, across(d) * SIDE + y)
            if q != turn or d != 1:
                to_y(q, d).wait_recv()
                part = part + rs2[q, d].astype(f32)
            if d == 0:
                mix[q, :rows, :] = part
                if q == 0:
                    dg_s[q] = part.astype(bf)
                    pl.when(cross)(to_diag(q).start)
            elif d == far and q in MERGED:
                zbuf[q, d - 1] = part.astype(bf)
                pl.when(inner_z)(to_z(q, d).start)
                pl.when(jnp.logical_not(inner_z))(to_side(q, zbuf.at[q, d - 1]).start)
            elif d == 2 and q in MERGED:
                pl.when(inner_z)(to_side(q, zbuf.at[q, d - 1]).wait_recv)
                extra = jnp.where(inner_z, side[q].astype(f32), 0.0)
                zbuf[q, d - 1] = (part + extra).astype(bf)
                to_z(q, d).start()
            else:
                zbuf[q, d - 1] = part.astype(bf)
                to_z(q, d).start()

    sums = []

    def gain_term(parts, gain):
        lanes_sum = parts[0]
        for part in parts[1:]:
            lanes_sum = lanes_sum + part
        return jnp.sum(lanes_sum.T, axis=0, keepdims=True) / gain

    def rs_end(q):
        result = mix[q, :rows, :]
        if q == 0:
            pl.when(cross)(to_diag(q).wait_recv)
            result = jnp.where(cross, dg_r[q].astype(f32), result)
        if q in MERGED:
            pl.when(inner_z)(lambda: got_all(rs3.at[q], z_recv.at[q]))
            pl.when(ends_z)(lambda: got_all(rs3.at[q, : far - 1], z_recv.at[q]))
        else:
            got_all(rs3.at[q], z_recv.at[q])
        for d in hops:
            part = rs3[q, d - 1].astype(f32)
            result = result + (jnp.where(inner_z, part, 0.0) if d == far and q in MERGED else part)
        store(q, result)
        if q:
            prod = wbuf[q, block].astype(f32) * result
            sums.append(prod[:, :HD] + prod[:, HD:])
            dg_s[q] = result.astype(bf)
            pl.when(cross)(to_diag(q).start)
            return
        prod = jnp.where(cross, w_own[...], wbuf[q, block]).astype(f32) * result
        gain = jnp.where(cross, gain_own[...], gbuf[:, gcol(block)])
        gg_ref[...] = gain_term([prod[:, :HD] + prod[:, HD:]], gain) + jnp.where(cross, gg_r[...], gg_s[...])

    def store(q, result):
        if q == 0:
            wg_ref[:, qcols:] = result
        else:
            for xx in range(2):
                first = (xx * half + q - 1) * HD
                wg_ref[:, first : first + HD] = result[:, xx * HD : (xx + 1) * HD]

    def rs_head(n):
        gq_msg[n].wait_recv()
        rs_terms(1 + n, jnp.concatenate([gq[n, 0], gq[n, 1]], axis=1))

    send_q(1)
    inner, grad_keys, grad_values = head(0, inner, grad_keys, grad_values)
    at_msg = [x_push(at_s.at[0, there], at_r.at[0])]
    block = c * chips + z * SIDE + y
    cross = c != x

    def to_diag(q):
        return rcopy(dg_s.at[q], dg_r.at[q], d_send.at[0], d_recv.at[min(q, 1)], d_peer)

    w_copy = rcopy(wbuf.at[0, block], w_own, d_send.at[0], d_recv.at[2], d_peer)
    gain_copy = rcopy(gbuf.at[:, gcol(block)], gain_own, d_send.at[1], d_recv.at[3], d_peer)
    gg_copy = rcopy(gg_s, gg_r, d_send.at[1], d_recv.at[4], d_peer)
    pl.when(cross)(w_copy.start)
    pl.when(cross)(gain_copy.start)
    rs_head(0)
    inner, grad_keys, grad_values = head(1, inner, grad_keys, grad_values)
    grad_keys = unrope(grad_keys)
    gkv_s[:, :HD] = grad_keys.astype(bf)
    gkv_s[:, HD:] = grad_values.astype(bf)
    gkv_msg = x_push(gkv_s, gkv_r)
    inner_all = jnp.broadcast_to(inner, (seq, HD))
    in_s[...] = inner_all.T[:8, :]
    in_msg = x_push(in_s, in_r, 2)
    at_msg.append(x_push(at_s.at[1, there], at_r.at[1]))
    for n in range(half):
        attn_ref[:, pl.ds(pl.multiple_of((x * half + n) * HD, HD), HD)] = at_s[n, here, :]

    rs_sums(1, [d for d in order if d == 1] + [d for d in order if d > 1])
    rs_head(1)
    rs_sums(1, [0])
    rs_sums(2, order)
    gkv_msg.wait_recv()
    keys_sum = gkv_s[:, :HD].astype(f32) + gkv_r[:, :HD].astype(f32)
    values_sum = gkv_s[:, HD:].astype(f32) + gkv_r[:, HD:].astype(f32)
    gkv_all = jnp.concatenate([keys_sum, values_sum], axis=1).astype(bf)
    rs_middle(1, [far, 1])
    in_msg.wait_recv()
    inner = inner + jnp.broadcast_to(in_r[:1, :], (HD, seq)).T[:, :1]
    inner = inner + jnp.sum(gkv_all.astype(f32) * mix[0], axis=1, keepdims=True)
    inv = inv_all[...]
    inv_all[...] = inner * (inv * inv / width)

    gqs = [jnp.concatenate([gq[n, 0], gq[n, 1]], axis=1) for n in range(half)]
    for p in range(PIECES):
        out = jnp.zeros((seq, lanes), f32)
        for q in range(chunks):
            w = wbuf[q, p * span : (p + 1) * span].reshape(lanes, CHUNK)
            out = out + nt_dot(gkv_all if q == 0 else gqs[q - 1], w)
        gain = gbuf[:, p * lanes : (p + 1) * lanes]
        gi_s[p] = (gain * out * inv[:, :1] - hx[p].astype(f32) * inv_all[:, :1]).astype(bf)
        x_push(gi_s.at[p, there], gi_r.at[p], 0, 1)
    queue = list(range(1, chunks)) + [0]
    rs_terms(0, gkv_all)
    rs_middle(1, [2])
    rs_sums(0, order)
    rs_middle(1, [0])
    rs_middle(2, [far, 1])
    for p in range(PIECES):
        for b in range(span):
            j = p * span + b
            gin_ref[:, pl.ds(pl.multiple_of((2 * j + x) * rows, rows), rows)] = gi_s[p, here, b * rows : (b + 1) * rows]
    rs_middle(2, [2, 0])
    rs_end(1)
    rs_middle(0, order)
    rs_end(2)
    gg_s[...] = gain_term(sums, gbuf[:, gcol(block)])
    pl.when(cross)(gg_copy.start)
    for n in range(half):
        at_msg[n].wait_recv()
        attn_ref[:, pl.ds(pl.multiple_of(((1 - x) * half + n) * HD, HD), HD)] = at_r[n]
    got_all(gi_r, x_recv.at[1])
    for p in range(PIECES):
        for b in range(span):
            j = p * span + b
            gin_ref[:, pl.ds(pl.multiple_of((2 * j + 1 - x) * rows, rows), rows)] = gi_r[p, :, b * rows : (b + 1) * rows]


    @pl.when(cross)
    def _():
        w_copy.wait_recv()
        gain_copy.wait_recv()
        gg_copy.wait_recv()
        got_all(dg_r.at[1:], d_recv.at[1])
        for q in range(1, chunks):
            store(q, dg_r[q].astype(f32))

    rs_end(0)
    for t in range(steps):
        near_sends = wbuf.at[t // SPLIT, : n_inter - 2, pl.ds(0, rows // SPLIT)]
        all_sends = wbuf.at[t // SPLIT, :, pl.ds(0, rows // SPLIT)]
        pl.when(inner_z)(lambda: sent_all(all_sends, ag_send.at[t]))
        pl.when(ends_z)(lambda: sent_all(near_sends, ag_send.at[t]))
    sent_all(gbuf.at[:, : len(plane) * rows], g_sem.at[0])
    sent_all(wbuf.at[:2, :13], x_send.at[0])
    sent_all(inv_s, x_send.at[1])
    sent_all(in_s, x_send.at[2])
    sent_all(tbuf.at[:, :chips], c_send)
    sent_all(tbuf.at[:, :7], r_send)

    @pl.when(cross)
    def _():
        sent_all(wbuf.at[0, : chunks + 1], d_send.at[0])
        sent_all(gbuf.at[:, : 2 * rows], d_send.at[1])


def copy_kernel(*refs):
    sems = refs[8]
    copies = [pltpu.make_async_copy(refs[k], refs[4 + k], sems.at[k]) for k in range(4)]
    for cp in copies:
        cp.start()
    for cp in copies:
        cp.wait()


def fused(n_inter, hidden_in, norm_gain, qkv_weight, attn_cotangent):
    toks, width = hidden_in.shape[1:]
    rows, cols = qkv_weight.shape
    nz = n_inter // (CORES * SIDE)
    chips = nz * SIDE
    seq, half, chunks = 2 * toks, HEADS // 2, cols // CHUNK
    lanes = n_inter // PIECES * rows
    freqs = rope_base ** (-np.arange(HD // 2, dtype=np.float32) / np.float32(HD // 2))
    angles = (np.arange(seq, dtype=np.float32)[:, None] * freqs.astype(np.float32)[None, :]).astype(np.float32)
    cosine = np.concatenate([np.cos(angles)] * 2, axis=1).astype(np.float32)
    sine = np.concatenate([-np.sin(angles), np.sin(angles)], axis=1).astype(np.float32)
    bf, f32, dma = jnp.bfloat16, jnp.float32, pltpu.SemaphoreType.DMA
    vmem = pl.BlockSpec(memory_space=pltpu.VMEM)
    hbm = pl.BlockSpec(memory_space=pltpu.HBM)
    V = pltpu.VMEM
    ins = (hidden_in[0], norm_gain[None], qkv_weight, attn_cotangent[0], jnp.asarray(cosine), jnp.asarray(sine))
    attn, gin, wg, gg = pl.pallas_call(
        functools.partial(fused_kernel, n_inter),
        out_shape=(V((toks, HEADS * HD), bf), V((toks, width), bf), V((rows, cols), f32), V((1, rows), f32)),
        in_specs=[hbm] * 6,
        out_specs=(vmem,) * 4,
        scratch_shapes=[
            V((chunks, n_inter, rows, CHUNK), bf),
            V((1, n_inter * rows), f32),
            V((1, rows), bf),
            V((PIECES, seq, lanes), bf),
            V((PIECES, toks, lanes), bf),
            V((PIECES, seq, lanes), bf),
            V((n_inter * rows, seq), bf),
            V((seq, HD), f32),
            V((8, toks), f32),
            V((8, toks), f32),
            V((seq, half * HD), bf),
            V((toks, half * HD), bf),
            V((seq, HD), f32),
            V((seq, HD), f32),
            V((chunks, seq, CHUNK), f32),
            V((seq, CHUNK), bf),
            V((seq, CHUNK), bf),
            V((half, seq, HD), bf),
            V((half, seq, HD), bf),
            V((half, 2, seq, HD), bf),
            V((seq, CHUNK), bf),
            V((seq, CHUNK), bf),
            V((8, seq), f32),
            V((8, seq), f32),
            V((half, seq, HD), bf),
            V((half, toks, HD), bf),
            V((PIECES, seq, lanes), bf),
            V((PIECES, toks, lanes), bf),
            V((chunks, n_inter, rows, CHUNK), bf),
            V((chunks, chips, rows, CHUNK), bf),
            V((chunks, nz, rows, CHUNK), bf),
            V((chunks, nz, rows, CHUNK), bf),
            V((chunks, nz - 1, rows, CHUNK), bf),
            V((chunks, nz - 1, rows, CHUNK), bf),
            V((chunks, rows, CHUNK), bf),
            V((chunks, rows, CHUNK), bf),
            V((chunks, rows, CHUNK), bf),
            V((1, rows), f32),
            V((1, rows), f32),
            V((rows, CHUNK), bf),
            V((1, rows), f32),
            dma((8,)),
            dma((chunks * SPLIT,)), dma((chunks * SPLIT, chips)), dma((chunks * SPLIT,)),
            dma((2,)), dma((3,)), dma((13,)),
            dma, dma((chunks, 2)), dma, dma((chunks, nz)), dma((chunks,)), dma((chunks,)),
            dma((2,)), dma((5,)),
        ],
        compiler_params=pltpu.CompilerParams(
            collective_id=0, has_side_effects=True, vmem_limit_bytes=32 * 2**20
        ),
    )(*[pltpu.with_memory_space_constraint(a, pltpu.HBM) for a in ins])
    outs = (attn, gin, wg, gg)
    attn, gin, wg, gg = pl.pallas_call(
        copy_kernel,
        out_shape=tuple(jax.ShapeDtypeStruct(o.shape, o.dtype) for o in outs),
        in_specs=[vmem] * 4,
        out_specs=(hbm,) * 4,
        scratch_shapes=[dma((4,))],
        compiler_params=pltpu.CompilerParams(vmem_limit_bytes=2**20),
    )(*[pltpu.with_memory_space_constraint(o, pltpu.VMEM) for o in outs])
    return attn[None], gin[None], wg, gg[0]


def solution(mesh):
    n_inter, n_intra = mesh.shape["inter"], mesh.shape["intra"]

    def body(hidden_in, norm_gain, qkv_weight, attn_cotangent):
        nz = n_inter // (CORES * SIDE)
        fits = n_intra == 2 and n_inter % (CORES * SIDE) == 0 and nz > 1 and nz & (nz - 1) == 0
        fits = fits and qkv_weight.shape[0] == HD and hidden_in.shape[0] == 1
        fits = fits and hidden_in.shape[1] == HD and n_inter % PIECES == 0 and HEADS == 4 and nz == 4
        if fits:
            return fused(n_inter, hidden_in, norm_gain, qkv_weight, attn_cotangent)
        return local(hidden_in, norm_gain, qkv_weight, attn_cotangent)

    return jax.shard_map(
        body,
        mesh=mesh,
        in_specs=(
            P("inter", "intra", None),
            P(("inter", "intra")),
            P(("inter", "intra"), None),
            P("inter", "intra", None),
        ),
        out_specs=(
            P("inter", "intra", None),
            P("inter", "intra", None),
            P(("intra", "inter"), None),
            P(("intra", "inter")),
        ),
        check_vma=False,
    )
```
